32 devices in a mesh: dom: 8 (over z, x), sub: 4 (over y, core).
Axes of the slice: x: 2, y: 2, z: 4, core: 2. Of those that a mesh axis runs over, the one named last changes fastest.
Arguments:
- load_vector: float32 [64, 128], P(('dom', 'sub')), may hold values from -38 to 38
- recycled: float32 [40, 64, 128], P(None, ('dom', 'sub')), may hold values from -6 to 6
- images: float32 [40, 64, 128], P(None, ('dom', 'sub')), may hold values from -6 to 6
- matrix_tiles: float32 [64, 8, 128, 128], P(('dom', 'sub')), may hold values from -7 to 7
- tile_columns: int32 [64, 8], P(('dom', 'sub')), may hold values from 0 to 5, as said below
- ghost_list: int32 [32, 4], P(('dom', 'sub')), may hold values from 0 to 23, as said below
- live_counts: int32 [32], P(('dom', 'sub')), may hold values from 1 to 2, as said below
Outputs:
- solution: float32 [64, 128], P(('dom', 'sub'))
- residual: float32 [64, 128], P(('dom', 'sub'))
The draws below stay inside these ranges and needn't reach their ends.
Inputs may be any that keep to these rules, and one draw needn't show every extreme that they name: `live_counts`: each device's live block rows are its first slots; some device has all 2 live. `tile_columns`: tile 0 of a block row names the row's own slot. Other entries below 2 name a live slot of the same device; entries from 2 on name a ghost slot of that device. `ghost_list`: each entry names a live slot q of a device with sub index s and dom index differing from the owner's by o - 1 (o of 0, 1, 2), coded as o * (size of sub) * 2 + s * 2 + q; it never points outside the dom axis and never to the owner itself.
All inputs are finite; a program needn't handle non-finite values.
Results may differ from the reference program's by a relative error of at most 0.0003.
Values sent between devices are 32-bit elements; how exact they have to be, the bound alone decides.
No kernel may reach another device: no remote copies, remote signals or barrier semaphores. Data moves between devices by JAX's collectives and lax.ppermute only.
A program may use at most 64 MiB of HBM per device.

```python
import math
import jax
import jax.numpy as jnp
from jax import lax

SLOTS = 2
BLK = 128
TPR = 8
K = 40
STEPS = 3
GHOSTS = 4
ROWBLOCKS = 64
ROWS = 8192
N_DOM = 8
N_SUB = 4
DEVICES = 32


def live_draw(key):
    base = jax.random.fold_in(key, 101)
    first_key, second_key, third_key = jax.random.split(base, 3)
    factor_a = jax.random.randint(first_key, (DEVICES,), 0, SLOTS + 1)
    factor_b = jax.random.randint(second_key, (DEVICES,), 0, SLOTS + 1)
    counts = 1 + jnp.minimum(factor_a * factor_b // SLOTS, SLOTS - 1)
    chosen = jax.random.randint(third_key, (), 0, DEVICES)
    counts = jnp.where(jnp.arange(DEVICES) == chosen, SLOTS, counts)
    return counts.astype(jnp.int32)


def draw_live_counts(key, part):
    return live_draw(key)


def draw_ghost_list(key, part):
    counts = live_draw(key)
    base = jax.random.fold_in(key, 202)
    first_key, second_key, third_key = jax.random.split(base, 3)
    device = jnp.arange(DEVICES, dtype=jnp.int32)[:, None]
    dom_index = device // N_SUB
    sub_index = device % N_SUB
    offset = jax.random.randint(first_key, (DEVICES, GHOSTS), 0, 3) - 1
    offset = jnp.where(dom_index + offset < 0, 1, offset)
    offset = jnp.where(dom_index + offset >= N_DOM, -1, offset)
    peer = jax.random.randint(second_key, (DEVICES, GHOSTS), 0, N_SUB)
    peer = jnp.where((offset == 0) & (peer == sub_index), (peer + 1) % N_SUB, peer)
    neighbour = (dom_index + offset) * N_SUB + peer
    slot_pick = jax.random.randint(third_key, (DEVICES, GHOSTS), 0, 1 << 20) % counts[neighbour]
    return ((offset + 1) * N_SUB * SLOTS + peer * SLOTS + slot_pick).astype(jnp.int32)


def draw_tile_columns(key, part):
    counts = live_draw(key)
    base = jax.random.fold_in(key, 303)
    first_key, second_key, third_key = jax.random.split(base, 3)
    block_row = jnp.arange(ROWBLOCKS, dtype=jnp.int32)
    device = block_row // SLOTS
    own_slot = block_row % SLOTS
    coin_flip = jax.random.randint(first_key, (ROWBLOCKS, TPR), 0, 2)
    local_pick = jax.random.randint(second_key, (ROWBLOCKS, TPR), 0, 1 << 20) % counts[device][:, None]
    ghost_pick = SLOTS + jax.random.randint(third_key, (ROWBLOCKS, TPR), 0, GHOSTS)
    columns = jnp.where(coin_flip == 1, ghost_pick, local_pick)
    columns = jnp.where(jnp.arange(TPR)[None, :] == 0, own_slot[:, None], columns)
    return columns.astype(jnp.int32)


def draw_matrix_tiles(key, part):
    base = jax.random.fold_in(key, 404)
    first_key, second_key = jax.random.split(base, 2)
    shape = (ROWBLOCKS, TPR, BLK, BLK)
    noise = jnp.clip(jax.random.normal(first_key, shape, jnp.float32), -5.0, 5.0)
    diagonal = jax.random.uniform(second_key, (ROWBLOCKS, 1, BLK, 1), jnp.float32, 2.0, 6.0)
    tile_index = jnp.arange(TPR)[None, :, None, None]
    scale = jnp.where(tile_index == 0, 0.5 / math.sqrt(BLK), 1.0 / math.sqrt(BLK * TPR))
    identity = jnp.eye(BLK, dtype=jnp.float32)[None, None]
    first_tile = jnp.where(tile_index == 0, 1.0, 0.0)
    return (noise * scale + first_tile * identity * diagonal).astype(jnp.float32)


def draw_load_vector(key, part):
    base = jax.random.fold_in(key, 505)
    first_key, second_key = jax.random.split(base, 2)
    device = (jnp.arange(ROWBLOCKS) // SLOTS).astype(jnp.float32)
    trend = 1.0 + 2.0 * device / (DEVICES - 1)
    spread = jnp.power(10.0, jax.random.uniform(second_key, (ROWBLOCKS, BLK), jnp.float32, 0.0, 1.0))
    values = jnp.clip(jax.random.normal(first_key, (ROWBLOCKS, BLK), jnp.float32), -5.0, 5.0)
    return (values * trend[:, None] * spread / 4.0).astype(jnp.float32)


def block_scale(key, extent, shards, low, largest):
    gain, own = 1.0, jax.random.fold_in(key, 6)
    for position, blocks in shards:
        heights = jnp.exp(jax.random.uniform(jax.random.fold_in(own, position), (blocks,), jnp.float32, low / len(shards), largest / len(shards)))
        gain = gain * jnp.repeat(heights, extent[position] // blocks).reshape([-1 if axis == position else 1 for axis in range(len(extent))])
    return gain


def bell_draw(own_key, extent, scale, bound, cuts=(), kind=jnp.bfloat16):
    level = block_scale(own_key, extent, cuts, -0.22, 0.18) if cuts else 1.0
    entries = jax.random.normal(own_key, extent, jnp.float32) * scale * level
    return jnp.minimum(jnp.maximum(entries, -bound), bound).astype(kind)


def setup_inputs(seed: int = 0) -> dict:
    seeds = jax.random.split(jax.random.key(seed), 8)
    return {
        "load_vector": draw_load_vector(jax.random.fold_in(seeds[7], 71), 0),
        "recycled": bell_draw(seeds[1], (K, ROWBLOCKS, BLK), (ROWS ** 0.5 / K), 6.0, ((1, 32),), jnp.float32),
        "images": bell_draw(seeds[2], (K, ROWBLOCKS, BLK), 1.0, 6.0, ((1, 32),), jnp.float32),
        "matrix_tiles": draw_matrix_tiles(jax.random.fold_in(seeds[7], 71), 0),
        "tile_columns": draw_tile_columns(jax.random.fold_in(seeds[7], 71), 0),
        "ghost_list": draw_ghost_list(jax.random.fold_in(seeds[7], 71), 0),
        "live_counts": draw_live_counts(jax.random.fold_in(seeds[7], 71), 0),
    }


def triangle_solve(factor, values, transpose):
    column = values if values.ndim == 2 else values[:, None]
    solved = lax.linalg.triangular_solve(factor, column, left_side=True, lower=True, transpose_a=transpose)
    return solved if values.ndim == 2 else solved[:, 0]

def global_columns(tile_columns, ghost_list):
    block_row = jnp.arange(ROWBLOCKS, dtype=jnp.int32)
    device = block_row // SLOTS
    ghost_rows = ghost_list[device]
    ghost_slot = jnp.clip(tile_columns - SLOTS, 0, GHOSTS - 1).astype(jnp.int32)
    ghost_code = jnp.take_along_axis(ghost_rows, ghost_slot, axis=1)
    group_size = N_SUB * SLOTS
    offset = ghost_code // group_size
    remainder = ghost_code % group_size
    dom_index = (device // N_SUB)[:, None]
    remote = ((dom_index + offset - 1) * N_SUB + remainder // SLOTS) * SLOTS + remainder % SLOTS
    local = device[:, None] * SLOTS + tile_columns
    return jnp.where(tile_columns < SLOTS, local, remote).astype(jnp.int32)

def apply_matrix(vector, matrix_tiles, columns, live_mask):
    picked = vector.reshape(ROWBLOCKS, BLK)[columns]
    product = jnp.einsum('rtij,rtj->ri', matrix_tiles, picked, precision=lax.Precision.HIGHEST)
    return (product * live_mask).reshape(-1)

def reference(load_vector, recycled, images, matrix_tiles, tile_columns, ghost_list, live_counts):
    highest = lax.Precision.HIGHEST
    block_row = jnp.arange(ROWBLOCKS, dtype=jnp.int32)
    live_mask = (block_row % SLOTS < live_counts[block_row // SLOTS]).astype(jnp.float32)[:, None]
    columns = global_columns(tile_columns, ghost_list)
    source = (load_vector * live_mask).reshape(-1)
    recycled_flat = (recycled * live_mask[None]).reshape(K, -1)
    images_flat = (images * live_mask[None]).reshape(K, -1)
    gram_matrix = jnp.dot(images_flat, images_flat.T, precision=highest)
    projection = jnp.dot(images_flat, source, precision=highest)
    source_norm = jnp.sum(source * source)
    cholesky_low = jnp.linalg.cholesky(gram_matrix)
    reduced = triangle_solve(cholesky_low, projection, False)
    start_coef = triangle_solve(cholesky_low, reduced, True)
    initial_norm = jnp.sqrt(source_norm - jnp.sum(reduced * reduced))
    start_point = jnp.dot(start_coef, recycled_flat, precision=highest)
    start_residual = source - jnp.dot(start_coef, images_flat, precision=highest)
    basis = [start_residual / initial_norm]
    hessenberg = jnp.zeros((STEPS + 1, STEPS), jnp.float32)
    coupling = jnp.zeros((K, STEPS), jnp.float32)
    for column in range(STEPS):
        image_now = apply_matrix(basis[column], matrix_tiles, columns, live_mask)
        stacked = jnp.stack(basis)
        against_images = triangle_solve(cholesky_low, jnp.dot(images_flat, image_now, precision=highest), False)
        against_basis = jnp.dot(stacked, image_now, precision=highest)
        image_norm = jnp.sum(image_now * image_now)
        next_norm = jnp.sqrt(image_norm - jnp.sum(against_images * against_images) - jnp.sum(against_basis * against_basis))
        back_coef = triangle_solve(cholesky_low, against_images, True)
        remaining = image_now - jnp.dot(back_coef, images_flat, precision=highest) - jnp.dot(against_basis, stacked, precision=highest)
        basis.append(remaining / next_norm)
        hessenberg = hessenberg.at[:column + 1, column].set(against_basis)
        hessenberg = hessenberg.at[column + 1, column].set(next_norm)
        coupling = coupling.at[:, column].set(against_images)
    normal_matrix = jnp.dot(hessenberg.T, hessenberg, precision=highest)
    target = initial_norm * hessenberg[0]
    small_factor = jnp.linalg.cholesky(normal_matrix)
    least = triangle_solve(small_factor, triangle_solve(small_factor, target, False), True)
    every_basis = jnp.stack(basis)
    update_coef = triangle_solve(cholesky_low, jnp.dot(coupling, least, precision=highest), True)
    solution = start_point + jnp.dot(least, every_basis[:STEPS], precision=highest) - jnp.dot(update_coef, recycled_flat, precision=highest)
    residual = start_residual - jnp.dot(jnp.dot(hessenberg, least, precision=highest), every_basis, precision=highest)
    return (solution.reshape(ROWBLOCKS, BLK), residual.reshape(ROWBLOCKS, BLK))
```

```python
import jax
import jax.numpy as jnp
from jax import lax
from jax.sharding import PartitionSpec as P

STEPS = 3


def total(values):
    axes = ("dom", "sub")
    flat = jnp.concatenate([value.reshape(-1) for value in values])
    lanes = 128
    rows = -(-flat.shape[0] // lanes)
    packed = jnp.pad(flat, (0, rows * lanes - flat.shape[0])).reshape(rows, lanes)
    count = lax.axis_size("dom") * lax.axis_size("sub")
    every = lax.all_to_all(jnp.broadcast_to(packed[None], (count, rows, lanes)), axes, 0, 0)
    summed = jnp.sum(every, axis=0).reshape(-1)
    results = []
    offset = 0
    for value in values:
        results.append(summed[offset : offset + value.size].reshape(value.shape))
        offset += value.size
    return results


def padded(value, sides, width):
    for axis, dim in sides:
        count, length = (lax.axis_size(axis), value.shape[dim])
        up = [(i, (i + 1) % count) for i in range(count - 1)]
        down = [(j, i) for i, j in up]
        last = lax.slice_in_dim(value, length - width, length, axis=dim)
        first = lax.slice_in_dim(value, 0, width, axis=dim)
        before = lax.ppermute(last, axis, up)
        after = lax.ppermute(first, axis, down)
        value = jnp.concatenate([before, value, after], axis=dim)
    return value


def triangle_solve(factor, values, transpose):
    column = values if values.ndim == 2 else values[:, None]
    solved = lax.linalg.triangular_solve(
        factor, column, left_side=True, lower=True, transpose_a=transpose
    )
    return solved if values.ndim == 2 else solved[:, 0]


def multiply(vector, matrix_tiles, tile_columns, ghost_codes):
    slot_count = vector.shape[0]
    group_size = lax.axis_size("sub") * slot_count
    gathered = lax.all_gather(vector, "sub", axis=0, tiled=True)
    nearby = padded(gathered, (("dom", 0),), group_size)
    ghosts = jnp.take(nearby, ghost_codes, axis=0)
    extended = jnp.concatenate([vector, ghosts], axis=0)
    picked = jnp.take(extended, tile_columns, axis=0)
    return jnp.einsum("stij,stj->si", matrix_tiles, picked, precision=lax.Precision.HIGHEST)


def local(load_vector, recycled, images, matrix_tiles, tile_columns, ghost_list, live_counts):
    highest = lax.Precision.HIGHEST
    slot_count, tile_width = load_vector.shape
    recycled_count = recycled.shape[0]
    live_mask = (jnp.arange(slot_count) < live_counts[0]).astype(jnp.float32)[:, None]
    ghost_codes = ghost_list[0]
    source = (load_vector * live_mask).reshape(-1)
    recycled_flat = (recycled * live_mask[None]).reshape(recycled_count, -1)
    images_flat = (images * live_mask[None]).reshape(recycled_count, -1)
    gram_matrix, projection, source_norm = total(
        (
            jnp.dot(images_flat, images_flat.T, precision=highest),
            jnp.dot(images_flat, source, precision=highest),
            jnp.sum(source * source),
        )
    )
    cholesky_low = jnp.linalg.cholesky(gram_matrix)
    reduced = triangle_solve(cholesky_low, projection, False)
    initial_norm = jnp.sqrt(source_norm - jnp.sum(reduced * reduced))
    images_hat = triangle_solve(cholesky_low, images_flat, False)
    recycled_hat = triangle_solve(cholesky_low, recycled_flat, False)
    start_point = jnp.dot(reduced, recycled_hat, precision=highest)
    start_residual = source - jnp.dot(reduced, images_hat, precision=highest)
    basis = [start_residual / initial_norm]
    hessenberg = jnp.zeros((STEPS + 1, STEPS), jnp.float32)
    coupling = jnp.zeros((recycled_count, STEPS), jnp.float32)
    for column in range(STEPS):
        image_now = multiply(
            basis[column].reshape(slot_count, tile_width), matrix_tiles, tile_columns, ghost_codes
        )
        image_now = (image_now * live_mask).reshape(-1)
        stacked = jnp.stack(basis)
        local_images = jnp.dot(images_hat, image_now, precision=highest)
        summed_images, against_basis, image_norm = total(
            (
                local_images,
                jnp.dot(stacked, image_now, precision=highest),
                jnp.sum(image_now * image_now),
            )
        )
        correction = jnp.dot(summed_images, images_hat, precision=highest)
        next_norm = jnp.sqrt(
            image_norm
            - jnp.sum(summed_images * summed_images)
            - jnp.sum(against_basis * against_basis)
        )
        remaining = image_now - correction - jnp.dot(against_basis, stacked, precision=highest)
        basis.append(remaining / next_norm)
        hessenberg = hessenberg.at[: column + 1, column].set(against_basis)
        hessenberg = hessenberg.at[column + 1, column].set(next_norm)
        coupling = coupling.at[:, column].set(summed_images)
    normal_matrix = jnp.dot(hessenberg.T, hessenberg, precision=highest)
    target = initial_norm * hessenberg[0]
    small_factor = jnp.linalg.cholesky(normal_matrix)
    least = triangle_solve(small_factor, triangle_solve(small_factor, target, False), True)
    every_basis = jnp.stack(basis)
    coupled = jnp.dot(coupling, least, precision=highest)
    recycled_term = jnp.dot(coupled, recycled_hat, precision=highest)
    solution = start_point + jnp.dot(least, every_basis[:STEPS], precision=highest) - recycled_term
    residual = start_residual - jnp.dot(
        jnp.dot(hessenberg, least, precision=highest), every_basis, precision=highest
    )
    return (solution.reshape(slot_count, tile_width), residual.reshape(slot_count, tile_width))


def solution(mesh):
    return jax.shard_map(
        local,
        mesh=mesh,
        in_specs=(
            P(("dom", "sub"), None),
            P(None, ("dom", "sub"), None),
            P(None, ("dom", "sub"), None),
            P(("dom", "sub"), None, None, None),
            P(("dom", "sub"), None),
            P(("dom", "sub"), None),
            P(("dom", "sub")),
        ),
        out_specs=(P(("dom", "sub"), None), P(("dom", "sub"), None)),
        check_vma=False,
    )
```

```python
import functools

import jax
import jax.numpy as jnp
from jax import lax
from jax.experimental import pallas as pl
from jax.experimental.pallas import tpu as pltpu
from jax.sharding import PartitionSpec as P

STEPS = 3
TAIL = 8
ROW_ALIGN = 8
AXES = ("dom", "sub")
VMEM = pl.BlockSpec(memory_space=pltpu.VMEM)
SMEM = pl.BlockSpec(memory_space=pltpu.SMEM)
F32 = jnp.float32


def call(body, name, outs, specs, scratch=()):
    return pl.pallas_call(
        body,
        name=name,
        out_shape=[jax.ShapeDtypeStruct(shape, F32) for shape in outs],
        in_specs=specs,
        out_specs=[VMEM] * len(outs),
        scratch_shapes=list(scratch),
        compiler_params=pltpu.CompilerParams(vmem_limit_bytes=16 * 1024 * 1024),
    )


def round_up(value, step):
    return -(-value // step) * step


def eye(rows, lanes):
    down = lax.broadcasted_iota(jnp.int32, (rows, lanes), 0)
    across = lax.broadcasted_iota(jnp.int32, (rows, lanes), 1)
    return down == across


def to_row(column, mask):
    return jnp.sum(jnp.where(mask, column, 0.0), axis=0, keepdims=True)


def live(live_ref, slot):
    return jnp.where(slot < live_ref[0], 1.0, 0.0).astype(F32)


def tree_sum(parts):
    while len(parts) > 1:
        pairs = [parts[i] + parts[i + 1] for i in range(0, len(parts) - 1, 2)]
        parts = pairs + parts[len(parts) - len(parts) % 2 :]
    return parts[0]


def pack_body(live_ref, load_ref, images_ref, own_ref):
    count, slots, width = images_ref.shape
    rows = own_ref.shape[1]
    for slot in range(slots):
        mask = live(live_ref, slot)
        own_ref[slot, 0:count, :] = images_ref[:, slot, :] * mask
        own_ref[slot, count : count + 1, :] = load_ref[slot : slot + 1, :] * mask
        own_ref[slot, count + 1 : rows, :] = jnp.zeros((rows - count - 1, width), F32)


def lane_groups(count, rows, width):
    groups = width // (count + 1)
    if rows % groups == 0 and (rows // groups) % ROW_ALIGN == 0:
        return groups
    return 1


def gram_body(count, group_ref, out_ref):
    blocks, rows, width = group_ref.shape
    products = []
    for block in range(blocks):
        part = group_ref[block]
        products.append(
            lax.dot_general(
                part, part, (((1,), (1,)), ((), ())),
                precision=lax.Precision.HIGHEST, preferred_element_type=F32,
            )
        )
    gram = jnp.concatenate([tree_sum(products), jnp.zeros((rows, width - rows), F32)], axis=1)
    groups = lane_groups(count, rows, width)
    each, lanes = rows // groups, width // groups
    packed = gram[0:each]
    for group in range(1, groups):
        packed = packed + pltpu.roll(gram[group * each : (group + 1) * each], group * lanes, 1)
    for copy in range(out_ref.shape[0]):
        out_ref[copy] = packed


def sweep(matrix, count):
    rows, width = matrix.shape
    down = lax.broadcasted_iota(jnp.int32, (rows, width), 0)
    across = lax.broadcasted_iota(jnp.int32, (rows, width), 1)
    for k in range(count):
        pivot_row = matrix[k : k + 1, :]
        column = matrix[:, k : k + 1]
        inverse = 1.0 / pivot_row[:, k : k + 1]
        lane_k = across == k
        scaled = jnp.where(lane_k[0:1], inverse, pivot_row * inverse)
        kept = jnp.where(lane_k, 0.0, matrix)
        matrix = jnp.where(down == k, scaled, kept - column * scaled)
    return matrix


def apply_tiles(tiles_ref, columns_ref, vector_ref, live_ref):
    slots, per_row, size, _ = tiles_ref.shape
    mask = eye(size, size)
    images = []
    for slot in range(slots):
        parts = []
        for t in range(per_row):
            picked = vector_ref[pl.ds(columns_ref[slot, t], 1), :]
            parts.append(tiles_ref[slot, t] * picked)
        column = jnp.sum(tree_sum(parts), axis=1, keepdims=True)
        images.append(to_row(column, mask) * live(live_ref, slot))
    return images


def tail_with(old, entries):
    down = lax.broadcasted_iota(jnp.int32, (TAIL, old.shape[1]), 0)
    for row, value in entries:
        old = jnp.where(down == row, value, old)
    return old


def finish_step(step, tails, own_ref, images, tail_ref, out_ref):
    slots, rows, width = own_ref.shape
    last = STEPS
    total = jnp.zeros((rows + TAIL, width), F32)
    for slot in range(slots):
        tails[slot] = tail_with(tails[slot], [(last, images[slot])])
        total = total + jnp.concatenate([own_ref[slot], tails[slot]], axis=0) * images[slot]
    for block, tail in enumerate(tails):
        tail_ref[block] = tail
    partial = to_row(jnp.sum(total, axis=1, keepdims=True), eye(rows + TAIL, width))
    copies, lines, _ = out_ref.shape
    if lines == 1:
        message = partial
    else:
        pad = [jnp.zeros((lines - slots - 1, width), F32)] if lines > slots + 1 else []
        message = jnp.concatenate([*images, partial, *pad], axis=0)
    out_ref[...] = jnp.broadcast_to(message[None], (copies, lines, width))


def start_body(
    count, live_ref, columns_ref, ghosts_ref, parts_ref, own_ref, before_ref, group_ref, after_ref, tiles_ref,
    out_ref, ghost_ref, tail_ref, inverse_ref, start_ref, vector_ref,
):
    slots, rows, width = own_ref.shape
    blocks = group_ref.shape[0]
    ghosts = ghosts_ref.shape[1]
    groups = lane_groups(count, rows, width)
    lanes = width // groups
    packed = tree_sum([parts_ref[i] for i in range(parts_ref.shape[0])])
    across = lax.broadcasted_iota(jnp.int32, (rows, width), 1)
    down = lax.broadcasted_iota(jnp.int32, (rows, width), 0)
    pieces = [packed]
    for group in range(1, groups):
        pieces.append(pltpu.roll(packed, width - group * lanes, 1))
    gram = jnp.where(across <= count, jnp.concatenate(pieces, axis=0), 0.0)
    swept = sweep(gram, count)
    keep = (down < count) & (across < count)
    inverse_ref[0:rows, :] = jnp.where(keep, swept, 0.0)
    tail_down = lax.broadcasted_iota(jnp.int32, (TAIL, width), 0)
    tail_across = lax.broadcasted_iota(jnp.int32, (TAIL, width), 1)
    inverse_ref[rows : rows + TAIL, :] = jnp.where(
        (tail_down < STEPS) & (tail_across == tail_down + rows), 1.0, 0.0
    )
    squared = swept[count : count + 1, count : count + 1]
    scale = 1.0 / jnp.sqrt(squared)
    start = jnp.where(down < count, -swept[:, count : count + 1], jnp.where(down == count, 1.0, 0.0))
    start_ref[0:rows, :] = start
    start_ref[rows : rows + TAIL, :] = jnp.broadcast_to(jnp.sqrt(squared), (TAIL, width))
    coefficients = start * scale
    tails = []
    for block in range(slots + ghosts):
        if block < slots:
            held = own_ref[block]
        else:
            code = ghosts_ref[0, block - slots]
            offset = code // blocks
            place = code - offset * blocks
            held = jnp.where(
                offset == 0, before_ref[place], jnp.where(offset == 1, group_ref[place], after_ref[place])
            )
            ghost_ref[block - slots] = held
        vector = jnp.sum(held * coefficients, axis=0, keepdims=True)
        vector_ref[block : block + 1, :] = vector
        tails.append(tail_with(jnp.zeros((TAIL, width), F32), [(0, vector)]))
    images = apply_tiles(tiles_ref, columns_ref, vector_ref, live_ref)
    finish_step(0, tails, own_ref, images, tail_ref, out_ref)


def project(total_row, inverse, rows, width):
    full = rows + TAIL
    down = lax.broadcasted_iota(jnp.int32, (full, width), 0)
    projected = jnp.sum(inverse * total_row, axis=1, keepdims=True)
    column = jnp.sum(jnp.where(eye(full, width), total_row, 0.0), axis=1, keepdims=True)
    projected = jnp.broadcast_to(projected, (full, width))
    squared = jnp.sum(
        jnp.where(down == rows + STEPS, column, -(column * projected)), axis=0, keepdims=True
    )
    return projected, jnp.sqrt(squared), down


def step_body(
    step, count, live_ref, columns_ref, ghosts_ref, every_ref, own_ref, ghost_ref, old_ref, inverse_ref, tiles_ref,
    out_ref, tail_ref, history_ref, vector_ref,
):
    slots, rows, width = own_ref.shape
    ghosts = ghosts_ref.shape[1]
    subs = lax.axis_size("sub")
    span = subs * slots
    dom = lax.axis_index("dom")
    total_row = tree_sum([every_ref[i, slots : slots + 1, :] for i in range(every_ref.shape[0])])
    projected, norm, down = project(total_row, inverse_ref[...], rows, width)
    history_ref[...] = jnp.where(down == count, norm, projected)
    inverse_norm = 1.0 / norm
    coefficients = jnp.where(down == rows + STEPS, inverse_norm, -(projected * inverse_norm))
    tails = []
    for block in range(slots + ghosts):
        old = old_ref[block]
        if block < slots:
            held = own_ref[block]
        else:
            held = ghost_ref[block - slots]
            code = ghosts_ref[0, block - slots]
            offset = code // span
            place = code - offset * span
            peer = place // slots
            device = (dom + offset - 1) * subs + peer
            image = every_ref[device, pl.ds(place - peer * slots, 1), :]
            old = tail_with(old, [(STEPS, image)])
        vector = jnp.sum(held * coefficients[0:rows], axis=0, keepdims=True)
        vector = vector + jnp.sum(old * coefficients[rows : rows + TAIL], axis=0, keepdims=True)
        vector_ref[block : block + 1, :] = vector
        tails.append(tail_with(old, [(step, vector), (STEPS, 0.0)]))
    images = apply_tiles(tiles_ref, columns_ref, vector_ref, live_ref)
    finish_step(step, tails, own_ref, images, tail_ref, out_ref)


def small_solve(matrix, target):
    size = len(target)
    low = [[None] * size for _ in range(size)]
    inverses = []
    for j in range(size):
        value = matrix[j][j]
        for k in range(j):
            value = value - low[j][k] * low[j][k]
        inverses.append(1.0 / jnp.sqrt(value))
        for i in range(j + 1, size):
            value = matrix[i][j]
            for k in range(j):
                value = value - low[i][k] * low[j][k]
            low[i][j] = value * inverses[j]
    forward = []
    for i in range(size):
        value = target[i]
        for k in range(i):
            value = value - low[i][k] * forward[k]
        forward.append(value * inverses[i])
    back = [None] * size
    for i in reversed(range(size)):
        value = forward[i]
        for k in range(i + 1, size):
            value = value - low[k][i] * back[k]
        back[i] = value * inverses[i]
    return back


def end_body(count, live_ref, every_ref, own_ref, tail_ref, inverse_ref, start_ref, recycled_ref, *rest):
    histories, (solution_ref, residual_ref) = rest[:-2], rest[-2:]
    slots, rows, width = own_ref.shape
    full = rows + TAIL
    total_row = tree_sum([every_ref[i] for i in range(every_ref.shape[0])])
    projected, norm, down = project(total_row, inverse_ref[...], rows, width)
    columns = [history[...] for history in histories]
    columns.append(jnp.where(down == count, norm, projected))
    entries = []
    for j in range(STEPS):
        column = [columns[j][rows + i : rows + i + 1, :] for i in range(j + 1)]
        column.append(columns[j][count : count + 1, :])
        entries.append(column)
    normal = [[None] * STEPS for _ in range(STEPS)]
    for a in range(STEPS):
        for b in range(a + 1):
            shared = range(min(len(entries[a]), len(entries[b])))
            normal[a][b] = tree_sum([entries[a][r] * entries[b][r] for r in shared])
    initial = start_ref[rows : rows + 1, :]
    least = small_solve(normal, [initial * entries[j][0] for j in range(STEPS)])
    image = []
    for r in range(STEPS + 1):
        image.append(tree_sum([entries[j][r] * least[j] for j in range(STEPS) if r < len(entries[j])]))
    start = start_ref[0:rows, :]
    recycled_coefficients = start[0:count] * -1.0
    for j in range(STEPS):
        recycled_coefficients = recycled_coefficients - columns[j][0:count] * least[j]
    ratio = image[STEPS] / norm
    head = jnp.where(down[0:rows] < count, start + columns[-1][0:rows] * ratio, start)
    tail_down = down[0:TAIL]
    solution_tail = jnp.zeros((TAIL, width), F32)
    residual_tail = jnp.zeros((TAIL, width), F32)
    for j in range(STEPS):
        solution_tail = jnp.where(tail_down == j, least[j], solution_tail)
        residual_tail = jnp.where(tail_down == j, entries[-1][j] * ratio - image[j], residual_tail)
    residual_tail = jnp.where(tail_down == STEPS, -ratio, residual_tail)
    for slot in range(slots):
        tail = tail_ref[slot]
        mask = live(live_ref, slot)
        point = jnp.sum(recycled_ref[:, slot, :] * mask * recycled_coefficients, axis=0, keepdims=True)
        point = point + jnp.sum(tail * solution_tail, axis=0, keepdims=True)
        solution_ref[slot : slot + 1, :] = point
        left = jnp.sum(own_ref[slot] * head, axis=0, keepdims=True)
        left = left + jnp.sum(tail * residual_tail, axis=0, keepdims=True)
        residual_ref[slot : slot + 1, :] = left


def local(load_vector, recycled, images, matrix_tiles, tile_columns, ghost_list, live_counts):
    slots, width = load_vector.shape
    count = recycled.shape[0]
    ghosts = ghost_list.shape[1]
    doms, subs = lax.axis_size("dom"), lax.axis_size("sub")
    devices = doms * subs
    rows = round_up(count + 1, ROW_ALIGN)
    full = rows + TAIL
    blocks = slots + ghosts
    (own,) = call(pack_body, "pack", [(slots, rows, width)], [SMEM, VMEM, VMEM])(live_counts, load_vector, images)
    group = lax.all_gather(own, "sub", axis=0, tiled=True)
    up = [(i, i + 1) for i in range(doms - 1)]
    down = [(j, i) for i, j in up]
    before = lax.ppermute(group, "dom", up)
    after = lax.ppermute(group, "dom", down)
    each = rows // lane_groups(count, rows, width)
    (grams,) = call(functools.partial(gram_body, count), "gram", [(doms, each, width)], [VMEM])(group)
    parts = lax.all_to_all(grams, "dom", 0, 0)
    lines = round_up(slots + 1, 4)
    scratch = [pltpu.VMEM((round_up(blocks, 8), width), F32)]
    message, ghost_images, tails, inverse, start = call(
        functools.partial(start_body, count),
        "start",
        [(devices, lines, width), (ghosts, rows, width), (blocks, TAIL, width), (full, width), (full, width)],
        [SMEM] * 3 + [VMEM] * 6,
        scratch,
    )(live_counts, tile_columns, ghost_list, parts, own, before, group, after, matrix_tiles)
    histories = []
    for step in range(1, STEPS):
        every = lax.all_to_all(message, AXES, 0, 0)
        sent = lines if step < STEPS - 1 else 1
        message, tails, history = call(
            functools.partial(step_body, step, count),
            f"step{step}",
            [(devices, sent, width), (blocks, TAIL, width), (full, width)],
            [SMEM] * 3 + [VMEM] * 6,
            scratch,
        )(live_counts, tile_columns, ghost_list, every, own, ghost_images, tails, inverse, matrix_tiles)
        histories.append(history)
    every = lax.all_to_all(message, AXES, 0, 0)
    return tuple(
        call(
            functools.partial(end_body, count),
            "end",
            [(slots, width), (slots, width)],
            [SMEM] + [VMEM] * (6 + len(histories)),
        )(live_counts, every, own, tails, inverse, start, recycled, *histories)
    )


def solution(mesh):
    return jax.shard_map(
        local,
        mesh=mesh,
        in_specs=(
            P(("dom", "sub"), None),
            P(None, ("dom", "sub"), None),
            P(None, ("dom", "sub"), None),
            P(("dom", "sub"), None, None, None),
            P(("dom", "sub"), None),
            P(("dom", "sub"), None),
            P(("dom", "sub")),
        ),
        out_specs=(P(("dom", "sub"), None), P(("dom", "sub"), None)),
        check_vma=False,
    )
```

```python
import functools

import jax
import jax.numpy as jnp
from jax import lax
from jax.experimental import pallas as pl
from jax.experimental.pallas import tpu as pltpu
from jax.sharding import PartitionSpec as P

STEPS = 3
TAIL = 8
ROW_ALIGN = 8
AXES = ("dom", "sub")
VMEM = pl.BlockSpec(memory_space=pltpu.VMEM)
SMEM = pl.BlockSpec(memory_space=pltpu.SMEM)
HBM = pl.BlockSpec(memory_space=pltpu.HBM)
F32 = jnp.float32


def call(body, name, outs, specs, scratch=(), work=10_000_000):
    return pl.pallas_call(
        body,
        name=name,
        out_shape=[jax.ShapeDtypeStruct(shape, F32) for shape in outs],
        in_specs=specs,
        out_specs=[VMEM] * len(outs),
        scratch_shapes=list(scratch),
        cost_estimate=pl.CostEstimate(flops=work, bytes_accessed=1 << 20, transcendentals=0),
        compiler_params=pltpu.CompilerParams(vmem_limit_bytes=16 * 1024 * 1024),
    )


def round_up(value, step):
    return -(-value // step) * step


def eye(rows, lanes):
    down = lax.broadcasted_iota(jnp.int32, (rows, lanes), 0)
    across = lax.broadcasted_iota(jnp.int32, (rows, lanes), 1)
    return down == across


def to_row(column, mask):
    return jnp.sum(jnp.where(mask, column, 0.0), axis=0, keepdims=True)


def tree_sum(parts):
    while len(parts) > 1:
        pairs = [parts[i] + parts[i + 1] for i in range(0, len(parts) - 1, 2)]
        parts = pairs + parts[len(parts) - len(parts) % 2 :]
    return parts[0]


def pack_body(live_ref, load_ref, images_ref, own_ref, mask_ref):
    count, slots, width = images_ref.shape
    rows = own_ref.shape[1]
    line = lax.broadcasted_iota(jnp.int32, mask_ref.shape, 0)
    mask_ref[...] = jnp.where(line < live_ref[0], 1.0, 0.0).astype(F32)
    for slot in range(slots):
        mask = jnp.where(slot < live_ref[0], 1.0, 0.0).astype(F32)
        own_ref[slot, 0:count, :] = images_ref[:, slot, :] * mask
        own_ref[slot, count : count + 1, :] = load_ref[slot : slot + 1, :] * mask
        own_ref[slot, count + 1 : rows, :] = jnp.zeros((rows - count - 1, width), F32)


def lane_groups(count, rows, width):
    groups = width // (count + 1)
    if rows % groups == 0 and (rows // groups) % ROW_ALIGN == 0:
        return groups
    return 1


def gram_body(count, group_ref, out_ref):
    blocks, rows, width = group_ref.shape
    products = []
    for block in range(blocks):
        part = group_ref[block]
        products.append(
            lax.dot_general(
                part, part, (((1,), (1,)), ((), ())),
                precision=lax.Precision.HIGHEST, preferred_element_type=F32,
            )
        )
    gram = jnp.concatenate([tree_sum(products), jnp.zeros((rows, width - rows), F32)], axis=1)
    groups = lane_groups(count, rows, width)
    each, lanes = rows // groups, width // groups
    packed = gram[0:each]
    for group in range(1, groups):
        packed = packed + pltpu.roll(gram[group * each : (group + 1) * each], group * lanes, 1)
    for copy in range(out_ref.shape[0]):
        out_ref[copy] = packed


def multiply(left, right):
    return [[tree_sum([a * right[k][j] for k, a in enumerate(row)]) for j in range(len(right[0]))] for row in left]


def small_inverse(matrix):
    size = len(matrix)
    if size == 1:
        return [[1.0 / matrix[0][0]]]
    half = size // 2
    corner = [row[half:] for row in matrix[:half]]
    rest = [row[half:] for row in matrix[half:]]
    first = small_inverse([row[:half] for row in matrix[:half]])
    across = multiply(first, corner)
    taken = multiply([list(row) for row in zip(*corner)], across)
    second = small_inverse([[rest[i][j] - taken[i][j] for j in range(half)] for i in range(half)])
    product = multiply(across, second)
    added = multiply(product, [list(row) for row in zip(*across)])
    top = [[first[i][j] + added[i][j] for j in range(half)] + [-value for value in product[i]] for i in range(half)]
    bottom = [[-product[j][i] for j in range(half)] + second[i] for i in range(half)]
    return top + bottom


def sweep(matrix, count):
    rows, width = matrix.shape
    size = next(size for size in (8, 4, 2, 1) if count % size == 0)
    tiles = [matrix[i : i + 8, :] for i in range(0, rows, 8)]
    across = lax.broadcasted_iota(jnp.int32, (8, width), 1)
    down = lax.broadcasted_iota(jnp.int32, (8, width), 0)

    def spread(value):
        return jnp.broadcast_to(value, (8, width))

    for k in range(0, count, size):
        at, inner = divmod(k, 8)
        columns = [[tile[:, k + i : k + i + 1] for tile in tiles] for i in range(size)]
        lines = [spread(tiles[at][inner + i : inner + i + 1, :]) for i in range(size)]
        full = [spread(columns[i][at]) for i in range(size)]
        pivots = [
            [spread(full[max(i, j)][inner + min(i, j) : inner + min(i, j) + 1, :]) for j in range(size)]
            for i in range(size)
        ]
        inverse = small_inverse(pivots)
        scaled = []
        for i in range(size):
            line = tree_sum([lines[j] * inverse[i][j] for j in range(size)])
            for j in range(size):
                line = jnp.where(across == k + j, inverse[i][j], line)
            scaled.append(line)
        inside = (across >= k) & (across < k + size)
        updated = []
        for n, tile in enumerate(tiles):
            value = jnp.where(inside, 0.0, tile)
            value = value - tree_sum([columns[i][n] * scaled[i] for i in range(size)])
            if n == at:
                for i in range(size):
                    value = jnp.where(down == inner + i, scaled[i], value)
            updated.append(value)
        tiles = updated
    return jnp.concatenate(tiles, axis=0)


def apply_tiles(tiles_ref, pick_ref, vectors, mask_ref):
    slots, per_row, size, _ = tiles_ref.shape
    mask = eye(size, size)
    images = []
    for slot in range(slots):
        picked = tree_sum(
            [pick_ref[e, slot * per_row : (slot + 1) * per_row, :] * vector for e, vector in enumerate(vectors)]
        )
        parts = [tiles_ref[slot, t] * picked[t : t + 1, :] for t in range(per_row)]
        column = jnp.sum(tree_sum(parts), axis=1, keepdims=True)
        images.append(to_row(column, mask) * mask_ref[slot : slot + 1, :])
    return images


def tail_with(old, entries):
    down = lax.broadcasted_iota(jnp.int32, (TAIL, old.shape[1]), 0)
    for row, value in entries:
        old = jnp.where(down == row, value, old)
    return old


def finish_step(tails, own_ref, images, tail_ref, out_ref):
    slots, rows, width = own_ref.shape
    last = STEPS
    total = jnp.zeros((rows + TAIL, width), F32)
    for slot in range(slots):
        tails[slot] = tail_with(tails[slot], [(last, images[slot])])
        total = total + jnp.concatenate([own_ref[slot], tails[slot]], axis=0) * images[slot]
    for block, tail in enumerate(tails):
        tail_ref[block] = tail
    partial = to_row(jnp.sum(total, axis=1, keepdims=True), eye(rows + TAIL, width))
    copies, lines, _ = out_ref.shape
    if lines == 1:
        message = partial
    else:
        pad = [jnp.zeros((lines - slots - 1, width), F32)] if lines > slots + 1 else []
        message = jnp.concatenate([*images, partial, *pad], axis=0)
    out_ref[...] = jnp.broadcast_to(message[None], (copies, lines, width))


def factor_body(
    count, rows, columns_ref, tiles_ref, parts_ref, inverse_ref, start_ref, pick_ref, here_ref, sem,
):
    move = pltpu.make_async_copy(tiles_ref, here_ref, sem)
    move.start()
    width = parts_ref.shape[2]
    slots, per_row = columns_ref.shape
    for slot in range(slots):
        names = columns_ref[slot : slot + 1, :].astype(F32)
        column = jnp.sum(jnp.where(eye(per_row, per_row), names, 0.0), axis=1, keepdims=True)
        column = jnp.broadcast_to(column, (per_row, width))
        for block in range(pick_ref.shape[0]):
            pick_ref[block, slot * per_row : (slot + 1) * per_row, :] = jnp.where(column == float(block), 1.0, 0.0)
    groups = lane_groups(count, rows, width)
    lanes = width // groups
    packed = tree_sum([parts_ref[i] for i in range(parts_ref.shape[0])])
    across = lax.broadcasted_iota(jnp.int32, (rows, width), 1)
    down = lax.broadcasted_iota(jnp.int32, (rows, width), 0)
    pieces = [packed]
    for group in range(1, groups):
        pieces.append(pltpu.roll(packed, width - group * lanes, 1))
    gram = jnp.where(across <= count, jnp.concatenate(pieces, axis=0), 0.0)
    swept = sweep(gram, count)
    keep = (down < count) & (across < count)
    inverse_ref[0:rows, :] = jnp.where(keep, swept, 0.0)
    tail_down = lax.broadcasted_iota(jnp.int32, (TAIL, width), 0)
    tail_across = lax.broadcasted_iota(jnp.int32, (TAIL, width), 1)
    inverse_ref[rows : rows + TAIL, :] = jnp.where(
        (tail_down < STEPS) & (tail_across == tail_down + rows), 1.0, 0.0
    )
    norm = jnp.sqrt(swept[count : count + 1, count : count + 1])
    start = jnp.where(down < count, -swept[:, count : count + 1], jnp.where(down == count, 1.0, 0.0))
    start_ref[0:rows, :] = start
    start_ref[rows : rows + TAIL, :] = jnp.broadcast_to(norm, (TAIL, width))
    move.wait()


def start_body(
    paired, ghosts_ref, start_ref, own_ref, one_ref, group_ref, two_ref, tiles_ref, pick_ref, mask_ref,
    out_ref, ghost_ref, tail_ref,
):
    slots, rows, width = own_ref.shape
    blocks = group_ref.shape[0]
    ghosts = ghosts_ref.shape[1]
    after = lax.axis_index("sub") % 2 * 2 if paired else 2
    coefficients = start_ref[0:rows, :] * (1.0 / start_ref[rows : rows + 1, :])
    vectors = []
    tails = []
    for block in range(slots + ghosts):
        if block < slots:
            held = own_ref[block]
        else:
            code = ghosts_ref[0, block - slots]
            offset = code // blocks
            place = code - offset * blocks
            held = jnp.where(
                offset == 1, group_ref[place], jnp.where(offset == after, two_ref[place], one_ref[place])
            )
            ghost_ref[block - slots] = held
        vector = jnp.sum(held * coefficients, axis=0, keepdims=True)
        vectors.append(vector)
        tails.append(tail_with(jnp.zeros((TAIL, width), F32), [(0, vector)]))
    images = apply_tiles(tiles_ref, pick_ref, vectors, mask_ref)
    finish_step(tails, own_ref, images, tail_ref, out_ref)


def project(total_row, inverse, rows, width):
    full = rows + TAIL
    down = lax.broadcasted_iota(jnp.int32, (full, width), 0)
    projected = jnp.sum(inverse * total_row, axis=1, keepdims=True)
    column = jnp.sum(jnp.where(eye(full, width), total_row, 0.0), axis=1, keepdims=True)
    projected = jnp.broadcast_to(projected, (full, width))
    squared = jnp.sum(
        jnp.where(down == rows + STEPS, column, -(column * projected)), axis=0, keepdims=True
    )
    return projected, jnp.sqrt(squared), down


def step_body(
    step, count, ghosts_ref, every_ref, own_ref, ghost_ref, old_ref, inverse_ref, tiles_ref, pick_ref, mask_ref,
    out_ref, tail_ref, history_ref,
):
    slots, rows, width = own_ref.shape
    ghosts = ghosts_ref.shape[1]
    subs = lax.axis_size("sub")
    span = subs * slots
    dom = lax.axis_index("dom")
    total_row = tree_sum([every_ref[i, slots : slots + 1, :] for i in range(every_ref.shape[0])])
    projected, norm, down = project(total_row, inverse_ref[...], rows, width)
    history_ref[...] = jnp.where(down == count, norm, projected)
    inverse_norm = 1.0 / norm
    coefficients = jnp.where(down == rows + STEPS, inverse_norm, -(projected * inverse_norm))
    vectors = []
    tails = []
    for block in range(slots + ghosts):
        old = old_ref[block]
        if block < slots:
            held = own_ref[block]
        else:
            held = ghost_ref[block - slots]
            code = ghosts_ref[0, block - slots]
            offset = code // span
            place = code - offset * span
            peer = place // slots
            device = (dom + offset - 1) * subs + peer
            image = every_ref[device, pl.ds(place - peer * slots, 1), :]
            old = tail_with(old, [(STEPS, image)])
        vector = jnp.sum(held * coefficients[0:rows], axis=0, keepdims=True)
        vector = vector + jnp.sum(old * coefficients[rows : rows + TAIL], axis=0, keepdims=True)
        vectors.append(vector)
        tails.append(tail_with(old, [(step, vector), (STEPS, 0.0)]))
    images = apply_tiles(tiles_ref, pick_ref, vectors, mask_ref)
    finish_step(tails, own_ref, images, tail_ref, out_ref)


def small_solve(matrix, target):
    size = len(target)
    low = [[None] * size for _ in range(size)]
    inverses = []
    for j in range(size):
        value = matrix[j][j]
        for k in range(j):
            value = value - low[j][k] * low[j][k]
        inverses.append(1.0 / jnp.sqrt(value))
        for i in range(j + 1, size):
            value = matrix[i][j]
            for k in range(j):
                value = value - low[i][k] * low[j][k]
            low[i][j] = value * inverses[j]
    forward = []
    for i in range(size):
        value = target[i]
        for k in range(i):
            value = value - low[i][k] * forward[k]
        forward.append(value * inverses[i])
    back = [None] * size
    for i in reversed(range(size)):
        value = forward[i]
        for k in range(i + 1, size):
            value = value - low[k][i] * back[k]
        back[i] = value * inverses[i]
    return back


def end_body(count, mask_ref, every_ref, own_ref, tail_ref, inverse_ref, start_ref, recycled_ref, *rest):
    histories, (solution_ref, residual_ref) = rest[:-2], rest[-2:]
    slots, rows, width = own_ref.shape
    full = rows + TAIL
    total_row = tree_sum([every_ref[i] for i in range(every_ref.shape[0])])
    projected, norm, down = project(total_row, inverse_ref[...], rows, width)
    columns = [history[...] for history in histories]
    columns.append(jnp.where(down == count, norm, projected))
    entries = []
    for j in range(STEPS):
        column = [columns[j][rows + i : rows + i + 1, :] for i in range(j + 1)]
        column.append(columns[j][count : count + 1, :])
        entries.append(column)
    normal = [[None] * STEPS for _ in range(STEPS)]
    for a in range(STEPS):
        for b in range(a + 1):
            shared = range(min(len(entries[a]), len(entries[b])))
            normal[a][b] = tree_sum([entries[a][r] * entries[b][r] for r in shared])
    initial = start_ref[rows : rows + 1, :]
    least = small_solve(normal, [initial * entries[j][0] for j in range(STEPS)])
    image = []
    for r in range(STEPS + 1):
        image.append(tree_sum([entries[j][r] * least[j] for j in range(STEPS) if r < len(entries[j])]))
    start = start_ref[0:rows, :]
    recycled_coefficients = start[0:count] * -1.0
    for j in range(STEPS):
        recycled_coefficients = recycled_coefficients - columns[j][0:count] * least[j]
    ratio = image[STEPS] / norm
    head = jnp.where(down[0:rows] < count, start + columns[-1][0:rows] * ratio, start)
    tail_down = down[0:TAIL]
    solution_tail = jnp.zeros((TAIL, width), F32)
    residual_tail = jnp.zeros((TAIL, width), F32)
    for j in range(STEPS):
        solution_tail = jnp.where(tail_down == j, least[j], solution_tail)
        residual_tail = jnp.where(tail_down == j, entries[-1][j] * ratio - image[j], residual_tail)
    residual_tail = jnp.where(tail_down == STEPS, -ratio, residual_tail)
    for slot in range(slots):
        tail = tail_ref[slot]
        mask = mask_ref[slot : slot + 1, :]
        point = jnp.sum(recycled_ref[:, slot, :] * mask * recycled_coefficients, axis=0, keepdims=True)
        point = point + jnp.sum(tail * solution_tail, axis=0, keepdims=True)
        solution_ref[slot : slot + 1, :] = point
        left = jnp.sum(own_ref[slot] * head, axis=0, keepdims=True)
        left = left + jnp.sum(tail * residual_tail, axis=0, keepdims=True)
        residual_ref[slot : slot + 1, :] = left


def local(load_vector, recycled, images, matrix_tiles, tile_columns, ghost_list, live_counts):
    slots, width = load_vector.shape
    count = recycled.shape[0]
    ghosts = ghost_list.shape[1]
    doms, subs = lax.axis_size("dom"), lax.axis_size("sub")
    devices = doms * subs
    rows = round_up(count + 1, ROW_ALIGN)
    full = rows + TAIL
    blocks = slots + ghosts
    per_row = tile_columns.shape[1]
    own, mask = call(
        pack_body,
        "pack",
        [(slots, rows, width), (round_up(slots, 8), width)],
        [SMEM, VMEM, VMEM],
    )(live_counts, load_vector, images)
    group = lax.all_gather(own, "sub", axis=0, tiled=True)
    each = rows // lane_groups(count, rows, width)
    (grams,) = call(functools.partial(gram_body, count), "gram", [(doms, each, width)], [VMEM])(group)
    parts = lax.all_to_all(grams, "dom", 0, 0)
    paired = subs % 2 == 0
    if paired:
        pairs = []
        for d in range(doms):
            for s in range(subs):
                to = d + 1 if s % 2 else d - 1
                if 0 <= to < doms:
                    pairs.append((d * subs + s, to * subs + s))
        one = lax.ppermute(group, AXES, pairs)
        one, parts = lax.optimization_barrier((one, parts))
        two = lax.ppermute(one, "sub", [(i, i ^ 1) for i in range(subs)])
    else:
        up = [(i, i + 1) for i in range(doms - 1)]
        one = lax.ppermute(group, "dom", up)
        two = lax.ppermute(group, "dom", [(j, i) for i, j in up])
    lines = round_up(slots + 1, 4)
    inverse, start, pick, tiles = call(
        functools.partial(factor_body, count, rows),
        "factor",
        [(full, width), (full, width), (blocks, slots * per_row, width), matrix_tiles.shape],
        [VMEM, HBM, VMEM],
        [pltpu.SemaphoreType.DMA],
    )(tile_columns, pltpu.with_memory_space_constraint(matrix_tiles, pltpu.HBM), parts)
    message, ghost_images, tails = call(
        functools.partial(start_body, paired),
        "start",
        [(devices, lines, width), (ghosts, rows, width), (blocks, TAIL, width)],
        [SMEM] + [VMEM] * 8,
    )(ghost_list, start, own, one, group, two, tiles, pick, mask)
    histories = []
    for step in range(1, STEPS):
        every = lax.all_to_all(message, AXES, 0, 0)
        sent = lines if step < STEPS - 1 else 1
        message, tails, history = call(
            functools.partial(step_body, step, count),
            f"step{step}",
            [(devices, sent, width), (blocks, TAIL, width), (full, width)],
            [SMEM] + [VMEM] * 8,
        )(ghost_list, every, own, ghost_images, tails, inverse, tiles, pick, mask)
        histories.append(history)
    every = lax.all_to_all(message, AXES, 0, 0)
    return tuple(
        call(
            functools.partial(end_body, count),
            "end",
            [(slots, width), (slots, width)],
            [VMEM] * (7 + len(histories)),
        )(mask, every, own, tails, inverse, start, recycled, *histories)
    )


def solution(mesh):
    return jax.shard_map(
        local,
        mesh=mesh,
        in_specs=(
            P(("dom", "sub"), None),
            P(None, ("dom", "sub"), None),
            P(None, ("dom", "sub"), None),
            P(("dom", "sub"), None, None, None),
            P(("dom", "sub"), None),
            P(("dom", "sub"), None),
            P(("dom", "sub")),
        ),
        out_specs=(P(("dom", "sub"), None), P(("dom", "sub"), None)),
        check_vma=False,
    )
```

```python
import functools

import jax
import jax.numpy as jnp
from jax import lax
from jax.experimental import pallas as pl
from jax.experimental.pallas import tpu as pltpu
from jax.sharding import PartitionSpec as P

STEPS = 3
TAIL = 8
ROW_ALIGN = 8
AXES = ("dom", "sub")
VMEM = pl.BlockSpec(memory_space=pltpu.VMEM)
SMEM = pl.BlockSpec(memory_space=pltpu.SMEM)
HBM = pl.BlockSpec(memory_space=pltpu.HBM)
F32 = jnp.float32


def call(body, name, outs, specs, scratch=(), work=10_000_000):
    return pl.pallas_call(
        body,
        name=name,
        out_shape=[jax.ShapeDtypeStruct(shape, F32) for shape in outs],
        in_specs=specs,
        out_specs=[VMEM] * len(outs),
        scratch_shapes=list(scratch),
        cost_estimate=pl.CostEstimate(flops=work, bytes_accessed=1 << 20, transcendentals=0),
        compiler_params=pltpu.CompilerParams(vmem_limit_bytes=16 * 1024 * 1024),
    )


def round_up(value, step):
    return -(-value // step) * step


def eye(rows, lanes):
    down = lax.broadcasted_iota(jnp.int32, (rows, lanes), 0)
    across = lax.broadcasted_iota(jnp.int32, (rows, lanes), 1)
    return down == across


def to_row(column, mask):
    return jnp.sum(jnp.where(mask, column, 0.0), axis=0, keepdims=True)


def tree_sum(parts):
    while len(parts) > 1:
        pairs = [parts[i] + parts[i + 1] for i in range(0, len(parts) - 1, 2)]
        parts = pairs + parts[len(parts) - len(parts) % 2 :]
    return parts[0]


def pack_body(live_ref, load_ref, images_ref, own_ref, mask_ref):
    count, slots, width = images_ref.shape
    rows = own_ref.shape[1]
    line = lax.broadcasted_iota(jnp.int32, mask_ref.shape, 0)
    mask_ref[...] = jnp.where(line < live_ref[0], 1.0, 0.0).astype(F32)
    for slot in range(slots):
        mask = jnp.where(slot < live_ref[0], 1.0, 0.0).astype(F32)
        own_ref[slot, 0:count, :] = images_ref[:, slot, :] * mask
        own_ref[slot, count : count + 1, :] = load_ref[slot : slot + 1, :] * mask
        own_ref[slot, count + 1 : rows, :] = jnp.zeros((rows - count - 1, width), F32)


def lane_groups(count, rows, width):
    groups = width // (count + 1)
    if rows % groups == 0 and (rows // groups) % ROW_ALIGN == 0:
        return groups
    return 1


def gram_body(count, group_ref, out_ref):
    blocks, rows, width = group_ref.shape
    products = []
    for block in range(blocks):
        part = group_ref[block]
        products.append(
            lax.dot_general(
                part, part, (((1,), (1,)), ((), ())),
                precision=lax.Precision.HIGHEST, preferred_element_type=F32,
            )
        )
    gram = jnp.concatenate([tree_sum(products), jnp.zeros((rows, width - rows), F32)], axis=1)
    groups = lane_groups(count, rows, width)
    each, lanes = rows // groups, width // groups
    packed = gram[0:each]
    for group in range(1, groups):
        packed = packed + pltpu.roll(gram[group * each : (group + 1) * each], group * lanes, 1)
    for copy in range(out_ref.shape[0]):
        out_ref[copy] = packed


def multiply(left, right):
    return [[tree_sum([a * right[k][j] for k, a in enumerate(row)]) for j in range(len(right[0]))] for row in left]


def small_inverse(matrix):
    size = len(matrix)
    if size == 1:
        return [[1.0 / matrix[0][0]]]
    half = size // 2
    corner = [row[half:] for row in matrix[:half]]
    rest = [row[half:] for row in matrix[half:]]
    first = small_inverse([row[:half] for row in matrix[:half]])
    across = multiply(first, corner)
    taken = multiply([list(row) for row in zip(*corner)], across)
    second = small_inverse([[rest[i][j] - taken[i][j] for j in range(half)] for i in range(half)])
    product = multiply(across, second)
    added = multiply(product, [list(row) for row in zip(*across)])
    top = [[first[i][j] + added[i][j] for j in range(half)] + [-value for value in product[i]] for i in range(half)]
    bottom = [[-product[j][i] for j in range(half)] + second[i] for i in range(half)]
    return top + bottom


def sweep(matrix, count):
    rows, width = matrix.shape
    size = next(size for size in (8, 4, 2, 1) if count % size == 0)
    tiles = [matrix[i : i + 8, :] for i in range(0, rows, 8)]
    across = lax.broadcasted_iota(jnp.int32, (8, width), 1)
    down = lax.broadcasted_iota(jnp.int32, (8, width), 0)

    def spread(value):
        return jnp.broadcast_to(value, (8, width))

    for k in range(0, count, size):
        at, inner = divmod(k, 8)
        columns = [[tile[:, k + i : k + i + 1] for tile in tiles] for i in range(size)]
        lines = [spread(tiles[at][inner + i : inner + i + 1, :]) for i in range(size)]
        full = [spread(columns[i][at]) for i in range(size)]
        pivots = [
            [spread(full[max(i, j)][inner + min(i, j) : inner + min(i, j) + 1, :]) for j in range(size)]
            for i in range(size)
        ]
        inverse = small_inverse(pivots)
        scaled = []
        for i in range(size):
            line = tree_sum([lines[j] * inverse[i][j] for j in range(size)])
            for j in range(size):
                line = jnp.where(across == k + j, inverse[i][j], line)
            scaled.append(line)
        inside = (across >= k) & (across < k + size)
        updated = []
        for n, tile in enumerate(tiles):
            value = jnp.where(inside, 0.0, tile)
            value = value - tree_sum([columns[i][n] * scaled[i] for i in range(size)])
            if n == at:
                for i in range(size):
                    value = jnp.where(down == inner + i, scaled[i], value)
            updated.append(value)
        tiles = updated
    return jnp.concatenate(tiles, axis=0)


def apply_tiles(tiles_ref, pick_ref, vectors, mask_ref):
    slots, per_row, size, _ = tiles_ref.shape
    mask = eye(size, size)
    images = []
    for slot in range(slots):
        picked = tree_sum(
            [pick_ref[e, slot * per_row : (slot + 1) * per_row, :] * vector for e, vector in enumerate(vectors)]
        )
        parts = [tiles_ref[slot, t] * picked[t : t + 1, :] for t in range(per_row)]
        column = jnp.sum(tree_sum(parts), axis=1, keepdims=True)
        images.append(to_row(column, mask) * mask_ref[slot : slot + 1, :])
    return images


def tail_with(old, row, value):
    down = lax.broadcasted_iota(jnp.int32, (TAIL, old.shape[1]), 0)
    return jnp.where(down == row, value, old)


def finish_step(vectors, tails, own_ref, tiles_ref, pick_ref, mask_ref, own_tail_ref, out_ref):
    slots, rows, width = own_ref.shape
    images = apply_tiles(tiles_ref, pick_ref, vectors, mask_ref)
    total = jnp.zeros((rows + TAIL, width), F32)
    for slot in range(slots):
        tail = tail_with(tails[slot], STEPS, images[slot])
        own_tail_ref[slot] = tail
        total = total + jnp.concatenate([own_ref[slot], tail], axis=0) * images[slot]
    partial = to_row(jnp.sum(total, axis=1, keepdims=True), eye(rows + TAIL, width))
    copies, lines, _ = out_ref.shape
    if lines == 1:
        message = partial
    else:
        pad = [jnp.zeros((lines - slots - 1, width), F32)] if lines > slots + 1 else []
        message = jnp.concatenate([*images, partial, *pad], axis=0)
    out_ref[...] = jnp.broadcast_to(message[None], (copies, lines, width))


def factor_body(
    count, rows, paired, columns_ref, ghosts_ref, tiles_ref, parts_ref, inverse_ref, start_ref, pick_ref, here_ref, sem
):
    move = pltpu.make_async_copy(tiles_ref, here_ref, sem)
    move.start()
    width = parts_ref.shape[2]
    slots, per_row = columns_ref.shape
    blocks = (pick_ref.shape[0] - slots) // 3
    codes = ghosts_ref[...].astype(F32)
    if paired:
        flipped = jnp.where(codes < blocks, codes + 2 * blocks, jnp.where(codes < 2 * blocks, codes, codes - 2 * blocks))
        codes = jnp.where(lax.axis_index("sub") % 2 == 0, flipped, codes)
    for slot in range(slots):
        names = columns_ref[slot : slot + 1, :].astype(F32)
        places = names + 3 * blocks
        for ghost in range(codes.shape[1]):
            places = jnp.where(names == slots + ghost, codes[:, ghost : ghost + 1], places)
        column = jnp.sum(jnp.where(eye(per_row, per_row), places, 0.0), axis=1, keepdims=True)
        column = jnp.broadcast_to(column, (per_row, width))
        for place in range(pick_ref.shape[0]):
            pick_ref[place, slot * per_row : (slot + 1) * per_row, :] = jnp.where(column == place, 1.0, 0.0)
    groups = lane_groups(count, rows, width)
    lanes = width // groups
    packed = tree_sum([parts_ref[i] for i in range(parts_ref.shape[0])])
    across = lax.broadcasted_iota(jnp.int32, (rows, width), 1)
    down = lax.broadcasted_iota(jnp.int32, (rows, width), 0)
    pieces = [packed]
    for group in range(1, groups):
        pieces.append(pltpu.roll(packed, width - group * lanes, 1))
    gram = jnp.where(across <= count, jnp.concatenate(pieces, axis=0), 0.0)
    swept = sweep(gram, count)
    keep = (down < count) & (across < count)
    inverse_ref[0:rows, :] = jnp.where(keep, swept, 0.0)
    tail_down = lax.broadcasted_iota(jnp.int32, (TAIL, width), 0)
    tail_across = lax.broadcasted_iota(jnp.int32, (TAIL, width), 1)
    inverse_ref[rows : rows + TAIL, :] = jnp.where(
        (tail_down < STEPS) & (tail_across == tail_down + rows), 1.0, 0.0
    )
    squared = jnp.broadcast_to(swept[count : count + 1, count : count + 1], (TAIL, width))
    inverse_norm = lax.rsqrt(squared)
    start = jnp.where(down < count, -swept[:, count : count + 1], jnp.where(down == count, 1.0, 0.0))
    start_ref[0:rows, :] = start
    start_ref[rows : rows + TAIL, :] = jnp.where(tail_down == 0, squared * inverse_norm, inverse_norm)
    move.wait()


def start_body(
    start_ref, own_ref, one_ref, group_ref, two_ref, tiles_ref, pick_ref, mask_ref, out_ref, tail_ref, own_tail_ref
):
    slots, rows, width = own_ref.shape
    blocks = group_ref.shape[0]
    coefficients = start_ref[0:rows, :] * start_ref[rows + 1 : rows + 2, :]
    empty = jnp.zeros((TAIL, width), F32)
    vectors = []
    tails = []
    for part in (one_ref, group_ref, two_ref, own_ref):
        for place in range(part.shape[0]):
            vector = jnp.sum(part[place] * coefficients, axis=0, keepdims=True)
            tail = tail_with(empty, 0, vector)
            if len(vectors) < 3 * blocks:
                tail_ref[len(vectors)] = tail
            else:
                tails.append(tail)
            vectors.append(vector)
    finish_step(vectors, tails, own_ref, tiles_ref, pick_ref, mask_ref, own_tail_ref, out_ref)


def project(total_row, inverse, rows, width):
    full = rows + TAIL
    down = lax.broadcasted_iota(jnp.int32, (full, width), 0)
    projected = jnp.sum(inverse * total_row, axis=1, keepdims=True)
    column = jnp.sum(jnp.where(eye(full, width), total_row, 0.0), axis=1, keepdims=True)
    projected = jnp.broadcast_to(projected, (full, width))
    squared = jnp.sum(
        jnp.where(down == rows + STEPS, column, -(column * projected)), axis=0, keepdims=True
    )
    inverse_norm = lax.rsqrt(squared)
    return projected, squared * inverse_norm, inverse_norm, down


def step_body(
    step, count, paired, every_ref, own_ref, one_ref, group_ref, two_ref, old_ref, old_own_ref, inverse_ref,
    tiles_ref, pick_ref, mask_ref, out_ref, tail_ref, own_tail_ref, history_ref,
):
    slots, rows, width = own_ref.shape
    subs = lax.axis_size("sub")
    dom = lax.axis_index("dom")
    toward = lax.axis_index("sub") % 2 * 2 - 1 if paired else 1
    total_row = tree_sum([every_ref[i, slots : slots + 1, :] for i in range(every_ref.shape[0])])
    projected, norm, inverse_norm, down = project(total_row, inverse_ref[...], rows, width)
    history_ref[...] = jnp.where(down == count, norm, projected)
    coefficients = jnp.where(down == rows + STEPS, inverse_norm, -(projected * inverse_norm))
    head, foot = coefficients[0:rows], coefficients[rows : rows + TAIL]
    vectors = []
    for part, shift in ((one_ref, -toward), (group_ref, 0), (two_ref, toward)):
        first = jnp.clip(dom + shift, 0, lax.axis_size("dom") - 1) * subs
        for place in range(part.shape[0]):
            at = len(vectors)
            old = old_ref[at]
            image = every_ref[first + place // slots, place % slots : place % slots + 1, :]
            vector = jnp.sum(part[place] * head, axis=0, keepdims=True)
            vector = vector + jnp.sum(old * foot, axis=0, keepdims=True) + image * inverse_norm
            if tail_ref is not None:
                tail_ref[at] = tail_with(old, step, vector)
            vectors.append(vector)
    tails = []
    for slot in range(slots):
        old = old_own_ref[slot]
        vector = jnp.sum(own_ref[slot] * head, axis=0, keepdims=True)
        vector = vector + jnp.sum(old * foot, axis=0, keepdims=True)
        tails.append(tail_with(old, step, vector))
        vectors.append(vector)
    finish_step(vectors, tails, own_ref, tiles_ref, pick_ref, mask_ref, own_tail_ref, out_ref)


def last_step_body(step, count, paired, *refs):
    step_body(step, count, paired, *refs[:12], None, *refs[12:])


def small_solve(matrix, target):
    size = len(target)
    low = [[None] * size for _ in range(size)]
    inverses = []
    for j in range(size):
        value = matrix[j][j]
        for k in range(j):
            value = value - low[j][k] * low[j][k]
        inverses.append(1.0 / jnp.sqrt(value))
        for i in range(j + 1, size):
            value = matrix[i][j]
            for k in range(j):
                value = value - low[i][k] * low[j][k]
            low[i][j] = value * inverses[j]
    forward = []
    for i in range(size):
        value = target[i]
        for k in range(i):
            value = value - low[i][k] * forward[k]
        forward.append(value * inverses[i])
    back = [None] * size
    for i in reversed(range(size)):
        value = forward[i]
        for k in range(i + 1, size):
            value = value - low[k][i] * back[k]
        back[i] = value * inverses[i]
    return back


def end_body(count, mask_ref, every_ref, own_ref, tail_ref, inverse_ref, start_ref, recycled_ref, *rest):
    histories, (solution_ref, residual_ref) = rest[:-2], rest[-2:]
    slots, rows, width = own_ref.shape
    full = rows + TAIL
    total_row = tree_sum([every_ref[i] for i in range(every_ref.shape[0])])
    projected, norm, _, down = project(total_row, inverse_ref[...], rows, width)
    columns = [history[...] for history in histories]
    columns.append(jnp.where(down == count, norm, projected))
    entries = []
    for j in range(STEPS):
        column = [columns[j][rows + i : rows + i + 1, :] for i in range(j + 1)]
        column.append(columns[j][count : count + 1, :])
        entries.append(column)
    normal = [[None] * STEPS for _ in range(STEPS)]
    for a in range(STEPS):
        for b in range(a + 1):
            shared = range(min(len(entries[a]), len(entries[b])))
            normal[a][b] = tree_sum([entries[a][r] * entries[b][r] for r in shared])
    initial = start_ref[rows : rows + 1, :]
    least = small_solve(normal, [initial * entries[j][0] for j in range(STEPS)])
    image = []
    for r in range(STEPS + 1):
        image.append(tree_sum([entries[j][r] * least[j] for j in range(STEPS) if r < len(entries[j])]))
    start = start_ref[0:rows, :]
    recycled_coefficients = start[0:count] * -1.0
    for j in range(STEPS):
        recycled_coefficients = recycled_coefficients - columns[j][0:count] * least[j]
    ratio = image[STEPS] / norm
    head = jnp.where(down[0:rows] < count, start + columns[-1][0:rows] * ratio, start)
    tail_down = down[0:TAIL]
    solution_tail = jnp.zeros((TAIL, width), F32)
    residual_tail = jnp.zeros((TAIL, width), F32)
    for j in range(STEPS):
        solution_tail = jnp.where(tail_down == j, least[j], solution_tail)
        residual_tail = jnp.where(tail_down == j, entries[-1][j] * ratio - image[j], residual_tail)
    residual_tail = jnp.where(tail_down == STEPS, -ratio, residual_tail)
    for slot in range(slots):
        tail = tail_ref[slot]
        mask = mask_ref[slot : slot + 1, :]
        point = jnp.sum(recycled_ref[:, slot, :] * mask * recycled_coefficients, axis=0, keepdims=True)
        point = point + jnp.sum(tail * solution_tail, axis=0, keepdims=True)
        solution_ref[slot : slot + 1, :] = point
        left = jnp.sum(own_ref[slot] * head, axis=0, keepdims=True)
        left = left + jnp.sum(tail * residual_tail, axis=0, keepdims=True)
        residual_ref[slot : slot + 1, :] = left


def local(load_vector, recycled, images, matrix_tiles, tile_columns, ghost_list, live_counts):
    slots, width = load_vector.shape
    count = recycled.shape[0]
    doms, subs = lax.axis_size("dom"), lax.axis_size("sub")
    devices = doms * subs
    rows = round_up(count + 1, ROW_ALIGN)
    full = rows + TAIL
    per_row = tile_columns.shape[1]
    own, mask = call(
        pack_body,
        "pack",
        [(slots, rows, width), (round_up(slots, 8), width)],
        [SMEM, VMEM, VMEM],
    )(live_counts, load_vector, images)
    group = lax.all_gather(own, "sub", axis=0, tiled=True)
    each = rows // lane_groups(count, rows, width)
    (grams,) = call(functools.partial(gram_body, count), "gram", [(doms, each, width)], [VMEM])(group)
    parts = lax.all_to_all(grams, "dom", 0, 0)
    paired = subs % 2 == 0
    if paired:
        pairs = []
        for d in range(doms):
            for s in range(subs):
                to = d + 1 if s % 2 else d - 1
                if 0 <= to < doms:
                    pairs.append((d * subs + s, to * subs + s))
        one = lax.ppermute(group, AXES, pairs)
        one, parts = lax.optimization_barrier((one, parts))
        two = lax.ppermute(one, "sub", [(i, i ^ 1) for i in range(subs)])
    else:
        up = [(i, i + 1) for i in range(doms - 1)]
        one = lax.ppermute(group, "dom", up)
        two = lax.ppermute(group, "dom", [(j, i) for i, j in up])
    lines = round_up(slots + 1, 4)
    near = 3 * group.shape[0]
    inverse, start, pick, tiles = call(
        functools.partial(factor_body, count, rows, paired),
        "factor",
        [(full, width), (full, width), (near + slots, slots * per_row, width), matrix_tiles.shape],
        [VMEM, VMEM, HBM, VMEM],
        [pltpu.SemaphoreType.DMA],
    )(tile_columns, ghost_list, pltpu.with_memory_space_constraint(matrix_tiles, pltpu.HBM), parts)
    message, tails, own_tails = call(
        start_body,
        "start",
        [(devices, lines, width), (near, TAIL, width), (slots, TAIL, width)],
        [VMEM] * 8,
    )(start, own, one, group, two, tiles, pick, mask)
    histories = []
    for step in range(1, STEPS):
        every = lax.all_to_all(message, AXES, 0, 0)
        last = step == STEPS - 1
        sent = 1 if last else lines
        results = call(
            functools.partial(last_step_body if last else step_body, step, count, paired),
            f"step{step}",
            [(devices, sent, width)]
            + ([] if last else [(near, TAIL, width)])
            + [(slots, TAIL, width), (full, width)],
            [VMEM] * 11,
        )(every, own, one, group, two, tails, own_tails, inverse, tiles, pick, mask)
        message, own_tails, history = results[0], results[-2], results[-1]
        tails = tails if last else results[1]
        histories.append(history)
    every = lax.all_to_all(message, AXES, 0, 0)
    return tuple(
        call(
            functools.partial(end_body, count),
            "end",
            [(slots, width), (slots, width)],
            [VMEM] * (7 + len(histories)),
        )(mask, every, own, own_tails, inverse, start, recycled, *histories)
    )


def solution(mesh):
    return jax.shard_map(
        local,
        mesh=mesh,
        in_specs=(
            P(("dom", "sub"), None),
            P(None, ("dom", "sub"), None),
            P(None, ("dom", "sub"), None),
            P(("dom", "sub"), None, None, None),
            P(("dom", "sub"), None),
            P(("dom", "sub"), None),
            P(("dom", "sub")),
        ),
        out_specs=(P(("dom", "sub"), None), P(("dom", "sub"), None)),
        check_vma=False,
    )
```

```python
import functools

import jax
import jax.numpy as jnp
from jax import lax
from jax.experimental import pallas as pl
from jax.experimental.pallas import tpu as pltpu
from jax.sharding import PartitionSpec as P

STEPS = 3
TAIL = 8
ROW_ALIGN = 8
AXES = ("dom", "sub")
VMEM = pl.BlockSpec(memory_space=pltpu.VMEM)
SMEM = pl.BlockSpec(memory_space=pltpu.SMEM)
HBM = pl.BlockSpec(memory_space=pltpu.HBM)
F32 = jnp.float32


def call(body, name, outs, specs, scratch=(), work=10_000_000):
    return pl.pallas_call(
        body,
        name=name,
        out_shape=[jax.ShapeDtypeStruct(shape, F32) for shape in outs],
        in_specs=specs,
        out_specs=[VMEM] * len(outs),
        scratch_shapes=list(scratch),
        cost_estimate=pl.CostEstimate(flops=work, bytes_accessed=1 << 20, transcendentals=0),
        compiler_params=pltpu.CompilerParams(vmem_limit_bytes=16 * 1024 * 1024),
    )


def round_up(value, step):
    return -(-value // step) * step


def eye(rows, lanes):
    down = lax.broadcasted_iota(jnp.int32, (rows, lanes), 0)
    across = lax.broadcasted_iota(jnp.int32, (rows, lanes), 1)
    return down == across


def to_row(column, mask):
    return jnp.sum(jnp.where(mask, column, 0.0), axis=0, keepdims=True)


def tree_sum(parts):
    while len(parts) > 1:
        pairs = [parts[i] + parts[i + 1] for i in range(0, len(parts) - 1, 2)]
        parts = pairs + parts[len(parts) - len(parts) % 2 :]
    return parts[0]


def pack_body(live_ref, load_ref, images_ref, own_ref, mask_ref):
    count, slots, width = images_ref.shape
    rows = own_ref.shape[1]
    line = lax.broadcasted_iota(jnp.int32, mask_ref.shape, 0)
    mask_ref[...] = jnp.where(line < live_ref[0], 1.0, 0.0).astype(F32)
    for slot in range(slots):
        mask = jnp.where(slot < live_ref[0], 1.0, 0.0).astype(F32)
        own_ref[slot, 0:count, :] = images_ref[:, slot, :] * mask
        own_ref[slot, count : count + 1, :] = load_ref[slot : slot + 1, :] * mask
        own_ref[slot, count + 1 : rows, :] = jnp.zeros((rows - count - 1, width), F32)


def lane_groups(count, rows, width):
    groups = width // (count + 1)
    if rows % groups == 0 and (rows // groups) % ROW_ALIGN == 0:
        return groups
    return 1


def gram_body(count, group_ref, out_ref):
    blocks, rows, width = group_ref.shape
    products = []
    for block in range(blocks):
        part = group_ref[block]
        products.append(
            lax.dot_general(
                part, part, (((1,), (1,)), ((), ())),
                precision=lax.Precision.HIGHEST, preferred_element_type=F32,
            )
        )
    gram = jnp.concatenate([tree_sum(products), jnp.zeros((rows, width - rows), F32)], axis=1)
    groups = lane_groups(count, rows, width)
    each, lanes = rows // groups, width // groups
    packed = gram[0:each]
    for group in range(1, groups):
        packed = packed + pltpu.roll(gram[group * each : (group + 1) * each], group * lanes, 1)
    for copy in range(out_ref.shape[0]):
        out_ref[copy] = packed


def multiply(left, right):
    return [[tree_sum([a * right[k][j] for k, a in enumerate(row)]) for j in range(len(right[0]))] for row in left]


def small_inverse(matrix):
    size = len(matrix)
    if size == 1:
        return [[1.0 / matrix[0][0]]]
    half = size // 2
    corner = [row[half:] for row in matrix[:half]]
    rest = [row[half:] for row in matrix[half:]]
    first = small_inverse([row[:half] for row in matrix[:half]])
    across = multiply(first, corner)
    taken = multiply([list(row) for row in zip(*corner)], across)
    second = small_inverse([[rest[i][j] - taken[i][j] for j in range(half)] for i in range(half)])
    product = multiply(across, second)
    added = multiply(product, [list(row) for row in zip(*across)])
    top = [[first[i][j] + added[i][j] for j in range(half)] + [-value for value in product[i]] for i in range(half)]
    bottom = [[-product[j][i] for j in range(half)] + second[i] for i in range(half)]
    return top + bottom


def sweep(matrix, count):
    rows, width = matrix.shape
    size = next(size for size in (8, 4, 2, 1) if count % size == 0)
    tiles = [matrix[i : i + 8, :] for i in range(0, rows, 8)]
    across = lax.broadcasted_iota(jnp.int32, (8, width), 1)
    down = lax.broadcasted_iota(jnp.int32, (8, width), 0)

    def spread(value):
        return jnp.broadcast_to(value, (8, width))

    for k in range(0, count, size):
        at, inner = divmod(k, 8)
        columns = [[tile[:, k + i : k + i + 1] for tile in tiles] for i in range(size)]
        lines = [spread(tiles[at][inner + i : inner + i + 1, :]) for i in range(size)]
        full = [spread(columns[i][at]) for i in range(size)]
        pivots = [
            [spread(full[max(i, j)][inner + min(i, j) : inner + min(i, j) + 1, :]) for j in range(size)]
            for i in range(size)
        ]
        inverse = small_inverse(pivots)
        scaled = []
        for i in range(size):
            line = tree_sum([lines[j] * inverse[i][j] for j in range(size)])
            for j in range(size):
                line = jnp.where(across == k + j, inverse[i][j], line)
            scaled.append(line)
        inside = (across >= k) & (across < k + size)
        updated = []
        for n, tile in enumerate(tiles):
            value = jnp.where(inside, 0.0, tile)
            value = value - tree_sum([columns[i][n] * scaled[i] for i in range(size)])
            if n == at:
                for i in range(size):
                    value = jnp.where(down == inner + i, scaled[i], value)
            updated.append(value)
        tiles = updated
    return jnp.concatenate(tiles, axis=0)


def apply_tiles(tiles_ref, pick_ref, vectors, mask_ref):
    slots, per_row, size, _ = tiles_ref.shape
    mask = eye(size, size)
    images = []
    for slot in range(slots):
        picked = tree_sum(
            [pick_ref[e, slot * per_row : (slot + 1) * per_row, :] * vector for e, vector in enumerate(vectors)]
        )
        parts = [tiles_ref[slot, t] * picked[t : t + 1, :] for t in range(per_row)]
        column = jnp.sum(tree_sum(parts), axis=1, keepdims=True)
        images.append(to_row(column, mask) * mask_ref[slot : slot + 1, :])
    return images


def tail_with(old, row, value):
    down = lax.broadcasted_iota(jnp.int32, (TAIL, old.shape[1]), 0)
    return jnp.where(down == row, value, old)


def finish_step(vectors, tails, own_ref, tiles_ref, pick_ref, mask_ref, own_tail_ref, out_ref):
    slots, rows, width = own_ref.shape
    images = apply_tiles(tiles_ref, pick_ref, vectors, mask_ref)
    total = jnp.zeros((rows + TAIL, width), F32)
    for slot in range(slots):
        tail = tail_with(tails[slot], STEPS, images[slot])
        own_tail_ref[slot] = tail
        total = total + jnp.concatenate([own_ref[slot], tail], axis=0) * images[slot]
    partial = to_row(jnp.sum(total, axis=1, keepdims=True), eye(rows + TAIL, width))
    copies, lines, _ = out_ref.shape
    if lines == 1:
        message = partial
    else:
        pad = [jnp.zeros((lines - slots - 1, width), F32)] if lines > slots + 1 else []
        message = jnp.concatenate([*images, partial, *pad], axis=0)
    out_ref[...] = jnp.broadcast_to(message[None], (copies, lines, width))


def factor_body(
    count, rows, paired, columns_ref, ghosts_ref, tiles_ref, parts_ref, inverse_ref, start_ref, pick_ref, here_ref, sem
):
    move = pltpu.make_async_copy(tiles_ref, here_ref, sem)
    move.start()
    width = parts_ref.shape[2]
    groups = lane_groups(count, rows, width)
    lanes = width // groups
    packed = lax.fori_loop(1, parts_ref.shape[0], lambda i, held: held + parts_ref[i], parts_ref[0])
    across = lax.broadcasted_iota(jnp.int32, (rows, width), 1)
    down = lax.broadcasted_iota(jnp.int32, (rows, width), 0)
    pieces = [packed]
    for group in range(1, groups):
        pieces.append(pltpu.roll(packed, width - group * lanes, 1))
    gram = jnp.where(across <= count, jnp.concatenate(pieces, axis=0), 0.0)
    swept = sweep(gram, count)
    keep = (down < count) & (across < count)
    inverse_ref[0:rows, :] = jnp.where(keep, swept, 0.0)
    tail_down = lax.broadcasted_iota(jnp.int32, (TAIL, width), 0)
    tail_across = lax.broadcasted_iota(jnp.int32, (TAIL, width), 1)
    inverse_ref[rows : rows + TAIL, :] = jnp.where(
        (tail_down < STEPS) & (tail_across == tail_down + rows), 1.0, 0.0
    )
    squared = jnp.broadcast_to(swept[count : count + 1, count : count + 1], (TAIL, width))
    inverse_norm = lax.rsqrt(squared)
    start = jnp.where(down < count, -swept[:, count : count + 1], jnp.where(down == count, 1.0, 0.0))
    start_ref[0:rows, :] = start
    start_ref[rows : rows + TAIL, :] = jnp.where(tail_down == 0, squared * inverse_norm, inverse_norm)
    slots, per_row = columns_ref.shape
    blocks = (pick_ref.shape[0] - slots) // 3
    codes = ghosts_ref[...].astype(F32)
    if paired:
        flipped = jnp.where(codes < blocks, codes + 2 * blocks, jnp.where(codes < 2 * blocks, codes, codes - 2 * blocks))
        codes = jnp.where(lax.axis_index("sub") % 2 == 0, flipped, codes)
    for slot in range(slots):
        names = columns_ref[slot : slot + 1, :].astype(F32)
        places = names + 3 * blocks
        for ghost in range(codes.shape[1]):
            places = jnp.where(names == slots + ghost, codes[:, ghost : ghost + 1], places)
        column = jnp.sum(jnp.where(eye(per_row, per_row), places, 0.0), axis=1, keepdims=True)
        column = jnp.broadcast_to(column, (per_row, width))
        for place in range(pick_ref.shape[0]):
            pick_ref[place, slot * per_row : (slot + 1) * per_row, :] = jnp.where(column == place, 1.0, 0.0)
    move.wait()


def start_body(
    start_ref, own_ref, one_ref, group_ref, two_ref, tiles_ref, pick_ref, mask_ref, out_ref, tail_ref, own_tail_ref
):
    slots, rows, width = own_ref.shape
    blocks = group_ref.shape[0]
    coefficients = start_ref[0:rows, :] * start_ref[rows + 1 : rows + 2, :]
    empty = jnp.zeros((TAIL, width), F32)
    vectors = []
    tails = []
    for part in (one_ref, group_ref, two_ref, own_ref):
        for place in range(part.shape[0]):
            vector = jnp.sum(part[place] * coefficients, axis=0, keepdims=True)
            tail = tail_with(empty, 0, vector)
            if len(vectors) < 3 * blocks:
                tail_ref[len(vectors)] = tail
            else:
                tails.append(tail)
            vectors.append(vector)
    finish_step(vectors, tails, own_ref, tiles_ref, pick_ref, mask_ref, own_tail_ref, out_ref)


def project(total_row, inverse, rows, width):
    full = rows + TAIL
    down = lax.broadcasted_iota(jnp.int32, (full, width), 0)
    projected = jnp.sum(inverse * total_row, axis=1, keepdims=True)
    column = jnp.sum(jnp.where(eye(full, width), total_row, 0.0), axis=1, keepdims=True)
    projected = jnp.broadcast_to(projected, (full, width))
    squared = jnp.sum(
        jnp.where(down == rows + STEPS, column, -(column * projected)), axis=0, keepdims=True
    )
    inverse_norm = lax.rsqrt(squared)
    return projected, squared * inverse_norm, inverse_norm, down


def step_body(
    step, count, paired, every_ref, own_ref, one_ref, group_ref, two_ref, old_ref, old_own_ref, inverse_ref,
    tiles_ref, pick_ref, mask_ref, out_ref, tail_ref, own_tail_ref, history_ref,
):
    slots, rows, width = own_ref.shape
    subs = lax.axis_size("sub")
    dom = lax.axis_index("dom")
    toward = lax.axis_index("sub") % 2 * 2 - 1 if paired else 1
    total_row = tree_sum([every_ref[i, slots : slots + 1, :] for i in range(every_ref.shape[0])])
    projected, norm, inverse_norm, down = project(total_row, inverse_ref[...], rows, width)
    history_ref[...] = jnp.where(down == count, norm, projected)
    coefficients = jnp.where(down == rows + STEPS, inverse_norm, -(projected * inverse_norm))
    head, foot = coefficients[0:rows], coefficients[rows : rows + TAIL]
    vectors = []
    for part, shift in ((one_ref, -toward), (group_ref, 0), (two_ref, toward)):
        first = jnp.clip(dom + shift, 0, lax.axis_size("dom") - 1) * subs
        for place in range(part.shape[0]):
            at = len(vectors)
            old = old_ref[at]
            image = every_ref[first + place // slots, place % slots : place % slots + 1, :]
            vector = jnp.sum(part[place] * head, axis=0, keepdims=True)
            vector = vector + jnp.sum(old * foot, axis=0, keepdims=True) + image * inverse_norm
            if tail_ref is not None:
                tail_ref[at] = tail_with(old, step, vector)
            vectors.append(vector)
    tails = []
    for slot in range(slots):
        old = old_own_ref[slot]
        vector = jnp.sum(own_ref[slot] * head, axis=0, keepdims=True)
        vector = vector + jnp.sum(old * foot, axis=0, keepdims=True)
        tails.append(tail_with(old, step, vector))
        vectors.append(vector)
    finish_step(vectors, tails, own_ref, tiles_ref, pick_ref, mask_ref, own_tail_ref, out_ref)


def last_step_body(step, count, paired, *refs):
    step_body(step, count, paired, *refs[:12], None, *refs[12:])


def small_solve(matrix, target):
    size = len(target)
    low = [[None] * size for _ in range(size)]
    inverses = []
    for j in range(size):
        value = matrix[j][j]
        for k in range(j):
            value = value - low[j][k] * low[j][k]
        inverses.append(1.0 / jnp.sqrt(value))
        for i in range(j + 1, size):
            value = matrix[i][j]
            for k in range(j):
                value = value - low[i][k] * low[j][k]
            low[i][j] = value * inverses[j]
    forward = []
    for i in range(size):
        value = target[i]
        for k in range(i):
            value = value - low[i][k] * forward[k]
        forward.append(value * inverses[i])
    back = [None] * size
    for i in reversed(range(size)):
        value = forward[i]
        for k in range(i + 1, size):
            value = value - low[k][i] * back[k]
        back[i] = value * inverses[i]
    return back


def end_body(count, mask_ref, every_ref, own_ref, tail_ref, inverse_ref, start_ref, recycled_ref, *rest):
    histories, (solution_ref, residual_ref) = rest[:-2], rest[-2:]
    slots, rows, width = own_ref.shape
    full = rows + TAIL
    total_row = tree_sum([every_ref[i] for i in range(every_ref.shape[0])])
    projected, norm, _, down = project(total_row, inverse_ref[...], rows, width)
    columns = [history[...] for history in histories]
    columns.append(jnp.where(down == count, norm, projected))
    entries = []
    for j in range(STEPS):
        column = [columns[j][rows + i : rows + i + 1, :] for i in range(j + 1)]
        column.append(columns[j][count : count + 1, :])
        entries.append(column)
    normal = [[None] * STEPS for _ in range(STEPS)]
    for a in range(STEPS):
        for b in range(a + 1):
            shared = range(min(len(entries[a]), len(entries[b])))
            normal[a][b] = tree_sum([entries[a][r] * entries[b][r] for r in shared])
    initial = start_ref[rows : rows + 1, :]
    least = small_solve(normal, [initial * entries[j][0] for j in range(STEPS)])
    image = []
    for r in range(STEPS + 1):
        image.append(tree_sum([entries[j][r] * least[j] for j in range(STEPS) if r < len(entries[j])]))
    start = start_ref[0:rows, :]
    recycled_coefficients = start[0:count] * -1.0
    for j in range(STEPS):
        recycled_coefficients = recycled_coefficients - columns[j][0:count] * least[j]
    ratio = image[STEPS] / norm
    head = jnp.where(down[0:rows] < count, start + columns[-1][0:rows] * ratio, start)
    tail_down = down[0:TAIL]
    solution_tail = jnp.zeros((TAIL, width), F32)
    residual_tail = jnp.zeros((TAIL, width), F32)
    for j in range(STEPS):
        solution_tail = jnp.where(tail_down == j, least[j], solution_tail)
        residual_tail = jnp.where(tail_down == j, entries[-1][j] * ratio - image[j], residual_tail)
    residual_tail = jnp.where(tail_down == STEPS, -ratio, residual_tail)
    for slot in range(slots):
        tail = tail_ref[slot]
        mask = mask_ref[slot : slot + 1, :]
        point = jnp.sum(recycled_ref[:, slot, :] * mask * recycled_coefficients, axis=0, keepdims=True)
        point = point + jnp.sum(tail * solution_tail, axis=0, keepdims=True)
        solution_ref[slot : slot + 1, :] = point
        left = jnp.sum(own_ref[slot] * head, axis=0, keepdims=True)
        left = left + jnp.sum(tail * residual_tail, axis=0, keepdims=True)
        residual_ref[slot : slot + 1, :] = left


def local(load_vector, recycled, images, matrix_tiles, tile_columns, ghost_list, live_counts):
    slots, width = load_vector.shape
    count = recycled.shape[0]
    doms, subs = lax.axis_size("dom"), lax.axis_size("sub")
    devices = doms * subs
    rows = round_up(count + 1, ROW_ALIGN)
    full = rows + TAIL
    per_row = tile_columns.shape[1]
    own, mask = call(
        pack_body,
        "pack",
        [(slots, rows, width), (round_up(slots, 8), width)],
        [SMEM, VMEM, VMEM],
    )(live_counts, load_vector, images)
    group = lax.all_gather(own, "sub", axis=0, tiled=True)
    each = rows // lane_groups(count, rows, width)
    (grams,) = call(functools.partial(gram_body, count), "gram", [(doms, each, width)], [VMEM])(group)
    parts = lax.all_to_all(grams, "dom", 0, 0)
    paired = subs % 2 == 0
    if paired:
        pairs = []
        for d in range(doms):
            for s in range(subs):
                to = d + 1 if s % 2 else d - 1
                if 0 <= to < doms:
                    pairs.append((d * subs + s, to * subs + s))
        one = lax.ppermute(group, AXES, pairs)
        one, parts = lax.optimization_barrier((one, parts))
        two = lax.ppermute(one, "sub", [(i, i ^ 1) for i in range(subs)])
    else:
        up = [(i, i + 1) for i in range(doms - 1)]
        one = lax.ppermute(group, "dom", up)
        two = lax.ppermute(group, "dom", [(j, i) for i, j in up])
    lines = round_up(slots + 1, 4)
    near = 3 * group.shape[0]
    inverse, start, pick, tiles = call(
        functools.partial(factor_body, count, rows, paired),
        "factor",
        [(full, width), (full, width), (near + slots, slots * per_row, width), matrix_tiles.shape],
        [VMEM, VMEM, HBM, VMEM],
        [pltpu.SemaphoreType.DMA],
    )(tile_columns, ghost_list, pltpu.with_memory_space_constraint(matrix_tiles, pltpu.HBM), parts)
    message, tails, own_tails = call(
        start_body,
        "start",
        [(devices, lines, width), (near, TAIL, width), (slots, TAIL, width)],
        [VMEM] * 8,
    )(start, own, one, group, two, tiles, pick, mask)
    histories = []
    for step in range(1, STEPS):
        every = lax.all_to_all(message, AXES, 0, 0)
        last = step == STEPS - 1
        sent = 1 if last else lines
        results = call(
            functools.partial(last_step_body if last else step_body, step, count, paired),
            f"step{step}",
            [(devices, sent, width)]
            + ([] if last else [(near, TAIL, width)])
            + [(slots, TAIL, width), (full, width)],
            [VMEM] * 11,
        )(every, own, one, group, two, tails, own_tails, inverse, tiles, pick, mask)
        message, own_tails, history = results[0], results[-2], results[-1]
        tails = tails if last else results[1]
        histories.append(history)
    every = lax.all_to_all(message, AXES, 0, 0)
    return tuple(
        call(
            functools.partial(end_body, count),
            "end",
            [(slots, width), (slots, width)],
            [VMEM] * (7 + len(histories)),
        )(mask, every, own, own_tails, inverse, start, recycled, *histories)
    )


def solution(mesh):
    return jax.shard_map(
        local,
        mesh=mesh,
        in_specs=(
            P(("dom", "sub"), None),
            P(None, ("dom", "sub"), None),
            P(None, ("dom", "sub"), None),
            P(("dom", "sub"), None, None, None),
            P(("dom", "sub"), None),
            P(("dom", "sub"), None),
            P(("dom", "sub")),
        ),
        out_specs=(P(("dom", "sub"), None), P(("dom", "sub"), None)),
        check_vma=False,
    )
```

```python
import functools

import jax
import jax.numpy as jnp
from jax import lax
from jax.experimental import pallas as pl
from jax.experimental.pallas import tpu as pltpu
from jax.sharding import PartitionSpec as P


STEPS = 3
TAIL = 8
ROW_ALIGN = 8
AXES = ("dom", "sub")
VMEM = pl.BlockSpec(memory_space=pltpu.VMEM)
SMEM = pl.BlockSpec(memory_space=pltpu.SMEM)
HBM = pl.BlockSpec(memory_space=pltpu.HBM)
F32 = jnp.float32


def call(body, outs, specs, scratch=(), work=10_000_000):
    return pl.pallas_call(
        body,
        out_shape=[jax.ShapeDtypeStruct(shape, F32) for shape in outs],
        in_specs=specs,
        out_specs=[VMEM] * len(outs),
        scratch_shapes=list(scratch),
        cost_estimate=pl.CostEstimate(flops=work, bytes_accessed=1 << 20, transcendentals=0),
        compiler_params=pltpu.CompilerParams(vmem_limit_bytes=16 * 1024 * 1024),
    )


def round_up(value, step):
    return -(-value // step) * step


def eye(rows, lanes):
    down = lax.broadcasted_iota(jnp.int32, (rows, lanes), 0)
    across = lax.broadcasted_iota(jnp.int32, (rows, lanes), 1)
    return down == across


def to_row(column, mask):
    return jnp.sum(jnp.where(mask, column, 0.0), axis=0, keepdims=True)


def tree_sum(parts):
    while len(parts) > 1:
        pairs = [parts[i] + parts[i + 1] for i in range(0, len(parts) - 1, 2)]
        parts = pairs + parts[len(parts) - len(parts) % 2 :]
    return parts[0]


def pack_body(live_ref, load_ref, images_ref, own_ref, mask_ref):
    count, slots, width = images_ref.shape
    rows = own_ref.shape[1]
    line = lax.broadcasted_iota(jnp.int32, mask_ref.shape, 0)
    mask_ref[...] = jnp.where(line < live_ref[0], 1.0, 0.0).astype(F32)
    for slot in range(slots):
        mask = jnp.where(slot < live_ref[0], 1.0, 0.0).astype(F32)
        own_ref[slot, 0:count, :] = images_ref[:, slot, :] * mask
        own_ref[slot, count : count + 1, :] = load_ref[slot : slot + 1, :] * mask
        own_ref[slot, count + 1 : rows, :] = jnp.zeros((rows - count - 1, width), F32)


def join_body(*refs):
    place = 0
    for part in refs[:-1]:
        for block in range(part.shape[0]):
            refs[-1][place] = part[block]
            place += 1


def lane_groups(count, rows, width):
    groups = width // (count + 1)
    if rows % groups == 0 and (rows // groups) % ROW_ALIGN == 0:
        return groups
    return 1


def gram_body(count, group_ref, out_ref):
    blocks, rows, width = group_ref.shape
    products = []
    for block in range(blocks):
        part = group_ref[block]
        products.append(
            lax.dot_general(
                part, part, (((1,), (1,)), ((), ())),
                precision=lax.Precision.HIGHEST, preferred_element_type=F32,
            )
        )
    gram = jnp.concatenate([tree_sum(products), jnp.zeros((rows, width - rows), F32)], axis=1)
    groups = lane_groups(count, rows, width)
    each, lanes = rows // groups, width // groups
    packed = gram[0:each]
    for group in range(1, groups):
        packed = packed + pltpu.roll(gram[group * each : (group + 1) * each], group * lanes, 1)
    for copy in range(out_ref.shape[0]):
        out_ref[copy] = packed


def multiply(left, right):
    return [[tree_sum([a * right[k][j] for k, a in enumerate(row)]) for j in range(len(right[0]))] for row in left]


def small_inverse(matrix):
    size = len(matrix)
    if size == 1:
        return [[1.0 / matrix[0][0]]]
    half = size // 2
    corner = [row[half:] for row in matrix[:half]]
    rest = [row[half:] for row in matrix[half:]]
    first = small_inverse([row[:half] for row in matrix[:half]])
    across = multiply(first, corner)
    taken = multiply([list(row) for row in zip(*corner)], across)
    second = small_inverse([[rest[i][j] - taken[i][j] for j in range(half)] for i in range(half)])
    product = multiply(across, second)
    added = multiply(product, [list(row) for row in zip(*across)])
    top = [[first[i][j] + added[i][j] for j in range(half)] + [-value for value in product[i]] for i in range(half)]
    bottom = [[-product[j][i] for j in range(half)] + second[i] for i in range(half)]
    return top + bottom


def sweep(matrix, count):
    rows, width = matrix.shape
    size = next(size for size in (8, 4, 2, 1) if count % size == 0)
    tiles = [matrix[i : i + 8, :] for i in range(0, rows, 8)]
    across = lax.broadcasted_iota(jnp.int32, (8, width), 1)
    down = lax.broadcasted_iota(jnp.int32, (8, width), 0)

    def spread(value):
        return jnp.broadcast_to(value, (8, width))

    for k in range(0, count, size):
        at, inner = divmod(k, 8)
        columns = [[tile[:, k + i : k + i + 1] for tile in tiles] for i in range(size)]
        lines = [spread(tiles[at][inner + i : inner + i + 1, :]) for i in range(size)]
        full = [spread(columns[i][at]) for i in range(size)]
        pivots = [
            [spread(full[max(i, j)][inner + min(i, j) : inner + min(i, j) + 1, :]) for j in range(size)]
            for i in range(size)
        ]
        inverse = small_inverse(pivots)
        scaled = []
        for i in range(size):
            line = tree_sum([lines[j] * inverse[i][j] for j in range(size)])
            for j in range(size):
                line = jnp.where(across == k + j, inverse[i][j], line)
            scaled.append(line)
        inside = (across >= k) & (across < k + size)
        updated = []
        for n, tile in enumerate(tiles):
            value = jnp.where(inside, 0.0, tile)
            value = value - tree_sum([columns[i][n] * scaled[i] for i in range(size)])
            if n == at:
                for i in range(size):
                    value = jnp.where(down == inner + i, scaled[i], value)
            updated.append(value)
        tiles = updated
    return jnp.concatenate(tiles, axis=0)


def apply_tiles(tiles_ref, pick_ref, vectors, mask_ref):
    slots, per_row, size, _ = tiles_ref.shape
    mask = eye(size, size)
    images = []
    for slot in range(slots):
        picked = tree_sum(
            [pick_ref[e, slot * per_row : (slot + 1) * per_row, :] * vector for e, vector in enumerate(vectors)]
        )
        parts = [tiles_ref[slot, t] * picked[t : t + 1, :] for t in range(per_row)]
        column = jnp.sum(tree_sum(parts), axis=1, keepdims=True)
        images.append(to_row(column, mask) * mask_ref[slot : slot + 1, :])
    return images


def tail_with(old, row, value):
    down = lax.broadcasted_iota(jnp.int32, (TAIL, old.shape[1]), 0)
    return jnp.where(down == row, value, old)


def finish_step(vectors, tails, own_ref, tiles_ref, pick_ref, mask_ref, own_tail_ref, out_ref):
    slots, rows, width = own_ref.shape
    images = apply_tiles(tiles_ref, pick_ref, vectors, mask_ref)
    total = jnp.zeros((rows + TAIL, width), F32)
    for slot in range(slots):
        tail = tail_with(tails[slot], STEPS, images[slot])
        own_tail_ref[slot] = tail
        total = total + jnp.concatenate([own_ref[slot], tail], axis=0) * images[slot]
    partial = to_row(jnp.sum(total, axis=1, keepdims=True), eye(rows + TAIL, width))
    copies, lines, _ = out_ref.shape
    if lines == 1:
        message = partial
    else:
        pad = [jnp.zeros((lines - slots - 1, width), F32)] if lines > slots + 1 else []
        message = jnp.concatenate([*images, partial, *pad], axis=0)
    out_ref[...] = jnp.broadcast_to(message[None], (copies, lines, width))


def near_peers(subs, paired, doubling):
    me = lax.axis_index("sub")
    first = (1 - me % 2) * 2 if paired else 0
    result = []
    for part, swapped in ((first, 0), (1, 0), (2 - first, 1 if paired else 0)):
        result.append((part, [(peer ^ swapped) ^ me if doubling else peer for peer in range(subs)]))
    return result


def factor_body(
    count, rows, paired, doubling, columns_ref, ghosts_ref, tiles_ref, parts_ref, inverse_ref, start_ref, pick_ref, here_ref, sem
):
    move = pltpu.make_async_copy(tiles_ref, here_ref, sem)
    move.start()
    width = parts_ref.shape[2]
    groups = lane_groups(count, rows, width)
    lanes = width // groups
    packed = lax.fori_loop(1, parts_ref.shape[0], lambda i, held: held + parts_ref[i], parts_ref[0])
    across = lax.broadcasted_iota(jnp.int32, (rows, width), 1)
    down = lax.broadcasted_iota(jnp.int32, (rows, width), 0)
    pieces = [packed]
    for group in range(1, groups):
        pieces.append(pltpu.roll(packed, width - group * lanes, 1))
    gram = jnp.where(across <= count, jnp.concatenate(pieces, axis=0), 0.0)
    swept = sweep(gram, count)
    keep = (down < count) & (across < count)
    inverse_ref[0:rows, :] = jnp.where(keep, swept, 0.0)
    tail_down = lax.broadcasted_iota(jnp.int32, (TAIL, width), 0)
    tail_across = lax.broadcasted_iota(jnp.int32, (TAIL, width), 1)
    inverse_ref[rows : rows + TAIL, :] = jnp.where(
        (tail_down < STEPS) & (tail_across == tail_down + rows), 1.0, 0.0
    )
    squared = jnp.broadcast_to(swept[count : count + 1, count : count + 1], (TAIL, width))
    inverse_norm = lax.rsqrt(squared)
    start = jnp.where(down < count, -swept[:, count : count + 1], jnp.where(down == count, 1.0, 0.0))
    start_ref[0:rows, :] = start
    start_ref[rows : rows + TAIL, :] = jnp.where(tail_down == 0, squared * inverse_norm, inverse_norm)
    slots, per_row = columns_ref.shape
    blocks = (pick_ref.shape[0] - slots) // 3
    places = [
        part * blocks + peer * slots + slot
        for part, peers in near_peers(blocks // slots, paired, doubling)
        for peer in peers
        for slot in range(slots)
    ]
    places += [3 * blocks + slot for slot in range(slots)]
    for slot in range(slots):
        names = columns_ref[slot : slot + 1, :]
        wanted = names + 3 * blocks
        for ghost in range(ghosts_ref.shape[1]):
            wanted = jnp.where(names == slots + ghost, ghosts_ref[:, ghost : ghost + 1], wanted)
        wanted = wanted.astype(F32)
        column = jnp.sum(jnp.where(eye(per_row, per_row), wanted, 0.0), axis=1, keepdims=True)
        column = jnp.broadcast_to(column, (per_row, width)).astype(jnp.int32)
        for at, place in enumerate(places):
            pick_ref[at, slot * per_row : (slot + 1) * per_row, :] = jnp.where(column == place, 1.0, 0.0)
    move.wait()


def start_body(
    start_ref, own_ref, one_ref, group_ref, two_ref, tiles_ref, pick_ref, mask_ref, out_ref, tail_ref, own_tail_ref
):
    _, rows, width = own_ref.shape
    blocks = group_ref.shape[0]
    coefficients = start_ref[0:rows, :] * start_ref[rows + 1 : rows + 2, :]
    empty = jnp.zeros((TAIL, width), F32)
    vectors = []
    tails = []
    for part in (one_ref, group_ref, two_ref, own_ref):
        for place in range(part.shape[0]):
            vector = jnp.sum(part[place] * coefficients, axis=0, keepdims=True)
            tail = tail_with(empty, 0, vector)
            if len(vectors) < 3 * blocks:
                tail_ref[len(vectors)] = tail
            else:
                tails.append(tail)
            vectors.append(vector)
    finish_step(vectors, tails, own_ref, tiles_ref, pick_ref, mask_ref, own_tail_ref, out_ref)


def project(total_row, inverse, rows, width):
    full = rows + TAIL
    down = lax.broadcasted_iota(jnp.int32, (full, width), 0)
    projected = jnp.sum(inverse * total_row, axis=1, keepdims=True)
    column = jnp.sum(jnp.where(eye(full, width), total_row, 0.0), axis=1, keepdims=True)
    projected = jnp.broadcast_to(projected, (full, width))
    squared = jnp.sum(
        jnp.where(down == rows + STEPS, column, -(column * projected)), axis=0, keepdims=True
    )
    inverse_norm = lax.rsqrt(squared)
    return projected, squared * inverse_norm, inverse_norm, down


def step_body(
    step, count, paired, doubling, every_ref, own_ref, one_ref, group_ref, two_ref, old_ref, old_own_ref, inverse_ref,
    tiles_ref, pick_ref, mask_ref, out_ref, tail_ref, own_tail_ref, history_ref,
):
    slots, rows, width = own_ref.shape
    subs = lax.axis_size("sub")
    last_dom = lax.axis_size("dom") - 1
    total_row = tree_sum([every_ref[i, slots : slots + 1, :] for i in range(every_ref.shape[0])])
    projected, norm, inverse_norm, down = project(total_row, inverse_ref[...], rows, width)
    history_ref[...] = jnp.where(down == count, norm, projected)
    coefficients = jnp.where(down == rows + STEPS, inverse_norm, -(projected * inverse_norm))
    head, foot = coefficients[0:rows], coefficients[rows : rows + TAIL]
    vectors = []
    for part, (offset, peers) in zip((one_ref, group_ref, two_ref), near_peers(subs, paired, doubling)):
        first = jnp.clip(lax.axis_index("dom") + offset - 1, 0, last_dom) * subs
        for place in range(part.shape[0]):
            at = len(vectors)
            old = old_ref[at]
            image = every_ref[first + peers[place // slots], place % slots : place % slots + 1, :]
            vector = jnp.sum(part[place] * head, axis=0, keepdims=True)
            vector = vector + jnp.sum(old * foot, axis=0, keepdims=True) + image * inverse_norm
            if tail_ref is not None:
                tail_ref[at] = tail_with(old, step, vector)
            vectors.append(vector)
    tails = []
    for slot in range(slots):
        old = old_own_ref[slot]
        vector = jnp.sum(own_ref[slot] * head, axis=0, keepdims=True)
        vector = vector + jnp.sum(old * foot, axis=0, keepdims=True)
        tails.append(tail_with(old, step, vector))
        vectors.append(vector)
    finish_step(vectors, tails, own_ref, tiles_ref, pick_ref, mask_ref, own_tail_ref, out_ref)


def last_step_body(step, count, paired, doubling, *refs):
    step_body(step, count, paired, doubling, *refs[:12], None, *refs[12:])


def small_solve(matrix, target):
    size = len(target)
    low = [[None] * size for _ in range(size)]
    inverses = []
    for j in range(size):
        value = matrix[j][j]
        for k in range(j):
            value = value - low[j][k] * low[j][k]
        inverses.append(1.0 / jnp.sqrt(value))
        for i in range(j + 1, size):
            value = matrix[i][j]
            for k in range(j):
                value = value - low[i][k] * low[j][k]
            low[i][j] = value * inverses[j]
    forward = []
    for i in range(size):
        value = target[i]
        for k in range(i):
            value = value - low[i][k] * forward[k]
        forward.append(value * inverses[i])
    back = [None] * size
    for i in reversed(range(size)):
        value = forward[i]
        for k in range(i + 1, size):
            value = value - low[k][i] * back[k]
        back[i] = value * inverses[i]
    return back


def end_body(count, mask_ref, every_ref, own_ref, tail_ref, inverse_ref, start_ref, recycled_ref, *rest):
    histories, (solution_ref, residual_ref) = rest[:-2], rest[-2:]
    slots, rows, width = own_ref.shape
    total_row = tree_sum([every_ref[i] for i in range(every_ref.shape[0])])
    projected, norm, _, down = project(total_row, inverse_ref[...], rows, width)
    columns = [history[...] for history in histories]
    columns.append(jnp.where(down == count, norm, projected))
    entries = []
    for j in range(STEPS):
        column = [columns[j][rows + i : rows + i + 1, :] for i in range(j + 1)]
        column.append(columns[j][count : count + 1, :])
        entries.append(column)
    normal = [[None] * STEPS for _ in range(STEPS)]
    for a in range(STEPS):
        for b in range(a + 1):
            shared = range(min(len(entries[a]), len(entries[b])))
            normal[a][b] = tree_sum([entries[a][r] * entries[b][r] for r in shared])
    initial = start_ref[rows : rows + 1, :]
    least = small_solve(normal, [initial * entries[j][0] for j in range(STEPS)])
    image = []
    for r in range(STEPS + 1):
        image.append(tree_sum([entries[j][r] * least[j] for j in range(STEPS) if r < len(entries[j])]))
    start = start_ref[0:rows, :]
    recycled_coefficients = start[0:count] * -1.0
    for j in range(STEPS):
        recycled_coefficients = recycled_coefficients - columns[j][0:count] * least[j]
    ratio = image[STEPS] / norm
    head = jnp.where(down[0:rows] < count, start + columns[-1][0:rows] * ratio, start)
    tail_down = down[0:TAIL]
    solution_tail = jnp.zeros((TAIL, width), F32)
    residual_tail = jnp.zeros((TAIL, width), F32)
    for j in range(STEPS):
        solution_tail = jnp.where(tail_down == j, least[j], solution_tail)
        residual_tail = jnp.where(tail_down == j, entries[-1][j] * ratio - image[j], residual_tail)
    residual_tail = jnp.where(tail_down == STEPS, -ratio, residual_tail)
    for slot in range(slots):
        tail = tail_ref[slot]
        mask = mask_ref[slot : slot + 1, :]
        point = jnp.sum(recycled_ref[:, slot, :] * mask * recycled_coefficients, axis=0, keepdims=True)
        point = point + jnp.sum(tail * solution_tail, axis=0, keepdims=True)
        solution_ref[slot : slot + 1, :] = point
        left = jnp.sum(own_ref[slot] * head, axis=0, keepdims=True)
        left = left + jnp.sum(tail * residual_tail, axis=0, keepdims=True)
        residual_ref[slot : slot + 1, :] = left


def local(load_vector, recycled, images, matrix_tiles, tile_columns, ghost_list, live_counts):
    slots, width = load_vector.shape
    count = recycled.shape[0]
    doms, subs = lax.axis_size("dom"), lax.axis_size("sub")
    devices = doms * subs
    rows = round_up(count + 1, ROW_ALIGN)
    full = rows + TAIL
    per_row = tile_columns.shape[1]
    own, mask = call(
        pack_body, [(slots, rows, width), (round_up(slots, 8), width)], [SMEM, VMEM, VMEM]
    )(live_counts, load_vector, images)
    each = rows // lane_groups(count, rows, width)
    paired = subs % 2 == 0
    doubling = subs == 4
    (grams,) = call(functools.partial(gram_body, count), [(devices, each, width)], [VMEM])(own)

    def turn(value, bit):
        return lax.ppermute(value, "sub", [(i, i ^ bit) for i in range(subs)])

    if doubling:
        inner = turn(own, 1)
        outer = turn(own, 2)
    parts = lax.all_to_all(grams, AXES, 0, 0)
    if doubling:
        corner = turn(outer, 1)
        (group,) = call(join_body, [(subs * slots, rows, width)], [VMEM] * 4)(own, inner, outer, corner)
    else:
        group = lax.all_gather(own, "sub", axis=0, tiled=True)
    if paired:
        pairs = []
        for d in range(doms):
            for s in range(subs):
                to = d + 1 if s % 2 else d - 1
                if 0 <= to < doms:
                    pairs.append((d * subs + s, to * subs + s))
        one = lax.ppermute(group, AXES, pairs)
    else:
        up = [(i, i + 1) for i in range(doms - 1)]
        one = lax.ppermute(group, "dom", up)
        two = lax.ppermute(group, "dom", [(j, i) for i, j in up])
    lines = round_up(slots + 1, 4)
    near = 3 * group.shape[0]
    inverse, start, pick, tiles = call(
        functools.partial(factor_body, count, rows, paired, doubling),
        [(full, width), (full, width), (near + slots, slots * per_row, width), matrix_tiles.shape],
        [VMEM, VMEM, HBM, VMEM],
        [pltpu.SemaphoreType.DMA],
    )(tile_columns, ghost_list, pltpu.with_memory_space_constraint(matrix_tiles, pltpu.HBM), parts)
    if paired:
        one, start = lax.optimization_barrier((one, start))
        two = turn(one, 1)
    message, tails, own_tails = call(
        start_body, [(devices, lines, width), (near, TAIL, width), (slots, TAIL, width)], [VMEM] * 8
    )(start, own, one, group, two, tiles, pick, mask)
    histories = []
    for step in range(1, STEPS):
        every = lax.all_to_all(message, AXES, 0, 0)
        last = step == STEPS - 1
        sent = 1 if last else lines
        results = call(
            functools.partial(last_step_body if last else step_body, step, count, paired, doubling),
            [(devices, sent, width)]
            + ([] if last else [(near, TAIL, width)])
            + [(slots, TAIL, width), (full, width)],
            [VMEM] * 11,
        )(every, own, one, group, two, tails, own_tails, inverse, tiles, pick, mask)
        message, own_tails, history = results[0], results[-2], results[-1]
        tails = tails if last else results[1]
        histories.append(history)
    every = lax.all_to_all(message, AXES, 0, 0)
    return tuple(
        call(
            functools.partial(end_body, count), [(slots, width), (slots, width)], [VMEM] * (7 + len(histories))
        )(mask, every, own, own_tails, inverse, start, recycled, *histories)
    )


def solution(mesh):
    return jax.shard_map(
        local,
        mesh=mesh,
        in_specs=(
            P(("dom", "sub"), None),
            P(None, ("dom", "sub"), None),
            P(None, ("dom", "sub"), None),
            P(("dom", "sub"), None, None, None),
            P(("dom", "sub"), None),
            P(("dom", "sub"), None),
            P(("dom", "sub")),
        ),
        out_specs=(P(("dom", "sub"), None), P(("dom", "sub"), None)),
        check_vma=False,
    )
```

```python
import functools

import jax
import jax.numpy as jnp
from jax import lax
from jax.experimental import pallas as pl
from jax.experimental.pallas import tpu as pltpu
from jax.sharding import PartitionSpec as P


STEPS = 3
TAIL = 8
ROW_ALIGN = 8
AXES = ("dom", "sub")
VMEM = pl.BlockSpec(memory_space=pltpu.VMEM)
SMEM = pl.BlockSpec(memory_space=pltpu.SMEM)
HBM = pl.BlockSpec(memory_space=pltpu.HBM)
F32 = jnp.float32


def call(body, outs, specs, scratch=(), work=10_000_000):
    return pl.pallas_call(
        body,
        out_shape=[jax.ShapeDtypeStruct(shape, F32) for shape in outs],
        in_specs=specs,
        out_specs=[VMEM] * len(outs),
        scratch_shapes=list(scratch),
        cost_estimate=pl.CostEstimate(flops=work, bytes_accessed=1 << 20, transcendentals=0),
        compiler_params=pltpu.CompilerParams(vmem_limit_bytes=16 * 1024 * 1024),
    )


def round_up(value, step):
    return -(-value // step) * step


def eye(rows, lanes):
    down = lax.broadcasted_iota(jnp.int32, (rows, lanes), 0)
    across = lax.broadcasted_iota(jnp.int32, (rows, lanes), 1)
    return down == across


def to_row(column, mask):
    return jnp.sum(jnp.where(mask, column, 0.0), axis=0, keepdims=True)


def tree_sum(parts):
    while len(parts) > 1:
        pairs = [parts[i] + parts[i + 1] for i in range(0, len(parts) - 1, 2)]
        parts = pairs + parts[len(parts) - len(parts) % 2 :]
    return parts[0]


def pack_body(live_ref, load_ref, images_ref, own_ref, mask_ref):
    count, slots, width = images_ref.shape
    rows = own_ref.shape[1]
    line = lax.broadcasted_iota(jnp.int32, mask_ref.shape, 0)
    mask_ref[...] = jnp.where(line < live_ref[0], 1.0, 0.0).astype(F32)
    for slot in range(slots):
        mask = jnp.where(slot < live_ref[0], 1.0, 0.0).astype(F32)
        own_ref[slot, 0:count, :] = images_ref[:, slot, :] * mask
        own_ref[slot, count : count + 1, :] = load_ref[slot : slot + 1, :] * mask
        own_ref[slot, count + 1 : rows, :] = jnp.zeros((rows - count - 1, width), F32)


def join_body(*refs):
    place = 0
    for part in refs[:-1]:
        for block in range(part.shape[0]):
            refs[-1][place] = part[block]
            place += 1


def half_groups(size, rows, width):
    lanes = size // 2 + 1
    fits = [g for g in range(1, width // lanes + 1) if rows % g == 0 and (rows // g) % ROW_ALIGN == 0]
    return lanes, max(fits)


def pack_symmetric(gram, size):
    rows, width = gram.shape
    lanes, groups = half_groups(size, rows, width)
    each = rows // groups
    across = lax.broadcasted_iota(jnp.int32, (each, width), 1)
    down = lax.broadcasted_iota(jnp.int32, (each, width), 0)
    twice = gram + pltpu.roll(gram, size, 1)
    pieces = []
    for group in range(groups):
        piece = twice[group * each : (group + 1) * each]
        bit = 1
        while bit < each:
            piece = jnp.where((down & bit) != 0, pltpu.roll(piece, width - bit, 1), piece)
            bit *= 2
        shift = group * (lanes - each) % width
        piece = pltpu.roll(piece, shift, 1) if shift else piece
        first = group * lanes
        if size % 2 == 0:
            piece = jnp.where(across == first + lanes - 1, piece * 0.5, piece)
        pieces.append(jnp.where((across >= first) & (across < first + lanes), piece, 0.0))
    return tree_sum(pieces)


def unpack_symmetric(packed, size, rows):
    each, width = packed.shape
    lanes, groups = half_groups(size, rows, width)
    across = lax.broadcasted_iota(jnp.int32, (each, width), 1)
    pieces = []
    for group in range(groups):
        shift = group * (each - lanes) % width
        piece = pltpu.roll(packed, shift, 1) if shift else packed
        first = group * each
        piece = jnp.where((across >= first) & (across < first + lanes), piece, 0.0)
        pieces.append(pltpu.roll(piece, 0, 1, stride=1, stride_axis=0))
    turned = jnp.concatenate(pieces, axis=0)
    across = lax.broadcasted_iota(jnp.int32, (rows, width), 1)
    folded = jnp.where(across < size, turned + pltpu.roll(turned, width - size, 1), 0.0)
    square = jnp.concatenate([folded, jnp.zeros((width - rows, width), F32)], axis=0)
    return jnp.where(eye(rows, width), folded, folded + square.T[0:rows])


def gram_body(count, group_ref, out_ref):
    blocks, rows, width = group_ref.shape
    products = []
    for block in range(blocks):
        part = group_ref[block]
        products.append(
            lax.dot_general(
                part, part, (((1,), (1,)), ((), ())),
                precision=lax.Precision.HIGHEST, preferred_element_type=F32,
            )
        )
    gram = jnp.concatenate([tree_sum(products), jnp.zeros((rows, width - rows), F32)], axis=1)
    packed = pack_symmetric(gram, count + 1)
    for copy in range(out_ref.shape[0]):
        out_ref[copy] = packed


def multiply(left, right):
    return [[tree_sum([a * right[k][j] for k, a in enumerate(row)]) for j in range(len(right[0]))] for row in left]


def small_inverse(matrix):
    size = len(matrix)
    if size == 1:
        return [[1.0 / matrix[0][0]]]
    half = size // 2
    corner = [row[half:] for row in matrix[:half]]
    rest = [row[half:] for row in matrix[half:]]
    first = small_inverse([row[:half] for row in matrix[:half]])
    across = multiply(first, corner)
    taken = multiply([list(row) for row in zip(*corner)], across)
    second = small_inverse([[rest[i][j] - taken[i][j] for j in range(half)] for i in range(half)])
    product = multiply(across, second)
    added = multiply(product, [list(row) for row in zip(*across)])
    top = [[first[i][j] + added[i][j] for j in range(half)] + [-value for value in product[i]] for i in range(half)]
    bottom = [[-product[j][i] for j in range(half)] + second[i] for i in range(half)]
    return top + bottom


def sweep(matrix, count):
    rows, width = matrix.shape
    size = next(size for size in (8, 4, 2, 1) if count % size == 0)
    tiles = [matrix[i : i + 8, :] for i in range(0, rows, 8)]
    across = lax.broadcasted_iota(jnp.int32, (8, width), 1)
    down = lax.broadcasted_iota(jnp.int32, (8, width), 0)

    def spread(value):
        return jnp.broadcast_to(value, (8, width))

    for k in range(0, count, size):
        at, inner = divmod(k, 8)
        columns = [[tile[:, k + i : k + i + 1] for tile in tiles] for i in range(size)]
        lines = [spread(tiles[at][inner + i : inner + i + 1, :]) for i in range(size)]
        full = [spread(columns[i][at]) for i in range(size)]
        pivots = [
            [spread(full[max(i, j)][inner + min(i, j) : inner + min(i, j) + 1, :]) for j in range(size)]
            for i in range(size)
        ]
        inverse = small_inverse(pivots)
        scaled = []
        for i in range(size):
            line = tree_sum([lines[j] * inverse[i][j] for j in range(size)])
            for j in range(size):
                line = jnp.where(across == k + j, inverse[i][j], line)
            scaled.append(line)
        inside = (across >= k) & (across < k + size)
        updated = []
        for n, tile in enumerate(tiles):
            value = jnp.where(inside, 0.0, tile)
            value = value - tree_sum([columns[i][n] * scaled[i] for i in range(size)])
            if n == at:
                for i in range(size):
                    value = jnp.where(down == inner + i, scaled[i], value)
            updated.append(value)
        tiles = updated
    return jnp.concatenate(tiles, axis=0)


def apply_tiles(tiles_ref, pick_ref, vectors, mask_ref):
    slots, per_row, size, _ = tiles_ref.shape
    mask = eye(size, size)
    images = []
    for slot in range(slots):
        picked = tree_sum(
            [pick_ref[e, slot * per_row : (slot + 1) * per_row, :] * vector for e, vector in enumerate(vectors)]
        )
        parts = [tiles_ref[slot, t] * picked[t : t + 1, :] for t in range(per_row)]
        column = jnp.sum(tree_sum(parts), axis=1, keepdims=True)
        images.append(to_row(column, mask) * mask_ref[slot : slot + 1, :])
    return images


def tail_with(old, row, value):
    down = lax.broadcasted_iota(jnp.int32, (TAIL, old.shape[1]), 0)
    return jnp.where(down == row, value, old)


def finish_step(vectors, tails, own_ref, tiles_ref, pick_ref, mask_ref, own_tail_ref, out_ref):
    slots, rows, width = own_ref.shape
    images = apply_tiles(tiles_ref, pick_ref, vectors, mask_ref)
    total = jnp.zeros((rows + TAIL, width), F32)
    for slot in range(slots):
        tail = tail_with(tails[slot], STEPS, images[slot])
        own_tail_ref[slot] = tail
        total = total + jnp.concatenate([own_ref[slot], tail], axis=0) * images[slot]
    partial = to_row(jnp.sum(total, axis=1, keepdims=True), eye(rows + TAIL, width))
    copies, lines, _ = out_ref.shape
    if lines == 1:
        message = partial
    else:
        pad = [jnp.zeros((lines - slots - 1, width), F32)] if lines > slots + 1 else []
        message = jnp.concatenate([*images, partial, *pad], axis=0)
    out_ref[...] = jnp.broadcast_to(message[None], (copies, lines, width))


def near_peers(subs, paired, doubling):
    me = lax.axis_index("sub")
    first = (1 - me % 2) * 2 if paired else 0
    result = []
    for part, swapped in ((first, 0), (1, 0), (2 - first, 1 if paired else 0)):
        result.append((part, [(peer ^ swapped) ^ me if doubling else peer for peer in range(subs)]))
    return result


def factor_body(
    count, rows, paired, doubling, columns_ref, ghosts_ref, tiles_ref, parts_ref, inverse_ref, start_ref, pick_ref, here_ref, sem
):
    move = pltpu.make_async_copy(tiles_ref, here_ref, sem)
    move.start()
    width = parts_ref.shape[2]
    packed = lax.fori_loop(1, parts_ref.shape[0], lambda i, held: held + parts_ref[i], parts_ref[0])
    across = lax.broadcasted_iota(jnp.int32, (rows, width), 1)
    down = lax.broadcasted_iota(jnp.int32, (rows, width), 0)
    gram = unpack_symmetric(packed, count + 1, rows)
    swept = sweep(gram, count)
    keep = (down < count) & (across < count)
    inverse_ref[0:rows, :] = jnp.where(keep, swept, 0.0)
    tail_down = lax.broadcasted_iota(jnp.int32, (TAIL, width), 0)
    tail_across = lax.broadcasted_iota(jnp.int32, (TAIL, width), 1)
    inverse_ref[rows : rows + TAIL, :] = jnp.where(
        (tail_down < STEPS) & (tail_across == tail_down + rows), 1.0, 0.0
    )
    squared = jnp.broadcast_to(swept[count : count + 1, count : count + 1], (TAIL, width))
    inverse_norm = lax.rsqrt(squared)
    start = jnp.where(down < count, -swept[:, count : count + 1], jnp.where(down == count, 1.0, 0.0))
    start_ref[0:rows, :] = start
    start_ref[rows : rows + TAIL, :] = jnp.where(tail_down == 0, squared * inverse_norm, inverse_norm)
    slots, per_row = columns_ref.shape
    blocks = (pick_ref.shape[0] - slots) // 3
    places = [
        part * blocks + peer * slots + slot
        for part, peers in near_peers(blocks // slots, paired, doubling)
        for peer in peers
        for slot in range(slots)
    ]
    places += [3 * blocks + slot for slot in range(slots)]
    for slot in range(slots):
        names = columns_ref[slot : slot + 1, :]
        wanted = names + 3 * blocks
        for ghost in range(ghosts_ref.shape[1]):
            wanted = jnp.where(names == slots + ghost, ghosts_ref[:, ghost : ghost + 1], wanted)
        wanted = wanted.astype(F32)
        column = jnp.sum(jnp.where(eye(per_row, per_row), wanted, 0.0), axis=1, keepdims=True)
        column = jnp.broadcast_to(column, (per_row, width)).astype(jnp.int32)
        for at, place in enumerate(places):
            pick_ref[at, slot * per_row : (slot + 1) * per_row, :] = jnp.where(column == place, 1.0, 0.0)
    move.wait()


def start_body(
    start_ref, own_ref, one_ref, group_ref, two_ref, tiles_ref, pick_ref, mask_ref, out_ref, tail_ref, own_tail_ref
):
    _, rows, width = own_ref.shape
    blocks = group_ref.shape[0]
    coefficients = start_ref[0:rows, :] * start_ref[rows + 1 : rows + 2, :]
    empty = jnp.zeros((TAIL, width), F32)
    vectors = []
    tails = []
    for part in (one_ref, group_ref, two_ref, own_ref):
        for place in range(part.shape[0]):
            vector = jnp.sum(part[place] * coefficients, axis=0, keepdims=True)
            tail = tail_with(empty, 0, vector)
            if len(vectors) < 3 * blocks:
                tail_ref[len(vectors)] = tail
            else:
                tails.append(tail)
            vectors.append(vector)
    finish_step(vectors, tails, own_ref, tiles_ref, pick_ref, mask_ref, own_tail_ref, out_ref)


def project(total_row, inverse, rows, width):
    full = rows + TAIL
    down = lax.broadcasted_iota(jnp.int32, (full, width), 0)
    projected = jnp.sum(inverse * total_row, axis=1, keepdims=True)
    column = jnp.sum(jnp.where(eye(full, width), total_row, 0.0), axis=1, keepdims=True)
    projected = jnp.broadcast_to(projected, (full, width))
    squared = jnp.sum(
        jnp.where(down == rows + STEPS, column, -(column * projected)), axis=0, keepdims=True
    )
    inverse_norm = lax.rsqrt(squared)
    return projected, squared * inverse_norm, inverse_norm, down


def step_body(
    step, count, paired, doubling, every_ref, own_ref, one_ref, group_ref, two_ref, old_ref, old_own_ref, inverse_ref,
    tiles_ref, pick_ref, mask_ref, out_ref, tail_ref, own_tail_ref, history_ref,
):
    slots, rows, width = own_ref.shape
    subs = lax.axis_size("sub")
    last_dom = lax.axis_size("dom") - 1
    total_row = tree_sum([every_ref[i, slots : slots + 1, :] for i in range(every_ref.shape[0])])
    projected, norm, inverse_norm, down = project(total_row, inverse_ref[...], rows, width)
    history_ref[...] = jnp.where(down == count, norm, projected)
    coefficients = jnp.where(down == rows + STEPS, inverse_norm, -(projected * inverse_norm))
    head, foot = coefficients[0:rows], coefficients[rows : rows + TAIL]
    vectors = []
    for part, (offset, peers) in zip((one_ref, group_ref, two_ref), near_peers(subs, paired, doubling)):
        first = jnp.clip(lax.axis_index("dom") + offset - 1, 0, last_dom) * subs
        for place in range(part.shape[0]):
            at = len(vectors)
            old = old_ref[at]
            image = every_ref[first + peers[place // slots], place % slots : place % slots + 1, :]
            vector = jnp.sum(part[place] * head, axis=0, keepdims=True)
            vector = vector + jnp.sum(old * foot, axis=0, keepdims=True) + image * inverse_norm
            if tail_ref is not None:
                tail_ref[at] = tail_with(old, step, vector)
            vectors.append(vector)
    tails = []
    for slot in range(slots):
        old = old_own_ref[slot]
        vector = jnp.sum(own_ref[slot] * head, axis=0, keepdims=True)
        vector = vector + jnp.sum(old * foot, axis=0, keepdims=True)
        tails.append(tail_with(old, step, vector))
        vectors.append(vector)
    finish_step(vectors, tails, own_ref, tiles_ref, pick_ref, mask_ref, own_tail_ref, out_ref)


def last_step_body(step, count, paired, doubling, *refs):
    step_body(step, count, paired, doubling, *refs[:12], None, *refs[12:])


def small_solve(matrix, target):
    size = len(target)
    low = [[None] * size for _ in range(size)]
    inverses = []
    for j in range(size):
        value = matrix[j][j]
        for k in range(j):
            value = value - low[j][k] * low[j][k]
        inverses.append(1.0 / jnp.sqrt(value))
        for i in range(j + 1, size):
            value = matrix[i][j]
            for k in range(j):
                value = value - low[i][k] * low[j][k]
            low[i][j] = value * inverses[j]
    forward = []
    for i in range(size):
        value = target[i]
        for k in range(i):
            value = value - low[i][k] * forward[k]
        forward.append(value * inverses[i])
    back = [None] * size
    for i in reversed(range(size)):
        value = forward[i]
        for k in range(i + 1, size):
            value = value - low[k][i] * back[k]
        back[i] = value * inverses[i]
    return back


def end_body(count, mask_ref, every_ref, own_ref, tail_ref, inverse_ref, start_ref, recycled_ref, *rest):
    histories, (solution_ref, residual_ref) = rest[:-2], rest[-2:]
    slots, rows, width = own_ref.shape
    total_row = tree_sum([every_ref[i] for i in range(every_ref.shape[0])])
    projected, norm, _, down = project(total_row, inverse_ref[...], rows, width)
    columns = [history[...] for history in histories]
    columns.append(jnp.where(down == count, norm, projected))
    entries = []
    for j in range(STEPS):
        column = [columns[j][rows + i : rows + i + 1, :] for i in range(j + 1)]
        column.append(columns[j][count : count + 1, :])
        entries.append(column)
    normal = [[None] * STEPS for _ in range(STEPS)]
    for a in range(STEPS):
        for b in range(a + 1):
            shared = range(min(len(entries[a]), len(entries[b])))
            normal[a][b] = tree_sum([entries[a][r] * entries[b][r] for r in shared])
    initial = start_ref[rows : rows + 1, :]
    least = small_solve(normal, [initial * entries[j][0] for j in range(STEPS)])
    image = []
    for r in range(STEPS + 1):
        image.append(tree_sum([entries[j][r] * least[j] for j in range(STEPS) if r < len(entries[j])]))
    start = start_ref[0:rows, :]
    recycled_coefficients = start[0:count] * -1.0
    for j in range(STEPS):
        recycled_coefficients = recycled_coefficients - columns[j][0:count] * least[j]
    ratio = image[STEPS] / norm
    head = jnp.where(down[0:rows] < count, start + columns[-1][0:rows] * ratio, start)
    tail_down = down[0:TAIL]
    solution_tail = jnp.zeros((TAIL, width), F32)
    residual_tail = jnp.zeros((TAIL, width), F32)
    for j in range(STEPS):
        solution_tail = jnp.where(tail_down == j, least[j], solution_tail)
        residual_tail = jnp.where(tail_down == j, entries[-1][j] * ratio - image[j], residual_tail)
    residual_tail = jnp.where(tail_down == STEPS, -ratio, residual_tail)
    for slot in range(slots):
        tail = tail_ref[slot]
        mask = mask_ref[slot : slot + 1, :]
        point = jnp.sum(recycled_ref[:, slot, :] * mask * recycled_coefficients, axis=0, keepdims=True)
        point = point + jnp.sum(tail * solution_tail, axis=0, keepdims=True)
        solution_ref[slot : slot + 1, :] = point
        left = jnp.sum(own_ref[slot] * head, axis=0, keepdims=True)
        left = left + jnp.sum(tail * residual_tail, axis=0, keepdims=True)
        residual_ref[slot : slot + 1, :] = left


def local(load_vector, recycled, images, matrix_tiles, tile_columns, ghost_list, live_counts):
    slots, width = load_vector.shape
    count = recycled.shape[0]
    doms, subs = lax.axis_size("dom"), lax.axis_size("sub")
    devices = doms * subs
    rows = round_up(count + 1, ROW_ALIGN)
    full = rows + TAIL
    per_row = tile_columns.shape[1]
    own, mask = call(
        pack_body, [(slots, rows, width), (round_up(slots, 8), width)], [SMEM, VMEM, VMEM]
    )(live_counts, load_vector, images)
    each = rows // half_groups(count + 1, rows, width)[1]
    paired = subs % 2 == 0
    doubling = subs == 4
    (grams,) = call(functools.partial(gram_body, count), [(devices, each, width)], [VMEM])(own)

    def turn(value, bit):
        return lax.ppermute(value, "sub", [(i, i ^ bit) for i in range(subs)])

    if doubling:
        inner = turn(own, 1)
        outer = turn(own, 2)
    if doubling:
        corner = turn(outer, 1)
        (group,) = call(join_body, [(subs * slots, rows, width)], [VMEM] * 4)(own, inner, outer, corner)
    else:
        group = lax.all_gather(own, "sub", axis=0, tiled=True)
    if paired:
        pairs = []
        for d in range(doms):
            for s in range(subs):
                to = d + 1 if s % 2 else d - 1
                if 0 <= to < doms:
                    pairs.append((d * subs + s, to * subs + s))
        one = lax.ppermute(group, AXES, pairs)
        two = turn(one, 1)
    else:
        up = [(i, i + 1) for i in range(doms - 1)]
        one = lax.ppermute(group, "dom", up)
        two = lax.ppermute(group, "dom", [(j, i) for i, j in up])
    parts = lax.all_to_all(grams, AXES, 0, 0)
    lines = round_up(slots + 1, 4)
    near = 3 * group.shape[0]
    inverse, start, pick, tiles = call(
        functools.partial(factor_body, count, rows, paired, doubling),
        [(full, width), (full, width), (near + slots, slots * per_row, width), matrix_tiles.shape],
        [VMEM, VMEM, HBM, VMEM],
        [pltpu.SemaphoreType.DMA],
    )(tile_columns, ghost_list, pltpu.with_memory_space_constraint(matrix_tiles, pltpu.HBM), parts)
    message, tails, own_tails = call(
        start_body, [(devices, lines, width), (near, TAIL, width), (slots, TAIL, width)], [VMEM] * 8
    )(start, own, one, group, two, tiles, pick, mask)
    histories = []
    for step in range(1, STEPS):
        every = lax.all_to_all(message, AXES, 0, 0)
        last = step == STEPS - 1
        sent = 1 if last else lines
        results = call(
            functools.partial(last_step_body if last else step_body, step, count, paired, doubling),
            [(devices, sent, width)]
            + ([] if last else [(near, TAIL, width)])
            + [(slots, TAIL, width), (full, width)],
            [VMEM] * 11,
        )(every, own, one, group, two, tails, own_tails, inverse, tiles, pick, mask)
        message, own_tails, history = results[0], results[-2], results[-1]
        tails = tails if last else results[1]
        histories.append(history)
    every = lax.all_to_all(message, AXES, 0, 0)
    return tuple(
        call(
            functools.partial(end_body, count), [(slots, width), (slots, width)], [VMEM] * (7 + len(histories))
        )(mask, every, own, own_tails, inverse, start, recycled, *histories)
    )


def solution(mesh):
    return jax.shard_map(
        local,
        mesh=mesh,
        in_specs=(
            P(("dom", "sub"), None),
            P(None, ("dom", "sub"), None),
            P(None, ("dom", "sub"), None),
            P(("dom", "sub"), None, None, None),
            P(("dom", "sub"), None),
            P(("dom", "sub"), None),
            P(("dom", "sub")),
        ),
        out_specs=(P(("dom", "sub"), None), P(("dom", "sub"), None)),
        check_vma=False,
    )
```

```python
import functools

import jax
import jax.numpy as jnp
from jax import lax
from jax.experimental import pallas as pl
from jax.experimental.pallas import tpu as pltpu
from jax.sharding import PartitionSpec as P

STEPS = 3
TAIL = 8
ROW_ALIGN = 8
AXES = ("dom", "sub")
VMEM = pl.BlockSpec(memory_space=pltpu.VMEM)
SMEM = pl.BlockSpec(memory_space=pltpu.SMEM)
HBM = pl.BlockSpec(memory_space=pltpu.HBM)
F32 = jnp.float32


def call(body, name, outs, specs, scratch=(), work=10_000_000):
    return pl.pallas_call(
        body,
        name=name,
        out_shape=[jax.ShapeDtypeStruct(shape, F32) for shape in outs],
        in_specs=specs,
        out_specs=[VMEM] * len(outs),
        scratch_shapes=list(scratch),
        cost_estimate=pl.CostEstimate(flops=work, bytes_accessed=1 << 20, transcendentals=0),
        compiler_params=pltpu.CompilerParams(vmem_limit_bytes=16 * 1024 * 1024),
    )


def round_up(value, step):
    return -(-value // step) * step


def eye(rows, lanes):
    down = lax.broadcasted_iota(jnp.int32, (rows, lanes), 0)
    across = lax.broadcasted_iota(jnp.int32, (rows, lanes), 1)
    return down == across


def to_row(column, mask):
    return jnp.sum(jnp.where(mask, column, 0.0), axis=0, keepdims=True)


def tree_sum(parts):
    while len(parts) > 1:
        pairs = [parts[i] + parts[i + 1] for i in range(0, len(parts) - 1, 2)]
        parts = pairs + parts[len(parts) - len(parts) % 2 :]
    return parts[0]


def pack_body(live_ref, load_ref, images_ref, own_ref, mask_ref):
    count, slots, width = images_ref.shape
    rows = own_ref.shape[1]
    line = lax.broadcasted_iota(jnp.int32, mask_ref.shape, 0)
    mask_ref[...] = jnp.where(line < live_ref[0], 1.0, 0.0).astype(F32)
    for slot in range(slots):
        mask = jnp.where(slot < live_ref[0], 1.0, 0.0).astype(F32)
        own_ref[slot, 0:count, :] = images_ref[:, slot, :] * mask
        own_ref[slot, count : count + 1, :] = load_ref[slot : slot + 1, :] * mask
        own_ref[slot, count + 1 : rows, :] = jnp.zeros((rows - count - 1, width), F32)


def join_body(*refs):
    place = 0
    for part in refs[:-1]:
        for block in range(part.shape[0]):
            refs[-1][place] = part[block]
            place += 1


def lane_groups(count, rows, width):
    groups = width // (count + 1)
    if rows % groups == 0 and (rows // groups) % ROW_ALIGN == 0:
        return groups
    return 1


def gram_of(*refs):
    products = []
    for ref in refs:
        for block in range(ref.shape[0]):
            part = ref[block]
            products.append(
                lax.dot_general(
                    part, part, (((1,), (1,)), ((), ())),
                    precision=lax.Precision.HIGHEST, preferred_element_type=F32,
                )
            )
    rows, width = refs[0].shape[1:]
    return jnp.concatenate([tree_sum(products), jnp.zeros((rows, width - rows), F32)], axis=1)


def first_gram_body(*refs):
    refs[-1][...] = gram_of(*refs[:-1])


def gram_body(count, held_ref, group_ref, out_ref):
    rows, width = group_ref.shape[1:]
    gram = gram_of(group_ref)
    if held_ref is not None:
        gram = gram + held_ref[...]
    groups = lane_groups(count, rows, width)
    each, lanes = rows // groups, width // groups
    packed = gram[0:each]
    for group in range(1, groups):
        packed = packed + pltpu.roll(gram[group * each : (group + 1) * each], group * lanes, 1)
    for copy in range(out_ref.shape[0]):
        out_ref[copy] = packed


def whole_gram_body(count, group_ref, out_ref):
    gram_body(count, None, group_ref, out_ref)


def multiply(left, right):
    return [[tree_sum([a * right[k][j] for k, a in enumerate(row)]) for j in range(len(right[0]))] for row in left]


def symmetric(left, right):
    size = len(left)
    half = [[tree_sum([a * right[k][j] for k, a in enumerate(left[i])]) for j in range(i + 1)] for i in range(size)]
    return [[half[max(i, j)][min(i, j)] for j in range(size)] for i in range(size)]


def small_inverse(matrix):
    size = len(matrix)
    if size == 1:
        return [[1.0 / matrix[0][0]]]
    half = size // 2
    corner = [row[half:] for row in matrix[:half]]
    rest = [row[half:] for row in matrix[half:]]
    first = small_inverse([row[:half] for row in matrix[:half]])
    across = multiply(first, corner)
    taken = symmetric([list(row) for row in zip(*corner)], across)
    left = [[rest[i][j] - taken[i][j] for j in range(i + 1)] for i in range(half)]
    second = small_inverse([[left[max(i, j)][min(i, j)] for j in range(half)] for i in range(half)])
    product = multiply(across, second)
    added = symmetric(product, [list(row) for row in zip(*across)])
    total = [[first[i][j] + added[i][j] for j in range(i + 1)] for i in range(half)]
    top = [[total[max(i, j)][min(i, j)] for j in range(half)] + [-value for value in product[i]] for i in range(half)]
    bottom = [[-product[j][i] for j in range(half)] + second[i] for i in range(half)]
    return top + bottom


def sweep(matrix, count):
    rows, width = matrix.shape
    size = next(size for size in (8, 4, 2, 1) if count % size == 0)
    tiles = [matrix[i : i + 8, :] for i in range(0, rows, 8)]
    across = lax.broadcasted_iota(jnp.int32, (8, width), 1)
    down = lax.broadcasted_iota(jnp.int32, (8, width), 0)

    def spread(value):
        return jnp.broadcast_to(value, (8, width))

    for k in range(0, count, size):
        at, inner = divmod(k, 8)
        columns = [[tile[:, k + i : k + i + 1] for tile in tiles] for i in range(size)]
        lines = [spread(tiles[at][inner + i : inner + i + 1, :]) for i in range(size)]
        full = [spread(columns[i][at]) for i in range(size)]
        pivots = [
            [spread(full[max(i, j)][inner + min(i, j) : inner + min(i, j) + 1, :]) for j in range(size)]
            for i in range(size)
        ]
        inverse = small_inverse(pivots)
        inside = (across >= k) & (across < k + size)
        lines = [jnp.where(inside, jnp.where(across == k + i, 1.0, 0.0), line) for i, line in enumerate(lines)]
        scaled = [tree_sum([lines[j] * inverse[i][j] for j in range(size)]) for i in range(size)]
        updated = []
        for n, tile in enumerate(tiles):
            if n == at and size == 8:
                value = scaled[0]
            else:
                value = jnp.where(inside, 0.0, tile)
                value = value - tree_sum([columns[i][n] * scaled[i] for i in range(size)])
            if n == at:
                for i in range(size):
                    value = jnp.where(down == inner + i, scaled[i], value)
            updated.append(value)
        tiles = updated
    return jnp.concatenate(tiles, axis=0)


def apply_tiles(tiles_ref, pick_ref, vectors, mask_ref):
    slots, per_row, size, _ = tiles_ref.shape
    mask = eye(size, size)
    images = []
    for slot in range(slots):
        picked = tree_sum(
            [pick_ref[e, slot * per_row : (slot + 1) * per_row, :] * vector for e, vector in enumerate(vectors)]
        )
        parts = [tiles_ref[slot, t] * picked[t : t + 1, :] for t in range(per_row)]
        column = jnp.sum(tree_sum(parts), axis=1, keepdims=True)
        images.append(to_row(column, mask) * mask_ref[slot : slot + 1, :])
    return images


def tail_with(old, row, value):
    down = lax.broadcasted_iota(jnp.int32, (TAIL, old.shape[1]), 0)
    return jnp.where(down == row, value, old)


def finish_step(vectors, tails, own_ref, tiles_ref, pick_ref, mask_ref, own_tail_ref, out_ref):
    slots, rows, width = own_ref.shape
    images = apply_tiles(tiles_ref, pick_ref, vectors, mask_ref)
    total = jnp.zeros((rows + TAIL, width), F32)
    for slot in range(slots):
        tail = tail_with(tails[slot], STEPS, images[slot])
        own_tail_ref[slot] = tail
        total = total + jnp.concatenate([own_ref[slot], tail], axis=0) * images[slot]
    partial = to_row(jnp.sum(total, axis=1, keepdims=True), eye(rows + TAIL, width))
    copies, lines, _ = out_ref.shape
    if lines == 1:
        message = partial
    else:
        pad = [jnp.zeros((lines - slots - 1, width), F32)] if lines > slots + 1 else []
        message = jnp.concatenate([*images, partial, *pad], axis=0)
    out_ref[...] = jnp.broadcast_to(message[None], (copies, lines, width))


def near_peers(subs, paired, doubling):
    me = lax.axis_index("sub")
    first = (1 - me % 2) * 2 if paired else 0
    result = []
    for part, swapped in ((first, 0), (1, 0), (2 - first, 1 if paired else 0)):
        result.append((part, [(peer ^ swapped) ^ me if doubling else peer for peer in range(subs)]))
    return result


def factor_body(
    count, rows, paired, doubling, columns_ref, ghosts_ref, tiles_ref, parts_ref, inverse_ref, start_ref, pick_ref, here_ref, sem
):
    move = pltpu.make_async_copy(tiles_ref, here_ref, sem)
    move.start()
    width = parts_ref.shape[2]
    groups = lane_groups(count, rows, width)
    lanes = width // groups
    packed = lax.fori_loop(1, parts_ref.shape[0], lambda i, held: held + parts_ref[i], parts_ref[0])
    across = lax.broadcasted_iota(jnp.int32, (rows, width), 1)
    down = lax.broadcasted_iota(jnp.int32, (rows, width), 0)
    pieces = [packed]
    for group in range(1, groups):
        pieces.append(pltpu.roll(packed, width - group * lanes, 1))
    gram = jnp.where(across <= count, jnp.concatenate(pieces, axis=0), 0.0)
    swept = sweep(gram, count)
    keep = (down < count) & (across < count)
    inverse_ref[0:rows, :] = jnp.where(keep, swept, 0.0)
    tail_down = lax.broadcasted_iota(jnp.int32, (TAIL, width), 0)
    tail_across = lax.broadcasted_iota(jnp.int32, (TAIL, width), 1)
    inverse_ref[rows : rows + TAIL, :] = jnp.where(
        (tail_down < STEPS) & (tail_across == tail_down + rows), 1.0, 0.0
    )
    squared = jnp.broadcast_to(swept[count : count + 1, count : count + 1], (TAIL, width))
    inverse_norm = lax.rsqrt(squared)
    start = jnp.where(down < count, -swept[:, count : count + 1], jnp.where(down == count, 1.0, 0.0))
    start_ref[0:rows, :] = start
    start_ref[rows : rows + TAIL, :] = jnp.where(tail_down == 0, squared * inverse_norm, inverse_norm)
    slots, per_row = columns_ref.shape
    blocks = (pick_ref.shape[0] - slots) // 3
    places = [
        part * blocks + peer * slots + slot
        for part, peers in near_peers(blocks // slots, paired, doubling)
        for peer in peers
        for slot in range(slots)
    ]
    places += [3 * blocks + slot for slot in range(slots)]
    for slot in range(slots):
        names = columns_ref[slot : slot + 1, :]
        wanted = names + 3 * blocks
        for ghost in range(ghosts_ref.shape[1]):
            wanted = jnp.where(names == slots + ghost, ghosts_ref[:, ghost : ghost + 1], wanted)
        wanted = wanted.astype(F32)
        column = jnp.sum(jnp.where(eye(per_row, per_row), wanted, 0.0), axis=1, keepdims=True)
        column = jnp.broadcast_to(column, (per_row, width)).astype(jnp.int32)
        for at, place in enumerate(places):
            pick_ref[at, slot * per_row : (slot + 1) * per_row, :] = jnp.where(column == place, 1.0, 0.0)
    move.wait()


def start_body(
    start_ref, own_ref, one_ref, group_ref, two_ref, tiles_ref, pick_ref, mask_ref, out_ref, tail_ref, own_tail_ref
):
    slots, rows, width = own_ref.shape
    blocks = group_ref.shape[0]
    coefficients = start_ref[0:rows, :] * start_ref[rows + 1 : rows + 2, :]
    empty = jnp.zeros((TAIL, width), F32)
    vectors = []
    tails = []
    for part in (one_ref, group_ref, two_ref, own_ref):
        for place in range(part.shape[0]):
            vector = jnp.sum(part[place] * coefficients, axis=0, keepdims=True)
            tail = tail_with(empty, 0, vector)
            if len(vectors) < 3 * blocks:
                tail_ref[len(vectors)] = tail
            else:
                tails.append(tail)
            vectors.append(vector)
    finish_step(vectors, tails, own_ref, tiles_ref, pick_ref, mask_ref, own_tail_ref, out_ref)


def project(total_row, inverse, rows, width):
    full = rows + TAIL
    down = lax.broadcasted_iota(jnp.int32, (full, width), 0)
    projected = jnp.sum(inverse * total_row, axis=1, keepdims=True)
    column = jnp.sum(jnp.where(eye(full, width), total_row, 0.0), axis=1, keepdims=True)
    projected = jnp.broadcast_to(projected, (full, width))
    squared = jnp.sum(
        jnp.where(down == rows + STEPS, column, -(column * projected)), axis=0, keepdims=True
    )
    inverse_norm = lax.rsqrt(squared)
    return projected, squared * inverse_norm, inverse_norm, down


def step_body(
    step, count, paired, doubling, every_ref, own_ref, one_ref, group_ref, two_ref, old_ref, old_own_ref, inverse_ref,
    tiles_ref, pick_ref, mask_ref, out_ref, tail_ref, own_tail_ref, history_ref,
):
    slots, rows, width = own_ref.shape
    subs = lax.axis_size("sub")
    last_dom = lax.axis_size("dom") - 1
    total_row = tree_sum([every_ref[i, slots : slots + 1, :] for i in range(every_ref.shape[0])])
    projected, norm, inverse_norm, down = project(total_row, inverse_ref[...], rows, width)
    history_ref[...] = jnp.where(down == count, norm, projected)
    coefficients = jnp.where(down == rows + STEPS, inverse_norm, -(projected * inverse_norm))
    head, foot = coefficients[0:rows], coefficients[rows : rows + TAIL]
    vectors = []
    for part, (offset, peers) in zip((one_ref, group_ref, two_ref), near_peers(subs, paired, doubling)):
        first = jnp.clip(lax.axis_index("dom") + offset - 1, 0, last_dom) * subs
        for place in range(part.shape[0]):
            at = len(vectors)
            old = old_ref[at]
            image = every_ref[first + peers[place // slots], place % slots : place % slots + 1, :]
            vector = jnp.sum(part[place] * head, axis=0, keepdims=True)
            vector = vector + jnp.sum(old * foot, axis=0, keepdims=True) + image * inverse_norm
            if tail_ref is not None:
                tail_ref[at] = tail_with(old, step, vector)
            vectors.append(vector)
    tails = []
    for slot in range(slots):
        old = old_own_ref[slot]
        vector = jnp.sum(own_ref[slot] * head, axis=0, keepdims=True)
        vector = vector + jnp.sum(old * foot, axis=0, keepdims=True)
        tails.append(tail_with(old, step, vector))
        vectors.append(vector)
    finish_step(vectors, tails, own_ref, tiles_ref, pick_ref, mask_ref, own_tail_ref, out_ref)


def last_step_body(step, count, paired, doubling, *refs):
    step_body(step, count, paired, doubling, *refs[:12], None, *refs[12:])


def small_solve(matrix, target):
    size = len(target)
    low = [[None] * size for _ in range(size)]
    inverses = []
    for j in range(size):
        value = matrix[j][j]
        for k in range(j):
            value = value - low[j][k] * low[j][k]
        inverses.append(1.0 / jnp.sqrt(value))
        for i in range(j + 1, size):
            value = matrix[i][j]
            for k in range(j):
                value = value - low[i][k] * low[j][k]
            low[i][j] = value * inverses[j]
    forward = []
    for i in range(size):
        value = target[i]
        for k in range(i):
            value = value - low[i][k] * forward[k]
        forward.append(value * inverses[i])
    back = [None] * size
    for i in reversed(range(size)):
        value = forward[i]
        for k in range(i + 1, size):
            value = value - low[k][i] * back[k]
        back[i] = value * inverses[i]
    return back


def end_body(count, mask_ref, every_ref, own_ref, tail_ref, inverse_ref, start_ref, recycled_ref, *rest):
    histories, (solution_ref, residual_ref) = rest[:-2], rest[-2:]
    slots, rows, width = own_ref.shape
    full = rows + TAIL
    total_row = tree_sum([every_ref[i] for i in range(every_ref.shape[0])])
    projected, norm, _, down = project(total_row, inverse_ref[...], rows, width)
    columns = [history[...] for history in histories]
    columns.append(jnp.where(down == count, norm, projected))
    entries = []
    for j in range(STEPS):
        column = [columns[j][rows + i : rows + i + 1, :] for i in range(j + 1)]
        column.append(columns[j][count : count + 1, :])
        entries.append(column)
    normal = [[None] * STEPS for _ in range(STEPS)]
    for a in range(STEPS):
        for b in range(a + 1):
            shared = range(min(len(entries[a]), len(entries[b])))
            normal[a][b] = tree_sum([entries[a][r] * entries[b][r] for r in shared])
    initial = start_ref[rows : rows + 1, :]
    least = small_solve(normal, [initial * entries[j][0] for j in range(STEPS)])
    image = []
    for r in range(STEPS + 1):
        image.append(tree_sum([entries[j][r] * least[j] for j in range(STEPS) if r < len(entries[j])]))
    start = start_ref[0:rows, :]
    recycled_coefficients = start[0:count] * -1.0
    for j in range(STEPS):
        recycled_coefficients = recycled_coefficients - columns[j][0:count] * least[j]
    ratio = image[STEPS] / norm
    head = jnp.where(down[0:rows] < count, start + columns[-1][0:rows] * ratio, start)
    tail_down = down[0:TAIL]
    solution_tail = jnp.zeros((TAIL, width), F32)
    residual_tail = jnp.zeros((TAIL, width), F32)
    for j in range(STEPS):
        solution_tail = jnp.where(tail_down == j, least[j], solution_tail)
        residual_tail = jnp.where(tail_down == j, entries[-1][j] * ratio - image[j], residual_tail)
    residual_tail = jnp.where(tail_down == STEPS, -ratio, residual_tail)
    for slot in range(slots):
        tail = tail_ref[slot]
        mask = mask_ref[slot : slot + 1, :]
        point = jnp.sum(recycled_ref[:, slot, :] * mask * recycled_coefficients, axis=0, keepdims=True)
        point = point + jnp.sum(tail * solution_tail, axis=0, keepdims=True)
        solution_ref[slot : slot + 1, :] = point
        left = jnp.sum(own_ref[slot] * head, axis=0, keepdims=True)
        left = left + jnp.sum(tail * residual_tail, axis=0, keepdims=True)
        residual_ref[slot : slot + 1, :] = left


def local(load_vector, recycled, images, matrix_tiles, tile_columns, ghost_list, live_counts):
    slots, width = load_vector.shape
    count = recycled.shape[0]
    doms, subs = lax.axis_size("dom"), lax.axis_size("sub")
    devices = doms * subs
    rows = round_up(count + 1, ROW_ALIGN)
    full = rows + TAIL
    per_row = tile_columns.shape[1]
    own, mask = call(
        pack_body,
        "pack",
        [(slots, rows, width), (round_up(slots, 8), width)],
        [SMEM, VMEM, VMEM],
    )(live_counts, load_vector, images)
    each = rows // lane_groups(count, rows, width)
    paired = subs % 2 == 0
    doubling = subs == 4

    def turn(value, bit):
        return lax.ppermute(value, "sub", [(i, i ^ bit) for i in range(subs)])

    if doubling:
        with jax.named_scope("inner"):
            inner = turn(own, 1)
        with jax.named_scope("outer"):
            outer = turn(own, 2)
        with jax.named_scope("corner"):
            corner = turn(outer, 1)
        (held,) = call(first_gram_body, "first_gram", [(rows, width)], [VMEM] * 3)(own, inner, outer)
        corner, held = lax.optimization_barrier((corner, held))
        (group,) = call(join_body, "join", [(subs * slots, rows, width)], [VMEM] * 4)(own, inner, outer, corner)
        (grams,) = call(functools.partial(gram_body, count), "gram", [(doms, each, width)], [VMEM] * 2)(held, corner)
    else:
        group = lax.all_gather(own, "sub", axis=0, tiled=True)
        (grams,) = call(functools.partial(whole_gram_body, count), "gram", [(doms, each, width)], [VMEM])(group)
    with jax.named_scope("collect"):
        parts = lax.all_to_all(grams, "dom", 0, 0)
    if paired:
        pairs = []
        for d in range(doms):
            for s in range(subs):
                to = d + 1 if s % 2 else d - 1
                if 0 <= to < doms:
                    pairs.append((d * subs + s, to * subs + s))
        with jax.named_scope("pair"):
            one = lax.ppermute(group, AXES, pairs)
        one, parts = lax.optimization_barrier((one, parts))
        with jax.named_scope("swap"):
            two = turn(one, 1)
    else:
        up = [(i, i + 1) for i in range(doms - 1)]
        one = lax.ppermute(group, "dom", up)
        two = lax.ppermute(group, "dom", [(j, i) for i, j in up])
    lines = round_up(slots + 1, 4)
    near = 3 * group.shape[0]
    inverse, start, pick, tiles = call(
        functools.partial(factor_body, count, rows, paired, doubling),
        "factor",
        [(full, width), (full, width), (near + slots, slots * per_row, width), matrix_tiles.shape],
        [VMEM, VMEM, HBM, VMEM],
        [pltpu.SemaphoreType.DMA],
    )(tile_columns, ghost_list, pltpu.with_memory_space_constraint(matrix_tiles, pltpu.HBM), parts)
    message, tails, own_tails = call(
        start_body,
        "start",
        [(devices, lines, width), (near, TAIL, width), (slots, TAIL, width)],
        [VMEM] * 8,
    )(start, own, one, group, two, tiles, pick, mask)
    histories = []
    for step in range(1, STEPS):
        every = lax.all_to_all(message, AXES, 0, 0)
        last = step == STEPS - 1
        sent = 1 if last else lines
        results = call(
            functools.partial(last_step_body if last else step_body, step, count, paired, doubling),
            f"step{step}",
            [(devices, sent, width)]
            + ([] if last else [(near, TAIL, width)])
            + [(slots, TAIL, width), (full, width)],
            [VMEM] * 11,
        )(every, own, one, group, two, tails, own_tails, inverse, tiles, pick, mask)
        message, own_tails, history = results[0], results[-2], results[-1]
        tails = tails if last else results[1]
        histories.append(history)
    every = lax.all_to_all(message, AXES, 0, 0)
    return tuple(
        call(
            functools.partial(end_body, count),
            "end",
            [(slots, width), (slots, width)],
            [VMEM] * (7 + len(histories)),
        )(mask, every, own, own_tails, inverse, start, recycled, *histories)
    )


def solution(mesh):
    return jax.shard_map(
        local,
        mesh=mesh,
        in_specs=(
            P(("dom", "sub"), None),
            P(None, ("dom", "sub"), None),
            P(None, ("dom", "sub"), None),
            P(("dom", "sub"), None, None, None),
            P(("dom", "sub"), None),
            P(("dom", "sub"), None),
            P(("dom", "sub")),
        ),
        out_specs=(P(("dom", "sub"), None), P(("dom", "sub"), None)),
        check_vma=False,
    )
```

```python
import functools

import jax
import jax.numpy as jnp
from jax import lax
from jax.experimental import pallas as pl
from jax.experimental.pallas import tpu as pltpu
from jax.sharding import PartitionSpec as P

STEPS = 3
TAIL = 8
ROW_ALIGN = 8
AXES = ("dom", "sub")
VMEM = pl.BlockSpec(memory_space=pltpu.VMEM)
SMEM = pl.BlockSpec(memory_space=pltpu.SMEM)
HBM = pl.BlockSpec(memory_space=pltpu.HBM)
F32 = jnp.float32


def call(body, name, outs, specs, scratch=(), work=10_000_000):
    return pl.pallas_call(
        body,
        name=name,
        out_shape=[jax.ShapeDtypeStruct(shape, F32) for shape in outs],
        in_specs=specs,
        out_specs=[VMEM] * len(outs),
        scratch_shapes=list(scratch),
        cost_estimate=pl.CostEstimate(flops=work, bytes_accessed=1 << 20, transcendentals=0),
        compiler_params=pltpu.CompilerParams(vmem_limit_bytes=16 * 1024 * 1024),
    )


def round_up(value, step):
    return -(-value // step) * step


def eye(rows, lanes):
    down = lax.broadcasted_iota(jnp.int32, (rows, lanes), 0)
    across = lax.broadcasted_iota(jnp.int32, (rows, lanes), 1)
    return down == across


def to_row(column, mask):
    return jnp.sum(jnp.where(mask, column, 0.0), axis=0, keepdims=True)


def tree_sum(parts):
    while len(parts) > 1:
        pairs = [parts[i] + parts[i + 1] for i in range(0, len(parts) - 1, 2)]
        parts = pairs + parts[len(parts) - len(parts) % 2 :]
    return parts[0]


def pack_body(live_ref, load_ref, images_ref, own_ref, mask_ref):
    count, slots, width = images_ref.shape
    rows = own_ref.shape[1]
    line = lax.broadcasted_iota(jnp.int32, mask_ref.shape, 0)
    mask_ref[...] = jnp.where(line < live_ref[0], 1.0, 0.0).astype(F32)
    for slot in range(slots):
        mask = jnp.where(slot < live_ref[0], 1.0, 0.0).astype(F32)
        own_ref[slot, 0:count, :] = images_ref[:, slot, :] * mask
        own_ref[slot, count : count + 1, :] = load_ref[slot : slot + 1, :] * mask
        own_ref[slot, count + 1 : rows, :] = jnp.zeros((rows - count - 1, width), F32)


def join_body(*refs):
    place = 0
    for part in refs[:-1]:
        for block in range(part.shape[0]):
            refs[-1][place] = part[block]
            place += 1


def lane_groups(count, rows, width):
    groups = width // (count + 1)
    if rows % groups == 0 and (rows // groups) % ROW_ALIGN == 0:
        return groups
    return 1


def gram_of(*refs):
    products = []
    for ref in refs:
        for block in range(ref.shape[0]):
            part = ref[block]
            products.append(
                lax.dot_general(
                    part, part, (((1,), (1,)), ((), ())),
                    precision=lax.Precision.HIGHEST, preferred_element_type=F32,
                )
            )
    rows, width = refs[0].shape[1:]
    return jnp.concatenate([tree_sum(products), jnp.zeros((rows, width - rows), F32)], axis=1)


def first_gram_body(*refs):
    refs[-1][...] = gram_of(*refs[:-1])


def gram_body(count, held_ref, group_ref, out_ref):
    rows, width = group_ref.shape[1:]
    gram = gram_of(group_ref)
    if held_ref is not None:
        gram = gram + held_ref[...]
    groups = lane_groups(count, rows, width)
    each, lanes = rows // groups, width // groups
    packed = gram[0:each]
    for group in range(1, groups):
        packed = packed + pltpu.roll(gram[group * each : (group + 1) * each], group * lanes, 1)
    for copy in range(out_ref.shape[0]):
        out_ref[copy] = packed


def whole_gram_body(count, group_ref, out_ref):
    gram_body(count, None, group_ref, out_ref)


def multiply(left, right):
    return [[tree_sum([a * right[k][j] for k, a in enumerate(row)]) for j in range(len(right[0]))] for row in left]


def symmetric(left, right):
    size = len(left)
    half = [[tree_sum([a * right[k][j] for k, a in enumerate(left[i])]) for j in range(i + 1)] for i in range(size)]
    return [[half[max(i, j)][min(i, j)] for j in range(size)] for i in range(size)]


def small_inverse(matrix):
    size = len(matrix)
    if size == 1:
        return [[1.0 / matrix[0][0]]]
    half = size // 2
    corner = [row[half:] for row in matrix[:half]]
    rest = [row[half:] for row in matrix[half:]]
    first = small_inverse([row[:half] for row in matrix[:half]])
    across = multiply(first, corner)
    taken = symmetric([list(row) for row in zip(*corner)], across)
    left = [[rest[i][j] - taken[i][j] for j in range(i + 1)] for i in range(half)]
    second = small_inverse([[left[max(i, j)][min(i, j)] for j in range(half)] for i in range(half)])
    product = multiply(across, second)
    added = symmetric(product, [list(row) for row in zip(*across)])
    total = [[first[i][j] + added[i][j] for j in range(i + 1)] for i in range(half)]
    top = [[total[max(i, j)][min(i, j)] for j in range(half)] + [-value for value in product[i]] for i in range(half)]
    bottom = [[-product[j][i] for j in range(half)] + second[i] for i in range(half)]
    return top + bottom


def sweep(matrix, count):
    rows, width = matrix.shape
    size = next(size for size in (8, 4, 2, 1) if count % size == 0)
    tiles = [matrix[i : i + 8, :] for i in range(0, rows, 8)]
    across = lax.broadcasted_iota(jnp.int32, (8, width), 1)
    down = lax.broadcasted_iota(jnp.int32, (8, width), 0)

    def spread(value):
        return jnp.broadcast_to(value, (8, width))

    for k in range(0, count, size):
        at, inner = divmod(k, 8)
        columns = [[tile[:, k + i : k + i + 1] for tile in tiles] for i in range(size)]
        lines = [spread(tiles[at][inner + i : inner + i + 1, :]) for i in range(size)]
        full = [spread(columns[i][at]) for i in range(size)]
        pivots = [
            [spread(full[max(i, j)][inner + min(i, j) : inner + min(i, j) + 1, :]) for j in range(size)]
            for i in range(size)
        ]
        inverse = small_inverse(pivots)
        inside = (across >= k) & (across < k + size)
        lines = [jnp.where(inside, jnp.where(across == k + i, 1.0, 0.0), line) for i, line in enumerate(lines)]
        scaled = [tree_sum([lines[j] * inverse[i][j] for j in range(size)]) for i in range(size)]
        updated = []
        for n, tile in enumerate(tiles):
            if n == at and size == 8:
                value = scaled[0]
            else:
                value = jnp.where(inside, 0.0, tile)
                value = value - tree_sum([columns[i][n] * scaled[i] for i in range(size)])
            if n == at:
                for i in range(size):
                    value = jnp.where(down == inner + i, scaled[i], value)
            updated.append(value)
        tiles = updated
    return jnp.concatenate(tiles, axis=0)


def apply_tiles(tiles_ref, pick_ref, vectors, mask_ref):
    slots, per_row, size, _ = tiles_ref.shape
    mask = eye(size, size)
    images = []
    for slot in range(slots):
        picked = tree_sum(
            [pick_ref[e, slot * per_row : (slot + 1) * per_row, :] * vector for e, vector in enumerate(vectors)]
        )
        parts = [tiles_ref[slot, t] * picked[t : t + 1, :] for t in range(per_row)]
        column = jnp.sum(tree_sum(parts), axis=1, keepdims=True)
        images.append(to_row(column, mask) * mask_ref[slot : slot + 1, :])
    return images


def tail_with(old, row, value):
    down = lax.broadcasted_iota(jnp.int32, (TAIL, old.shape[1]), 0)
    return jnp.where(down == row, value, old)


def finish_step(vectors, tails, own_ref, tiles_ref, pick_ref, mask_ref, own_tail_ref, out_ref):
    slots, rows, width = own_ref.shape
    images = apply_tiles(tiles_ref, pick_ref, vectors, mask_ref)
    total = jnp.zeros((rows + TAIL, width), F32)
    for slot in range(slots):
        tail = tail_with(tails[slot], STEPS, images[slot])
        own_tail_ref[slot] = tail
        total = total + jnp.concatenate([own_ref[slot], tail], axis=0) * images[slot]
    partial = to_row(jnp.sum(total, axis=1, keepdims=True), eye(rows + TAIL, width))
    copies, lines, _ = out_ref.shape
    if lines == 1:
        message = partial
    else:
        pad = [jnp.zeros((lines - slots - 1, width), F32)] if lines > slots + 1 else []
        message = jnp.concatenate([*images, partial, *pad], axis=0)
    out_ref[...] = jnp.broadcast_to(message[None], (copies, lines, width))


def near_peers(subs, paired, doubling):
    me = lax.axis_index("sub")
    first = (me + lax.axis_index("dom") + 1) % 2 * 2 if paired else 0
    result = []
    for part, swapped in ((first, 0), (1, 0), (2 - first, 1 if paired else 0)):
        result.append((part, [(peer ^ swapped) ^ me if doubling else peer for peer in range(subs)]))
    return result


def factor_body(
    count, rows, paired, doubling, columns_ref, ghosts_ref, tiles_ref, parts_ref, inverse_ref, start_ref, pick_ref, here_ref, sem
):
    move = pltpu.make_async_copy(tiles_ref, here_ref, sem)
    move.start()
    width = parts_ref.shape[2]
    groups = lane_groups(count, rows, width)
    lanes = width // groups
    packed = lax.fori_loop(1, parts_ref.shape[0], lambda i, held: held + parts_ref[i], parts_ref[0])
    across = lax.broadcasted_iota(jnp.int32, (rows, width), 1)
    down = lax.broadcasted_iota(jnp.int32, (rows, width), 0)
    pieces = [packed]
    for group in range(1, groups):
        pieces.append(pltpu.roll(packed, width - group * lanes, 1))
    gram = jnp.where(across <= count, jnp.concatenate(pieces, axis=0), 0.0)
    swept = sweep(gram, count)
    keep = (down < count) & (across < count)
    inverse_ref[0:rows, :] = jnp.where(keep, swept, 0.0)
    tail_down = lax.broadcasted_iota(jnp.int32, (TAIL, width), 0)
    tail_across = lax.broadcasted_iota(jnp.int32, (TAIL, width), 1)
    inverse_ref[rows : rows + TAIL, :] = jnp.where(
        (tail_down < STEPS) & (tail_across == tail_down + rows), 1.0, 0.0
    )
    squared = jnp.broadcast_to(swept[count : count + 1, count : count + 1], (TAIL, width))
    inverse_norm = lax.rsqrt(squared)
    start = jnp.where(down < count, -swept[:, count : count + 1], jnp.where(down == count, 1.0, 0.0))
    start_ref[0:rows, :] = start
    start_ref[rows : rows + TAIL, :] = jnp.where(tail_down == 0, squared * inverse_norm, inverse_norm)
    slots, per_row = columns_ref.shape
    blocks = (pick_ref.shape[0] - slots) // 3
    places = [
        part * blocks + peer * slots + slot
        for part, peers in near_peers(blocks // slots, paired, doubling)
        for peer in peers
        for slot in range(slots)
    ]
    places += [3 * blocks + slot for slot in range(slots)]
    for slot in range(slots):
        names = columns_ref[slot : slot + 1, :]
        wanted = names + 3 * blocks
        for ghost in range(ghosts_ref.shape[1]):
            wanted = jnp.where(names == slots + ghost, ghosts_ref[:, ghost : ghost + 1], wanted)
        wanted = wanted.astype(F32)
        column = jnp.sum(jnp.where(eye(per_row, per_row), wanted, 0.0), axis=1, keepdims=True)
        column = jnp.broadcast_to(column, (per_row, width)).astype(jnp.int32)
        for at, place in enumerate(places):
            pick_ref[at, slot * per_row : (slot + 1) * per_row, :] = jnp.where(column == place, 1.0, 0.0)
    move.wait()


def start_body(
    start_ref, own_ref, one_ref, group_ref, two_ref, tiles_ref, pick_ref, mask_ref, out_ref, tail_ref, own_tail_ref
):
    slots, rows, width = own_ref.shape
    blocks = group_ref.shape[0]
    coefficients = start_ref[0:rows, :] * start_ref[rows + 1 : rows + 2, :]
    empty = jnp.zeros((TAIL, width), F32)
    vectors = []
    tails = []
    for part in (one_ref, group_ref, two_ref, own_ref):
        for place in range(part.shape[0]):
            vector = jnp.sum(part[place] * coefficients, axis=0, keepdims=True)
            tail = tail_with(empty, 0, vector)
            if len(vectors) < 3 * blocks:
                tail_ref[len(vectors)] = tail
            else:
                tails.append(tail)
            vectors.append(vector)
    finish_step(vectors, tails, own_ref, tiles_ref, pick_ref, mask_ref, own_tail_ref, out_ref)


def project(total_row, inverse, rows, width):
    full = rows + TAIL
    down = lax.broadcasted_iota(jnp.int32, (full, width), 0)
    projected = jnp.sum(inverse * total_row, axis=1, keepdims=True)
    column = jnp.sum(jnp.where(eye(full, width), total_row, 0.0), axis=1, keepdims=True)
    projected = jnp.broadcast_to(projected, (full, width))
    squared = jnp.sum(
        jnp.where(down == rows + STEPS, column, -(column * projected)), axis=0, keepdims=True
    )
    inverse_norm = lax.rsqrt(squared)
    return projected, squared * inverse_norm, inverse_norm, down


def step_body(
    step, count, paired, doubling, every_ref, own_ref, one_ref, group_ref, two_ref, old_ref, old_own_ref, inverse_ref,
    tiles_ref, pick_ref, mask_ref, out_ref, tail_ref, own_tail_ref, history_ref,
):
    slots, rows, width = own_ref.shape
    subs = lax.axis_size("sub")
    last_dom = lax.axis_size("dom") - 1
    total_row = tree_sum([every_ref[i, slots : slots + 1, :] for i in range(every_ref.shape[0])])
    projected, norm, inverse_norm, down = project(total_row, inverse_ref[...], rows, width)
    history_ref[...] = jnp.where(down == count, norm, projected)
    coefficients = jnp.where(down == rows + STEPS, inverse_norm, -(projected * inverse_norm))
    head, foot = coefficients[0:rows], coefficients[rows : rows + TAIL]
    vectors = []
    for part, (offset, peers) in zip((one_ref, group_ref, two_ref), near_peers(subs, paired, doubling)):
        first = jnp.clip(lax.axis_index("dom") + offset - 1, 0, last_dom) * subs
        for place in range(part.shape[0]):
            at = len(vectors)
            old = old_ref[at]
            image = every_ref[first + peers[place // slots], place % slots : place % slots + 1, :]
            vector = jnp.sum(part[place] * head, axis=0, keepdims=True)
            vector = vector + jnp.sum(old * foot, axis=0, keepdims=True) + image * inverse_norm
            if tail_ref is not None:
                tail_ref[at] = tail_with(old, step, vector)
            vectors.append(vector)
    tails = []
    for slot in range(slots):
        old = old_own_ref[slot]
        vector = jnp.sum(own_ref[slot] * head, axis=0, keepdims=True)
        vector = vector + jnp.sum(old * foot, axis=0, keepdims=True)
        tails.append(tail_with(old, step, vector))
        vectors.append(vector)
    finish_step(vectors, tails, own_ref, tiles_ref, pick_ref, mask_ref, own_tail_ref, out_ref)


def last_step_body(step, count, paired, doubling, *refs):
    step_body(step, count, paired, doubling, *refs[:12], None, *refs[12:])


def small_solve(matrix, target):
    size = len(target)
    low = [[None] * size for _ in range(size)]
    inverses = []
    for j in range(size):
        value = matrix[j][j]
        for k in range(j):
            value = value - low[j][k] * low[j][k]
        inverses.append(1.0 / jnp.sqrt(value))
        for i in range(j + 1, size):
            value = matrix[i][j]
            for k in range(j):
                value = value - low[i][k] * low[j][k]
            low[i][j] = value * inverses[j]
    forward = []
    for i in range(size):
        value = target[i]
        for k in range(i):
            value = value - low[i][k] * forward[k]
        forward.append(value * inverses[i])
    back = [None] * size
    for i in reversed(range(size)):
        value = forward[i]
        for k in range(i + 1, size):
            value = value - low[k][i] * back[k]
        back[i] = value * inverses[i]
    return back


def end_body(count, mask_ref, every_ref, own_ref, tail_ref, inverse_ref, start_ref, recycled_ref, *rest):
    histories, (solution_ref, residual_ref) = rest[:-2], rest[-2:]
    slots, rows, width = own_ref.shape
    full = rows + TAIL
    total_row = tree_sum([every_ref[i] for i in range(every_ref.shape[0])])
    projected, norm, _, down = project(total_row, inverse_ref[...], rows, width)
    columns = [history[...] for history in histories]
    columns.append(jnp.where(down == count, norm, projected))
    entries = []
    for j in range(STEPS):
        column = [columns[j][rows + i : rows + i + 1, :] for i in range(j + 1)]
        column.append(columns[j][count : count + 1, :])
        entries.append(column)
    normal = [[None] * STEPS for _ in range(STEPS)]
    for a in range(STEPS):
        for b in range(a + 1):
            shared = range(min(len(entries[a]), len(entries[b])))
            normal[a][b] = tree_sum([entries[a][r] * entries[b][r] for r in shared])
    initial = start_ref[rows : rows + 1, :]
    least = small_solve(normal, [initial * entries[j][0] for j in range(STEPS)])
    image = []
    for r in range(STEPS + 1):
        image.append(tree_sum([entries[j][r] * least[j] for j in range(STEPS) if r < len(entries[j])]))
    start = start_ref[0:rows, :]
    recycled_coefficients = start[0:count] * -1.0
    for j in range(STEPS):
        recycled_coefficients = recycled_coefficients - columns[j][0:count] * least[j]
    ratio = image[STEPS] / norm
    head = jnp.where(down[0:rows] < count, start + columns[-1][0:rows] * ratio, start)
    tail_down = down[0:TAIL]
    solution_tail = jnp.zeros((TAIL, width), F32)
    residual_tail = jnp.zeros((TAIL, width), F32)
    for j in range(STEPS):
        solution_tail = jnp.where(tail_down == j, least[j], solution_tail)
        residual_tail = jnp.where(tail_down == j, entries[-1][j] * ratio - image[j], residual_tail)
    residual_tail = jnp.where(tail_down == STEPS, -ratio, residual_tail)
    for slot in range(slots):
        tail = tail_ref[slot]
        mask = mask_ref[slot : slot + 1, :]
        point = jnp.sum(recycled_ref[:, slot, :] * mask * recycled_coefficients, axis=0, keepdims=True)
        point = point + jnp.sum(tail * solution_tail, axis=0, keepdims=True)
        solution_ref[slot : slot + 1, :] = point
        left = jnp.sum(own_ref[slot] * head, axis=0, keepdims=True)
        left = left + jnp.sum(tail * residual_tail, axis=0, keepdims=True)
        residual_ref[slot : slot + 1, :] = left


def local(load_vector, recycled, images, matrix_tiles, tile_columns, ghost_list, live_counts):
    slots, width = load_vector.shape
    count = recycled.shape[0]
    doms, subs = lax.axis_size("dom"), lax.axis_size("sub")
    devices = doms * subs
    rows = round_up(count + 1, ROW_ALIGN)
    full = rows + TAIL
    per_row = tile_columns.shape[1]
    own, mask = call(
        pack_body,
        "pack",
        [(slots, rows, width), (round_up(slots, 8), width)],
        [SMEM, VMEM, VMEM],
    )(live_counts, load_vector, images)
    each = rows // lane_groups(count, rows, width)
    paired = subs % 2 == 0
    doubling = subs == 4

    def turn(value, bit):
        return lax.ppermute(value, "sub", [(i, i ^ bit) for i in range(subs)])

    if doubling:
        with jax.named_scope("inner"):
            inner = turn(own, 1)
        with jax.named_scope("outer"):
            outer = turn(own, 2)
        with jax.named_scope("corner"):
            corner = turn(own, 3)
        (held,) = call(first_gram_body, "first_gram", [(rows, width)], [VMEM] * 3)(own, inner, outer)
        corner, held = lax.optimization_barrier((corner, held))
        (group,) = call(join_body, "join", [(subs * slots, rows, width)], [VMEM] * 4)(own, inner, outer, corner)
        (grams,) = call(functools.partial(gram_body, count), "gram", [(doms, each, width)], [VMEM] * 2)(held, corner)
    else:
        group = lax.all_gather(own, "sub", axis=0, tiled=True)
        (grams,) = call(functools.partial(whole_gram_body, count), "gram", [(doms, each, width)], [VMEM])(group)
    with jax.named_scope("collect"):
        parts = lax.all_to_all(grams, "dom", 0, 0)
    if paired:
        pairs = []
        for d in range(doms):
            for s in range(subs):
                to = d + 1 if (s + d) % 2 == 0 else d - 1
                if 0 <= to < doms:
                    pairs.append((d * subs + s, to * subs + s))
        with jax.named_scope("pair"):
            one = lax.ppermute(group, AXES, pairs)
        one, parts = lax.optimization_barrier((one, parts))
        with jax.named_scope("swap"):
            two = turn(one, 1)
    else:
        up = [(i, i + 1) for i in range(doms - 1)]
        one = lax.ppermute(group, "dom", up)
        two = lax.ppermute(group, "dom", [(j, i) for i, j in up])
    lines = round_up(slots + 1, 4)
    near = 3 * group.shape[0]
    inverse, start, pick, tiles = call(
        functools.partial(factor_body, count, rows, paired, doubling),
        "factor",
        [(full, width), (full, width), (near + slots, slots * per_row, width), matrix_tiles.shape],
        [VMEM, VMEM, HBM, VMEM],
        [pltpu.SemaphoreType.DMA],
    )(tile_columns, ghost_list, pltpu.with_memory_space_constraint(matrix_tiles, pltpu.HBM), parts)
    message, tails, own_tails = call(
        start_body,
        "start",
        [(devices, lines, width), (near, TAIL, width), (slots, TAIL, width)],
        [VMEM] * 8,
    )(start, own, one, group, two, tiles, pick, mask)
    histories = []
    for step in range(1, STEPS):
        every = lax.all_to_all(message, AXES, 0, 0)
        last = step == STEPS - 1
        sent = 1 if last else lines
        results = call(
            functools.partial(last_step_body if last else step_body, step, count, paired, doubling),
            f"step{step}",
            [(devices, sent, width)]
            + ([] if last else [(near, TAIL, width)])
            + [(slots, TAIL, width), (full, width)],
            [VMEM] * 11,
        )(every, own, one, group, two, tails, own_tails, inverse, tiles, pick, mask)
        message, own_tails, history = results[0], results[-2], results[-1]
        tails = tails if last else results[1]
        histories.append(history)
    every = lax.all_to_all(message, AXES, 0, 0)
    return tuple(
        call(
            functools.partial(end_body, count),
            "end",
            [(slots, width), (slots, width)],
            [VMEM] * (7 + len(histories)),
        )(mask, every, own, own_tails, inverse, start, recycled, *histories)
    )


def solution(mesh):
    return jax.shard_map(
        local,
        mesh=mesh,
        in_specs=(
            P(("dom", "sub"), None),
            P(None, ("dom", "sub"), None),
            P(None, ("dom", "sub"), None),
            P(("dom", "sub"), None, None, None),
            P(("dom", "sub"), None),
            P(("dom", "sub"), None),
            P(("dom", "sub")),
        ),
        out_specs=(P(("dom", "sub"), None), P(("dom", "sub"), None)),
        check_vma=False,
    )
```

```python
import functools

import jax
import jax.numpy as jnp
from jax import lax
from jax.experimental import pallas as pl
from jax.experimental.pallas import tpu as pltpu
from jax.sharding import PartitionSpec as P

STEPS = 3
TAIL = 8
ROW_ALIGN = 8
AXES = ("dom", "sub")
VMEM = pl.BlockSpec(memory_space=pltpu.VMEM)
SMEM = pl.BlockSpec(memory_space=pltpu.SMEM)
HBM = pl.BlockSpec(memory_space=pltpu.HBM)
F32 = jnp.float32


def call(body, name, outs, specs, scratch=(), work=10_000_000):
    return pl.pallas_call(
        body,
        name=name,
        out_shape=[jax.ShapeDtypeStruct(shape, F32) for shape in outs],
        in_specs=specs,
        out_specs=[VMEM] * len(outs),
        scratch_shapes=list(scratch),
        cost_estimate=pl.CostEstimate(flops=work, bytes_accessed=1 << 20, transcendentals=0),
        compiler_params=pltpu.CompilerParams(vmem_limit_bytes=16 * 1024 * 1024),
    )


def round_up(value, step):
    return -(-value // step) * step


def eye(rows, lanes):
    down = lax.broadcasted_iota(jnp.int32, (rows, lanes), 0)
    across = lax.broadcasted_iota(jnp.int32, (rows, lanes), 1)
    return down == across


def to_row(column, mask):
    return jnp.sum(jnp.where(mask, column, 0.0), axis=0, keepdims=True)


def tree_sum(parts):
    while len(parts) > 1:
        pairs = [parts[i] + parts[i + 1] for i in range(0, len(parts) - 1, 2)]
        parts = pairs + parts[len(parts) - len(parts) % 2 :]
    return parts[0]


def pack_body(live_ref, load_ref, images_ref, own_ref, mask_ref):
    count, slots, width = images_ref.shape
    rows = own_ref.shape[1]
    line = lax.broadcasted_iota(jnp.int32, mask_ref.shape, 0)
    mask_ref[...] = jnp.where(line < live_ref[0], 1.0, 0.0).astype(F32)
    for slot in range(slots):
        mask = jnp.where(slot < live_ref[0], 1.0, 0.0).astype(F32)
        own_ref[slot, 0:count, :] = images_ref[:, slot, :] * mask
        own_ref[slot, count : count + 1, :] = load_ref[slot : slot + 1, :] * mask
        own_ref[slot, count + 1 : rows, :] = jnp.zeros((rows - count - 1, width), F32)


def join_body(*refs):
    place = 0
    for part in refs[:-1]:
        for block in range(part.shape[0]):
            refs[-1][place] = part[block]
            place += 1


def lane_groups(count, rows, width):
    groups = width // (count + 1)
    if rows % groups == 0 and (rows // groups) % ROW_ALIGN == 0:
        return groups
    return 1


def gram_of(*refs):
    products = []
    for ref in refs:
        for block in range(ref.shape[0]):
            part = ref[block]
            products.append(
                lax.dot_general(
                    part, part, (((1,), (1,)), ((), ())),
                    precision=lax.Precision.HIGHEST, preferred_element_type=F32,
                )
            )
    rows, width = refs[0].shape[1:]
    return jnp.concatenate([tree_sum(products), jnp.zeros((rows, width - rows), F32)], axis=1)


def first_gram_body(*refs):
    refs[-1][...] = gram_of(*refs[:-1])


def gram_body(count, held_ref, *refs):
    parts, out_ref = refs[:-1], refs[-1]
    rows, width = parts[0].shape[1:]
    gram = gram_of(*parts)
    if held_ref is not None:
        gram = gram + held_ref[...]
    groups = lane_groups(count, rows, width)
    each, lanes = rows // groups, width // groups
    packed = gram[0:each]
    for group in range(1, groups):
        packed = packed + pltpu.roll(gram[group * each : (group + 1) * each], group * lanes, 1)
    for copy in range(out_ref.shape[0]):
        out_ref[copy] = packed


def whole_gram_body(count, group_ref, out_ref):
    gram_body(count, None, group_ref, out_ref)


def multiply(left, right):
    return [[tree_sum([a * right[k][j] for k, a in enumerate(row)]) for j in range(len(right[0]))] for row in left]


def symmetric(left, right):
    size = len(left)
    half = [[tree_sum([a * right[k][j] for k, a in enumerate(left[i])]) for j in range(i + 1)] for i in range(size)]
    return [[half[max(i, j)][min(i, j)] for j in range(size)] for i in range(size)]


def small_inverse(matrix):
    size = len(matrix)
    if size == 1:
        return [[1.0 / matrix[0][0]]]
    half = size // 2
    corner = [row[half:] for row in matrix[:half]]
    rest = [row[half:] for row in matrix[half:]]
    first = small_inverse([row[:half] for row in matrix[:half]])
    across = multiply(first, corner)
    taken = symmetric([list(row) for row in zip(*corner)], across)
    left = [[rest[i][j] - taken[i][j] for j in range(i + 1)] for i in range(half)]
    second = small_inverse([[left[max(i, j)][min(i, j)] for j in range(half)] for i in range(half)])
    product = multiply(across, second)
    added = symmetric(product, [list(row) for row in zip(*across)])
    total = [[first[i][j] + added[i][j] for j in range(i + 1)] for i in range(half)]
    top = [[total[max(i, j)][min(i, j)] for j in range(half)] + [-value for value in product[i]] for i in range(half)]
    bottom = [[-product[j][i] for j in range(half)] + second[i] for i in range(half)]
    return top + bottom


def sweep(matrix, count):
    rows, width = matrix.shape
    size = next(size for size in (8, 4, 2, 1) if count % size == 0)
    tiles = [matrix[i : i + 8, :] for i in range(0, rows, 8)]
    across = lax.broadcasted_iota(jnp.int32, (8, width), 1)
    down = lax.broadcasted_iota(jnp.int32, (8, width), 0)

    def spread(value):
        return jnp.broadcast_to(value, (8, width))

    for k in range(0, count, size):
        at, inner = divmod(k, 8)
        columns = [[tile[:, k + i : k + i + 1] for tile in tiles] for i in range(size)]
        lines = [spread(tiles[at][inner + i : inner + i + 1, :]) for i in range(size)]
        full = [spread(columns[i][at]) for i in range(size)]
        pivots = [
            [spread(full[max(i, j)][inner + min(i, j) : inner + min(i, j) + 1, :]) for j in range(size)]
            for i in range(size)
        ]
        inverse = small_inverse(pivots)
        inside = (across >= k) & (across < k + size)
        lines = [jnp.where(inside, jnp.where(across == k + i, 1.0, 0.0), line) for i, line in enumerate(lines)]
        scaled = [tree_sum([lines[j] * inverse[i][j] for j in range(size)]) for i in range(size)]
        updated = []
        for n, tile in enumerate(tiles):
            if n == at and size == 8:
                value = scaled[0]
            else:
                value = jnp.where(inside, 0.0, tile)
                value = value - tree_sum([columns[i][n] * scaled[i] for i in range(size)])
            if n == at:
                for i in range(size):
                    value = jnp.where(down == inner + i, scaled[i], value)
            updated.append(value)
        tiles = updated
    return jnp.concatenate(tiles, axis=0)


def apply_tiles(tiles_ref, pick_ref, vectors, mask_ref):
    slots, per_row, size, _ = tiles_ref.shape
    mask = eye(size, size)
    images = []
    for slot in range(slots):
        picked = tree_sum(
            [pick_ref[e, slot * per_row : (slot + 1) * per_row, :] * vector for e, vector in enumerate(vectors)]
        )
        parts = [tiles_ref[slot, t] * picked[t : t + 1, :] for t in range(per_row)]
        column = jnp.sum(tree_sum(parts), axis=1, keepdims=True)
        images.append(to_row(column, mask) * mask_ref[slot : slot + 1, :])
    return images


def tail_with(old, row, value):
    down = lax.broadcasted_iota(jnp.int32, (TAIL, old.shape[1]), 0)
    return jnp.where(down == row, value, old)


def finish_step(vectors, tails, own_ref, tiles_ref, pick_ref, mask_ref, own_tail_ref, out_ref):
    slots, rows, width = own_ref.shape
    images = apply_tiles(tiles_ref, pick_ref, vectors, mask_ref)
    total = jnp.zeros((rows + TAIL, width), F32)
    for slot in range(slots):
        tail = tail_with(tails[slot], STEPS, images[slot])
        own_tail_ref[slot] = tail
        total = total + jnp.concatenate([own_ref[slot], tail], axis=0) * images[slot]
    partial = to_row(jnp.sum(total, axis=1, keepdims=True), eye(rows + TAIL, width))
    copies, lines, _ = out_ref.shape
    if lines == 1:
        message = partial
    else:
        pad = [jnp.zeros((lines - slots - 1, width), F32)] if lines > slots + 1 else []
        message = jnp.concatenate([*images, partial, *pad], axis=0)
    out_ref[...] = jnp.broadcast_to(message[None], (copies, lines, width))


def near_peers(subs, paired, doubling):
    me = lax.axis_index("sub")
    first = (me + lax.axis_index("dom") + 1) % 2 * 2 if paired else 0
    result = []
    for part, swapped in ((first, 0), (1, 0), (2 - first, 1 if paired else 0)):
        result.append((part, [(peer ^ swapped) ^ me if doubling else peer for peer in range(subs)]))
    return result


def factor_body(
    count, rows, paired, doubling, columns_ref, ghosts_ref, tiles_ref, parts_ref, inverse_ref, start_ref, pick_ref, here_ref, sem
):
    move = pltpu.make_async_copy(tiles_ref, here_ref, sem)
    move.start()
    width = parts_ref.shape[2]
    groups = lane_groups(count, rows, width)
    lanes = width // groups
    packed = lax.fori_loop(1, parts_ref.shape[0], lambda i, held: held + parts_ref[i], parts_ref[0])
    across = lax.broadcasted_iota(jnp.int32, (rows, width), 1)
    down = lax.broadcasted_iota(jnp.int32, (rows, width), 0)
    pieces = [packed]
    for group in range(1, groups):
        pieces.append(pltpu.roll(packed, width - group * lanes, 1))
    gram = jnp.where(across <= count, jnp.concatenate(pieces, axis=0), 0.0)
    swept = sweep(gram, count)
    keep = (down < count) & (across < count)
    inverse_ref[0:rows, :] = jnp.where(keep, swept, 0.0)
    tail_down = lax.broadcasted_iota(jnp.int32, (TAIL, width), 0)
    tail_across = lax.broadcasted_iota(jnp.int32, (TAIL, width), 1)
    inverse_ref[rows : rows + TAIL, :] = jnp.where(
        (tail_down < STEPS) & (tail_across == tail_down + rows), 1.0, 0.0
    )
    squared = jnp.broadcast_to(swept[count : count + 1, count : count + 1], (TAIL, width))
    inverse_norm = lax.rsqrt(squared)
    start = jnp.where(down < count, -swept[:, count : count + 1], jnp.where(down == count, 1.0, 0.0))
    start_ref[0:rows, :] = start
    start_ref[rows : rows + TAIL, :] = jnp.where(tail_down == 0, squared * inverse_norm, inverse_norm)
    slots, per_row = columns_ref.shape
    blocks = (pick_ref.shape[0] - slots) // 3
    places = [
        part * blocks + peer * slots + slot
        for part, peers in near_peers(blocks // slots, paired, doubling)
        for peer in peers
        for slot in range(slots)
    ]
    places += [3 * blocks + slot for slot in range(slots)]
    for slot in range(slots):
        names = columns_ref[slot : slot + 1, :]
        wanted = names + 3 * blocks
        for ghost in range(ghosts_ref.shape[1]):
            wanted = jnp.where(names == slots + ghost, ghosts_ref[:, ghost : ghost + 1], wanted)
        wanted = wanted.astype(F32)
        column = jnp.sum(jnp.where(eye(per_row, per_row), wanted, 0.0), axis=1, keepdims=True)
        column = jnp.broadcast_to(column, (per_row, width)).astype(jnp.int32)
        for at, place in enumerate(places):
            pick_ref[at, slot * per_row : (slot + 1) * per_row, :] = jnp.where(column == place, 1.0, 0.0)
    move.wait()


def start_body(
    start_ref, own_ref, one_ref, group_ref, two_ref, tiles_ref, pick_ref, mask_ref, out_ref, tail_ref, own_tail_ref
):
    slots, rows, width = own_ref.shape
    blocks = group_ref.shape[0]
    coefficients = start_ref[0:rows, :] * start_ref[rows + 1 : rows + 2, :]
    empty = jnp.zeros((TAIL, width), F32)
    vectors = []
    tails = []
    for part in (one_ref, group_ref, two_ref, own_ref):
        for place in range(part.shape[0]):
            vector = jnp.sum(part[place] * coefficients, axis=0, keepdims=True)
            tail = tail_with(empty, 0, vector)
            if len(vectors) < 3 * blocks:
                tail_ref[len(vectors)] = tail
            else:
                tails.append(tail)
            vectors.append(vector)
    finish_step(vectors, tails, own_ref, tiles_ref, pick_ref, mask_ref, own_tail_ref, out_ref)


def project(total_row, inverse, rows, width):
    full = rows + TAIL
    down = lax.broadcasted_iota(jnp.int32, (full, width), 0)
    projected = jnp.sum(inverse * total_row, axis=1, keepdims=True)
    column = jnp.sum(jnp.where(eye(full, width), total_row, 0.0), axis=1, keepdims=True)
    projected = jnp.broadcast_to(projected, (full, width))
    squared = jnp.sum(
        jnp.where(down == rows + STEPS, column, -(column * projected)), axis=0, keepdims=True
    )
    inverse_norm = lax.rsqrt(squared)
    return projected, squared * inverse_norm, inverse_norm, down


def step_body(
    step, count, paired, doubling, every_ref, own_ref, one_ref, group_ref, two_ref, old_ref, old_own_ref, inverse_ref,
    tiles_ref, pick_ref, mask_ref, out_ref, tail_ref, own_tail_ref, history_ref,
):
    slots, rows, width = own_ref.shape
    subs = lax.axis_size("sub")
    last_dom = lax.axis_size("dom") - 1
    total_row = tree_sum([every_ref[i, slots : slots + 1, :] for i in range(every_ref.shape[0])])
    projected, norm, inverse_norm, down = project(total_row, inverse_ref[...], rows, width)
    history_ref[...] = jnp.where(down == count, norm, projected)
    coefficients = jnp.where(down == rows + STEPS, inverse_norm, -(projected * inverse_norm))
    head, foot = coefficients[0:rows], coefficients[rows : rows + TAIL]
    vectors = []
    for part, (offset, peers) in zip((one_ref, group_ref, two_ref), near_peers(subs, paired, doubling)):
        first = jnp.clip(lax.axis_index("dom") + offset - 1, 0, last_dom) * subs
        for place in range(part.shape[0]):
            at = len(vectors)
            old = old_ref[at]
            image = every_ref[first + peers[place // slots], place % slots : place % slots + 1, :]
            vector = jnp.sum(part[place] * head, axis=0, keepdims=True)
            vector = vector + jnp.sum(old * foot, axis=0, keepdims=True) + image * inverse_norm
            if tail_ref is not None:
                tail_ref[at] = tail_with(old, step, vector)
            vectors.append(vector)
    tails = []
    for slot in range(slots):
        old = old_own_ref[slot]
        vector = jnp.sum(own_ref[slot] * head, axis=0, keepdims=True)
        vector = vector + jnp.sum(old * foot, axis=0, keepdims=True)
        tails.append(tail_with(old, step, vector))
        vectors.append(vector)
    finish_step(vectors, tails, own_ref, tiles_ref, pick_ref, mask_ref, own_tail_ref, out_ref)


def last_step_body(step, count, paired, doubling, *refs):
    step_body(step, count, paired, doubling, *refs[:12], None, *refs[12:])


def small_solve(matrix, target):
    size = len(target)
    low = [[None] * size for _ in range(size)]
    inverses = []
    for j in range(size):
        value = matrix[j][j]
        for k in range(j):
            value = value - low[j][k] * low[j][k]
        inverses.append(1.0 / jnp.sqrt(value))
        for i in range(j + 1, size):
            value = matrix[i][j]
            for k in range(j):
                value = value - low[i][k] * low[j][k]
            low[i][j] = value * inverses[j]
    forward = []
    for i in range(size):
        value = target[i]
        for k in range(i):
            value = value - low[i][k] * forward[k]
        forward.append(value * inverses[i])
    back = [None] * size
    for i in reversed(range(size)):
        value = forward[i]
        for k in range(i + 1, size):
            value = value - low[k][i] * back[k]
        back[i] = value * inverses[i]
    return back


def end_body(count, mask_ref, every_ref, own_ref, tail_ref, inverse_ref, start_ref, recycled_ref, *rest):
    histories, (solution_ref, residual_ref) = rest[:-2], rest[-2:]
    slots, rows, width = own_ref.shape
    full = rows + TAIL
    total_row = tree_sum([every_ref[i] for i in range(every_ref.shape[0])])
    projected, norm, _, down = project(total_row, inverse_ref[...], rows, width)
    columns = [history[...] for history in histories]
    columns.append(jnp.where(down == count, norm, projected))
    entries = []
    for j in range(STEPS):
        column = [columns[j][rows + i : rows + i + 1, :] for i in range(j + 1)]
        column.append(columns[j][count : count + 1, :])
        entries.append(column)
    normal = [[None] * STEPS for _ in range(STEPS)]
    for a in range(STEPS):
        for b in range(a + 1):
            shared = range(min(len(entries[a]), len(entries[b])))
            normal[a][b] = tree_sum([entries[a][r] * entries[b][r] for r in shared])
    initial = start_ref[rows : rows + 1, :]
    least = small_solve(normal, [initial * entries[j][0] for j in range(STEPS)])
    image = []
    for r in range(STEPS + 1):
        image.append(tree_sum([entries[j][r] * least[j] for j in range(STEPS) if r < len(entries[j])]))
    start = start_ref[0:rows, :]
    recycled_coefficients = start[0:count] * -1.0
    for j in range(STEPS):
        recycled_coefficients = recycled_coefficients - columns[j][0:count] * least[j]
    ratio = image[STEPS] / norm
    head = jnp.where(down[0:rows] < count, start + columns[-1][0:rows] * ratio, start)
    tail_down = down[0:TAIL]
    solution_tail = jnp.zeros((TAIL, width), F32)
    residual_tail = jnp.zeros((TAIL, width), F32)
    for j in range(STEPS):
        solution_tail = jnp.where(tail_down == j, least[j], solution_tail)
        residual_tail = jnp.where(tail_down == j, entries[-1][j] * ratio - image[j], residual_tail)
    residual_tail = jnp.where(tail_down == STEPS, -ratio, residual_tail)
    for slot in range(slots):
        tail = tail_ref[slot]
        mask = mask_ref[slot : slot + 1, :]
        point = jnp.sum(recycled_ref[:, slot, :] * mask * recycled_coefficients, axis=0, keepdims=True)
        point = point + jnp.sum(tail * solution_tail, axis=0, keepdims=True)
        solution_ref[slot : slot + 1, :] = point
        left = jnp.sum(own_ref[slot] * head, axis=0, keepdims=True)
        left = left + jnp.sum(tail * residual_tail, axis=0, keepdims=True)
        residual_ref[slot : slot + 1, :] = left


def local(load_vector, recycled, images, matrix_tiles, tile_columns, ghost_list, live_counts):
    slots, width = load_vector.shape
    count = recycled.shape[0]
    doms, subs = lax.axis_size("dom"), lax.axis_size("sub")
    devices = doms * subs
    rows = round_up(count + 1, ROW_ALIGN)
    full = rows + TAIL
    per_row = tile_columns.shape[1]
    own, mask = call(
        pack_body,
        "pack",
        [(slots, rows, width), (round_up(slots, 8), width)],
        [SMEM, VMEM, VMEM],
    )(live_counts, load_vector, images)
    each = rows // lane_groups(count, rows, width)
    paired = subs % 2 == 0
    doubling = subs == 4

    def turn(value, bit):
        return lax.ppermute(value, "sub", [(i, i ^ bit) for i in range(subs)])

    if doubling:
        with jax.named_scope("inner"):
            inner = turn(own, 1)
        with jax.named_scope("outer"):
            outer = turn(own, 2)
        with jax.named_scope("corner"):
            corner = turn(own, 3)
        (held,) = call(first_gram_body, "first_gram", [(rows, width)], [VMEM] * 2)(own, inner)
        outer, corner, held = lax.optimization_barrier((outer, corner, held))
        (group,) = call(join_body, "join", [(subs * slots, rows, width)], [VMEM] * 4)(own, inner, outer, corner)
        (grams,) = call(functools.partial(gram_body, count), "gram", [(doms, each, width)], [VMEM] * 3)(
            held, outer, corner
        )
    else:
        group = lax.all_gather(own, "sub", axis=0, tiled=True)
        (grams,) = call(functools.partial(whole_gram_body, count), "gram", [(doms, each, width)], [VMEM])(group)
    with jax.named_scope("collect"):
        parts = lax.all_to_all(grams, "dom", 0, 0)
    if paired:
        pairs = []
        for d in range(doms):
            for s in range(subs):
                to = d + 1 if (s + d) % 2 == 0 else d - 1
                if 0 <= to < doms:
                    pairs.append((d * subs + s, to * subs + s))
        with jax.named_scope("pair"):
            one = lax.ppermute(group, AXES, pairs)
        one, parts = lax.optimization_barrier((one, parts))
        with jax.named_scope("swap"):
            two = turn(one, 1)
    else:
        up = [(i, i + 1) for i in range(doms - 1)]
        one = lax.ppermute(group, "dom", up)
        two = lax.ppermute(group, "dom", [(j, i) for i, j in up])
    lines = round_up(slots + 1, 4)
    near = 3 * group.shape[0]
    inverse, start, pick, tiles = call(
        functools.partial(factor_body, count, rows, paired, doubling),
        "factor",
        [(full, width), (full, width), (near + slots, slots * per_row, width), matrix_tiles.shape],
        [VMEM, VMEM, HBM, VMEM],
        [pltpu.SemaphoreType.DMA],
    )(tile_columns, ghost_list, pltpu.with_memory_space_constraint(matrix_tiles, pltpu.HBM), parts)
    message, tails, own_tails = call(
        start_body,
        "start",
        [(devices, lines, width), (near, TAIL, width), (slots, TAIL, width)],
        [VMEM] * 8,
    )(start, own, one, group, two, tiles, pick, mask)
    histories = []
    for step in range(1, STEPS):
        every = lax.all_to_all(message, AXES, 0, 0)
        last = step == STEPS - 1
        sent = 1 if last else lines
        results = call(
            functools.partial(last_step_body if last else step_body, step, count, paired, doubling),
            f"step{step}",
            [(devices, sent, width)]
            + ([] if last else [(near, TAIL, width)])
            + [(slots, TAIL, width), (full, width)],
            [VMEM] * 11,
        )(every, own, one, group, two, tails, own_tails, inverse, tiles, pick, mask)
        message, own_tails, history = results[0], results[-2], results[-1]
        tails = tails if last else results[1]
        histories.append(history)
    every = lax.all_to_all(message, AXES, 0, 0)
    return tuple(
        call(
            functools.partial(end_body, count),
            "end",
            [(slots, width), (slots, width)],
            [VMEM] * (7 + len(histories)),
        )(mask, every, own, own_tails, inverse, start, recycled, *histories)
    )


def solution(mesh):
    return jax.shard_map(
        local,
        mesh=mesh,
        in_specs=(
            P(("dom", "sub"), None),
            P(None, ("dom", "sub"), None),
            P(None, ("dom", "sub"), None),
            P(("dom", "sub"), None, None, None),
            P(("dom", "sub"), None),
            P(("dom", "sub"), None),
            P(("dom", "sub")),
        ),
        out_specs=(P(("dom", "sub"), None), P(("dom", "sub"), None)),
        check_vma=False,
    )
```

```python
import functools

import jax
import jax.numpy as jnp
from jax import lax
from jax.experimental import pallas as pl
from jax.experimental.pallas import tpu as pltpu
from jax.sharding import PartitionSpec as P


STEPS = 3
TAIL = 8
ROW_ALIGN = 8
AXES = ("dom", "sub")
VMEM = pl.BlockSpec(memory_space=pltpu.VMEM)
SMEM = pl.BlockSpec(memory_space=pltpu.SMEM)
HBM = pl.BlockSpec(memory_space=pltpu.HBM)
F32 = jnp.float32


def call(body, outs, specs, scratch=(), work=10_000_000):
    return pl.pallas_call(
        body,
        out_shape=[jax.ShapeDtypeStruct(shape, F32) for shape in outs],
        in_specs=specs,
        out_specs=[VMEM] * len(outs),
        scratch_shapes=list(scratch),
        cost_estimate=pl.CostEstimate(flops=work, bytes_accessed=1 << 20, transcendentals=0),
        compiler_params=pltpu.CompilerParams(vmem_limit_bytes=16 * 1024 * 1024),
    )


def round_up(value, step):
    return -(-value // step) * step


def eye(rows, lanes):
    down = lax.broadcasted_iota(jnp.int32, (rows, lanes), 0)
    across = lax.broadcasted_iota(jnp.int32, (rows, lanes), 1)
    return down == across


def to_row(column, mask):
    return jnp.sum(jnp.where(mask, column, 0.0), axis=0, keepdims=True)


def tree_sum(parts):
    while len(parts) > 1:
        pairs = [parts[i] + parts[i + 1] for i in range(0, len(parts) - 1, 2)]
        parts = pairs + parts[len(parts) - len(parts) % 2 :]
    return parts[0]


def pack_body(live_ref, load_ref, images_ref, own_ref, mask_ref):
    count, slots, width = images_ref.shape
    rows = own_ref.shape[1]
    line = lax.broadcasted_iota(jnp.int32, mask_ref.shape, 0)
    mask_ref[...] = jnp.where(line < live_ref[0], 1.0, 0.0).astype(F32)
    for slot in range(slots):
        mask = jnp.where(slot < live_ref[0], 1.0, 0.0).astype(F32)
        own_ref[slot, 0:count, :] = images_ref[:, slot, :] * mask
        own_ref[slot, count : count + 1, :] = load_ref[slot : slot + 1, :] * mask
        own_ref[slot, count + 1 : rows, :] = jnp.zeros((rows - count - 1, width), F32)


def join_body(*refs):
    place = 0
    for part in refs[:-1]:
        for block in range(part.shape[0]):
            refs[-1][place] = part[block]
            place += 1


def lane_groups(count, rows, width):
    groups = width // (count + 1)
    if rows % groups == 0 and (rows // groups) % ROW_ALIGN == 0:
        return groups
    return 1


def gram_of(*refs):
    products = []
    for ref in refs:
        for block in range(ref.shape[0]):
            part = ref[block]
            products.append(
                lax.dot_general(
                    part, part, (((1,), (1,)), ((), ())),
                    precision=lax.Precision.HIGHEST, preferred_element_type=F32,
                )
            )
    rows, width = refs[0].shape[1:]
    return jnp.concatenate([tree_sum(products), jnp.zeros((rows, width - rows), F32)], axis=1)


def first_gram_body(*refs):
    refs[-1][...] = gram_of(*refs[:-1])


def gram_body(count, held_ref, *refs):
    parts, out_ref = refs[:-1], refs[-1]
    rows, width = parts[0].shape[1:]
    gram = gram_of(*parts)
    if held_ref is not None:
        gram = gram + held_ref[...]
    groups = lane_groups(count, rows, width)
    each, lanes = rows // groups, width // groups
    packed = gram[0:each]
    for group in range(1, groups):
        packed = packed + pltpu.roll(gram[group * each : (group + 1) * each], group * lanes, 1)
    for copy in range(out_ref.shape[0]):
        out_ref[copy] = packed


def whole_gram_body(count, group_ref, out_ref):
    gram_body(count, None, group_ref, out_ref)


def multiply(left, right):
    return [[tree_sum([a * right[k][j] for k, a in enumerate(row)]) for j in range(len(right[0]))] for row in left]


def symmetric(left, right):
    size = len(left)
    half = [[tree_sum([a * right[k][j] for k, a in enumerate(left[i])]) for j in range(i + 1)] for i in range(size)]
    return [[half[max(i, j)][min(i, j)] for j in range(size)] for i in range(size)]


def small_inverse(matrix):
    size = len(matrix)
    if size == 1:
        return [[1.0 / matrix[0][0]]]
    half = size // 2
    corner = [row[half:] for row in matrix[:half]]
    rest = [row[half:] for row in matrix[half:]]
    first = small_inverse([row[:half] for row in matrix[:half]])
    across = multiply(first, corner)
    taken = symmetric([list(row) for row in zip(*corner)], across)
    left = [[rest[i][j] - taken[i][j] for j in range(i + 1)] for i in range(half)]
    second = small_inverse([[left[max(i, j)][min(i, j)] for j in range(half)] for i in range(half)])
    product = multiply(across, second)
    added = symmetric(product, [list(row) for row in zip(*across)])
    total = [[first[i][j] + added[i][j] for j in range(i + 1)] for i in range(half)]
    top = [[total[max(i, j)][min(i, j)] for j in range(half)] + [-value for value in product[i]] for i in range(half)]
    bottom = [[-product[j][i] for j in range(half)] + second[i] for i in range(half)]
    return top + bottom


def sweep(matrix, count):
    rows, width = matrix.shape
    size = next(size for size in (8, 4, 2, 1) if count % size == 0)
    tiles = [matrix[i : i + 8, :] for i in range(0, rows, 8)]
    across = lax.broadcasted_iota(jnp.int32, (8, width), 1)
    down = lax.broadcasted_iota(jnp.int32, (8, width), 0)

    def spread(value):
        return jnp.broadcast_to(value, (8, width))

    for k in range(0, count, size):
        at, inner = divmod(k, 8)
        columns = [[tile[:, k + i : k + i + 1] for tile in tiles] for i in range(size)]
        lines = [spread(tiles[at][inner + i : inner + i + 1, :]) for i in range(size)]
        full = [spread(columns[i][at]) for i in range(size)]
        pivots = [
            [spread(full[max(i, j)][inner + min(i, j) : inner + min(i, j) + 1, :]) for j in range(size)]
            for i in range(size)
        ]
        inverse = small_inverse(pivots)
        inside = (across >= k) & (across < k + size)
        lines = [jnp.where(inside, jnp.where(across == k + i, 1.0, 0.0), line) for i, line in enumerate(lines)]
        scaled = [tree_sum([lines[j] * inverse[i][j] for j in range(size)]) for i in range(size)]
        updated = []
        for n, tile in enumerate(tiles):
            if n == at and size == 8:
                value = scaled[0]
            else:
                value = jnp.where(inside, 0.0, tile)
                value = value - tree_sum([columns[i][n] * scaled[i] for i in range(size)])
            if n == at:
                for i in range(size):
                    value = jnp.where(down == inner + i, scaled[i], value)
            updated.append(value)
        tiles = updated
    return jnp.concatenate(tiles, axis=0)


def apply_tiles(tiles_ref, pick_ref, vectors, mask_ref):
    slots, per_row, size, _ = tiles_ref.shape
    mask = eye(size, size)
    images = []
    for slot in range(slots):
        picked = tree_sum(
            [pick_ref[e, slot * per_row : (slot + 1) * per_row, :] * vector for e, vector in enumerate(vectors)]
        )
        parts = [tiles_ref[slot, t] * picked[t : t + 1, :] for t in range(per_row)]
        column = jnp.sum(tree_sum(parts), axis=1, keepdims=True)
        images.append(to_row(column, mask) * mask_ref[slot : slot + 1, :])
    return images


def tail_with(old, row, value):
    down = lax.broadcasted_iota(jnp.int32, (TAIL, old.shape[1]), 0)
    return jnp.where(down == row, value, old)


def finish_step(vectors, tails, own_ref, tiles_ref, pick_ref, mask_ref, own_tail_ref, out_ref):
    slots, rows, width = own_ref.shape
    images = apply_tiles(tiles_ref, pick_ref, vectors, mask_ref)
    total = jnp.zeros((rows + TAIL, width), F32)
    for slot in range(slots):
        tail = tail_with(tails[slot], STEPS, images[slot])
        own_tail_ref[slot] = tail
        total = total + jnp.concatenate([own_ref[slot], tail], axis=0) * images[slot]
    partial = to_row(jnp.sum(total, axis=1, keepdims=True), eye(rows + TAIL, width))
    copies, lines, _ = out_ref.shape
    if lines == 1:
        message = partial
    else:
        pad = [jnp.zeros((lines - slots - 1, width), F32)] if lines > slots + 1 else []
        message = jnp.concatenate([*images, partial, *pad], axis=0)
    out_ref[...] = jnp.broadcast_to(message[None], (copies, lines, width))


def near_peers(subs, paired, doubling):
    me = lax.axis_index("sub")
    first = (me + lax.axis_index("dom") + 1) % 2 * 2 if paired else 0
    result = []
    for part, swapped in ((first, 0), (1, 0), (2 - first, 1 if paired else 0)):
        result.append((part, [(peer ^ swapped) ^ me if doubling else peer for peer in range(subs)]))
    return result


def factor_body(
    count, rows, paired, doubling, columns_ref, ghosts_ref, tiles_ref, parts_ref, inverse_ref, start_ref, pick_ref, here_ref, sem
):
    move = pltpu.make_async_copy(tiles_ref, here_ref, sem)
    move.start()
    width = parts_ref.shape[2]
    groups = lane_groups(count, rows, width)
    lanes = width // groups
    packed = lax.fori_loop(1, parts_ref.shape[0], lambda i, held: held + parts_ref[i], parts_ref[0])
    across = lax.broadcasted_iota(jnp.int32, (rows, width), 1)
    down = lax.broadcasted_iota(jnp.int32, (rows, width), 0)
    pieces = [packed]
    for group in range(1, groups):
        pieces.append(pltpu.roll(packed, width - group * lanes, 1))
    gram = jnp.where(across <= count, jnp.concatenate(pieces, axis=0), 0.0)
    swept = sweep(gram, count)
    keep = (down < count) & (across < count)
    inverse_ref[0:rows, :] = jnp.where(keep, swept, 0.0)
    tail_down = lax.broadcasted_iota(jnp.int32, (TAIL, width), 0)
    tail_across = lax.broadcasted_iota(jnp.int32, (TAIL, width), 1)
    inverse_ref[rows : rows + TAIL, :] = jnp.where(
        (tail_down < STEPS) & (tail_across == tail_down + rows), 1.0, 0.0
    )
    squared = jnp.broadcast_to(swept[count : count + 1, count : count + 1], (TAIL, width))
    inverse_norm = lax.rsqrt(squared)
    start = jnp.where(down < count, -swept[:, count : count + 1], jnp.where(down == count, 1.0, 0.0))
    start_ref[0:rows, :] = start
    start_ref[rows : rows + TAIL, :] = jnp.where(tail_down == 0, squared * inverse_norm, inverse_norm)
    slots, per_row = columns_ref.shape
    blocks = (pick_ref.shape[0] - slots) // 3
    places = [
        part * blocks + peer * slots + slot
        for part, peers in near_peers(blocks // slots, paired, doubling)
        for peer in peers
        for slot in range(slots)
    ]
    places += [3 * blocks + slot for slot in range(slots)]
    for slot in range(slots):
        names = columns_ref[slot : slot + 1, :]
        wanted = names + 3 * blocks
        for ghost in range(ghosts_ref.shape[1]):
            wanted = jnp.where(names == slots + ghost, ghosts_ref[:, ghost : ghost + 1], wanted)
        wanted = wanted.astype(F32)
        column = jnp.sum(jnp.where(eye(per_row, per_row), wanted, 0.0), axis=1, keepdims=True)
        column = jnp.broadcast_to(column, (per_row, width)).astype(jnp.int32)
        for at, place in enumerate(places):
            pick_ref[at, slot * per_row : (slot + 1) * per_row, :] = jnp.where(column == place, 1.0, 0.0)
    move.wait()


def start_body(
    start_ref, own_ref, one_ref, group_ref, two_ref, tiles_ref, pick_ref, mask_ref, out_ref, tail_ref, own_tail_ref
):
    _, rows, width = own_ref.shape
    blocks = group_ref.shape[0]
    coefficients = start_ref[0:rows, :] * start_ref[rows + 1 : rows + 2, :]
    empty = jnp.zeros((TAIL, width), F32)
    vectors = []
    tails = []
    for part in (one_ref, group_ref, two_ref, own_ref):
        for place in range(part.shape[0]):
            vector = jnp.sum(part[place] * coefficients, axis=0, keepdims=True)
            tail = tail_with(empty, 0, vector)
            if len(vectors) < 3 * blocks:
                tail_ref[len(vectors)] = tail
            else:
                tails.append(tail)
            vectors.append(vector)
    finish_step(vectors, tails, own_ref, tiles_ref, pick_ref, mask_ref, own_tail_ref, out_ref)


def project(total_row, inverse, rows, width):
    full = rows + TAIL
    down = lax.broadcasted_iota(jnp.int32, (full, width), 0)
    projected = jnp.sum(inverse * total_row, axis=1, keepdims=True)
    column = jnp.sum(jnp.where(eye(full, width), total_row, 0.0), axis=1, keepdims=True)
    projected = jnp.broadcast_to(projected, (full, width))
    squared = jnp.sum(
        jnp.where(down == rows + STEPS, column, -(column * projected)), axis=0, keepdims=True
    )
    inverse_norm = lax.rsqrt(squared)
    return projected, squared * inverse_norm, inverse_norm, down


def step_body(
    step, count, paired, doubling, every_ref, own_ref, one_ref, group_ref, two_ref, old_ref, old_own_ref, inverse_ref,
    tiles_ref, pick_ref, mask_ref, out_ref, tail_ref, own_tail_ref, history_ref,
):
    slots, rows, width = own_ref.shape
    subs = lax.axis_size("sub")
    last_dom = lax.axis_size("dom") - 1
    total_row = tree_sum([every_ref[i, slots : slots + 1, :] for i in range(every_ref.shape[0])])
    projected, norm, inverse_norm, down = project(total_row, inverse_ref[...], rows, width)
    history_ref[...] = jnp.where(down == count, norm, projected)
    coefficients = jnp.where(down == rows + STEPS, inverse_norm, -(projected * inverse_norm))
    head, foot = coefficients[0:rows], coefficients[rows : rows + TAIL]
    vectors = []
    for part, (offset, peers) in zip((one_ref, group_ref, two_ref), near_peers(subs, paired, doubling)):
        first = jnp.clip(lax.axis_index("dom") + offset - 1, 0, last_dom) * subs
        for place in range(part.shape[0]):
            at = len(vectors)
            old = old_ref[at]
            image = every_ref[first + peers[place // slots], place % slots : place % slots + 1, :]
            vector = jnp.sum(part[place] * head, axis=0, keepdims=True)
            vector = vector + jnp.sum(old * foot, axis=0, keepdims=True) + image * inverse_norm
            if tail_ref is not None:
                tail_ref[at] = tail_with(old, step, vector)
            vectors.append(vector)
    tails = []
    for slot in range(slots):
        old = old_own_ref[slot]
        vector = jnp.sum(own_ref[slot] * head, axis=0, keepdims=True)
        vector = vector + jnp.sum(old * foot, axis=0, keepdims=True)
        tails.append(tail_with(old, step, vector))
        vectors.append(vector)
    finish_step(vectors, tails, own_ref, tiles_ref, pick_ref, mask_ref, own_tail_ref, out_ref)


def last_step_body(step, count, paired, doubling, *refs):
    step_body(step, count, paired, doubling, *refs[:12], None, *refs[12:])


def small_solve(matrix, target):
    size = len(target)
    low = [[None] * size for _ in range(size)]
    inverses = []
    for j in range(size):
        value = matrix[j][j]
        for k in range(j):
            value = value - low[j][k] * low[j][k]
        inverses.append(1.0 / jnp.sqrt(value))
        for i in range(j + 1, size):
            value = matrix[i][j]
            for k in range(j):
                value = value - low[i][k] * low[j][k]
            low[i][j] = value * inverses[j]
    forward = []
    for i in range(size):
        value = target[i]
        for k in range(i):
            value = value - low[i][k] * forward[k]
        forward.append(value * inverses[i])
    back = [None] * size
    for i in reversed(range(size)):
        value = forward[i]
        for k in range(i + 1, size):
            value = value - low[k][i] * back[k]
        back[i] = value * inverses[i]
    return back


def end_body(count, mask_ref, every_ref, own_ref, tail_ref, inverse_ref, start_ref, recycled_ref, *rest):
    histories, (solution_ref, residual_ref) = rest[:-2], rest[-2:]
    slots, rows, width = own_ref.shape
    total_row = tree_sum([every_ref[i] for i in range(every_ref.shape[0])])
    projected, norm, _, down = project(total_row, inverse_ref[...], rows, width)
    columns = [history[...] for history in histories]
    columns.append(jnp.where(down == count, norm, projected))
    entries = []
    for j in range(STEPS):
        column = [columns[j][rows + i : rows + i + 1, :] for i in range(j + 1)]
        column.append(columns[j][count : count + 1, :])
        entries.append(column)
    normal = [[None] * STEPS for _ in range(STEPS)]
    for a in range(STEPS):
        for b in range(a + 1):
            shared = range(min(len(entries[a]), len(entries[b])))
            normal[a][b] = tree_sum([entries[a][r] * entries[b][r] for r in shared])
    initial = start_ref[rows : rows + 1, :]
    least = small_solve(normal, [initial * entries[j][0] for j in range(STEPS)])
    image = []
    for r in range(STEPS + 1):
        image.append(tree_sum([entries[j][r] * least[j] for j in range(STEPS) if r < len(entries[j])]))
    start = start_ref[0:rows, :]
    recycled_coefficients = start[0:count] * -1.0
    for j in range(STEPS):
        recycled_coefficients = recycled_coefficients - columns[j][0:count] * least[j]
    ratio = image[STEPS] / norm
    head = jnp.where(down[0:rows] < count, start + columns[-1][0:rows] * ratio, start)
    tail_down = down[0:TAIL]
    solution_tail = jnp.zeros((TAIL, width), F32)
    residual_tail = jnp.zeros((TAIL, width), F32)
    for j in range(STEPS):
        solution_tail = jnp.where(tail_down == j, least[j], solution_tail)
        residual_tail = jnp.where(tail_down == j, entries[-1][j] * ratio - image[j], residual_tail)
    residual_tail = jnp.where(tail_down == STEPS, -ratio, residual_tail)
    for slot in range(slots):
        tail = tail_ref[slot]
        mask = mask_ref[slot : slot + 1, :]
        point = jnp.sum(recycled_ref[:, slot, :] * mask * recycled_coefficients, axis=0, keepdims=True)
        point = point + jnp.sum(tail * solution_tail, axis=0, keepdims=True)
        solution_ref[slot : slot + 1, :] = point
        left = jnp.sum(own_ref[slot] * head, axis=0, keepdims=True)
        left = left + jnp.sum(tail * residual_tail, axis=0, keepdims=True)
        residual_ref[slot : slot + 1, :] = left


def local(load_vector, recycled, images, matrix_tiles, tile_columns, ghost_list, live_counts):
    slots, width = load_vector.shape
    count = recycled.shape[0]
    doms, subs = lax.axis_size("dom"), lax.axis_size("sub")
    devices = doms * subs
    rows = round_up(count + 1, ROW_ALIGN)
    full = rows + TAIL
    per_row = tile_columns.shape[1]
    own, mask = call(
        pack_body, [(slots, rows, width), (round_up(slots, 8), width)], [SMEM, VMEM, VMEM]
    )(live_counts, load_vector, images)
    each = rows // lane_groups(count, rows, width)
    paired = subs % 2 == 0
    doubling = subs == 4

    def turn(value, bit):
        return lax.ppermute(value, "sub", [(i, i ^ bit) for i in range(subs)])

    if doubling:
        inner = turn(own, 1)
        outer = turn(own, 2)
        corner = turn(own, 3)
        (held,) = call(first_gram_body, [(rows, width)], [VMEM] * 2)(own, inner)
        outer, corner, held = lax.optimization_barrier((outer, corner, held))
        (group,) = call(join_body, [(subs * slots, rows, width)], [VMEM] * 4)(own, inner, outer, corner)
        (grams,) = call(functools.partial(gram_body, count), [(doms, each, width)], [VMEM] * 3)(held, outer, corner)
    else:
        group = lax.all_gather(own, "sub", axis=0, tiled=True)
        (grams,) = call(functools.partial(whole_gram_body, count), [(doms, each, width)], [VMEM])(group)
    parts = lax.all_to_all(grams, "dom", 0, 0)
    if paired:
        pairs = []
        for d in range(doms):
            for s in range(subs):
                to = d + 1 if (s + d) % 2 == 0 else d - 1
                if 0 <= to < doms:
                    pairs.append((d * subs + s, to * subs + s))
        one = lax.ppermute(group, AXES, pairs)
        one, parts = lax.optimization_barrier((one, parts))
        two = turn(one, 1)
    else:
        up = [(i, i + 1) for i in range(doms - 1)]
        one = lax.ppermute(group, "dom", up)
        two = lax.ppermute(group, "dom", [(j, i) for i, j in up])
    lines = round_up(slots + 1, 4)
    near = 3 * group.shape[0]
    inverse, start, pick, tiles = call(
        functools.partial(factor_body, count, rows, paired, doubling),
        [(full, width), (full, width), (near + slots, slots * per_row, width), matrix_tiles.shape],
        [VMEM, VMEM, HBM, VMEM],
        [pltpu.SemaphoreType.DMA],
    )(tile_columns, ghost_list, pltpu.with_memory_space_constraint(matrix_tiles, pltpu.HBM), parts)
    message, tails, own_tails = call(
        start_body, [(devices, lines, width), (near, TAIL, width), (slots, TAIL, width)], [VMEM] * 8
    )(start, own, one, group, two, tiles, pick, mask)
    histories = []
    for step in range(1, STEPS):
        every = lax.all_to_all(message, AXES, 0, 0)
        last = step == STEPS - 1
        sent = 1 if last else lines
        results = call(
            functools.partial(last_step_body if last else step_body, step, count, paired, doubling),
            [(devices, sent, width)]
            + ([] if last else [(near, TAIL, width)])
            + [(slots, TAIL, width), (full, width)],
            [VMEM] * 11,
        )(every, own, one, group, two, tails, own_tails, inverse, tiles, pick, mask)
        message, own_tails, history = results[0], results[-2], results[-1]
        tails = tails if last else results[1]
        histories.append(history)
    every = lax.all_to_all(message, AXES, 0, 0)
    return tuple(
        call(
            functools.partial(end_body, count), [(slots, width), (slots, width)], [VMEM] * (7 + len(histories))
        )(mask, every, own, own_tails, inverse, start, recycled, *histories)
    )


def solution(mesh):
    return jax.shard_map(
        local,
        mesh=mesh,
        in_specs=(
            P(("dom", "sub"), None),
            P(None, ("dom", "sub"), None),
            P(None, ("dom", "sub"), None),
            P(("dom", "sub"), None, None, None),
            P(("dom", "sub"), None),
            P(("dom", "sub"), None),
            P(("dom", "sub")),
        ),
        out_specs=(P(("dom", "sub"), None), P(("dom", "sub"), None)),
        check_vma=False,
    )
```

```python
import functools

import jax
import jax.numpy as jnp
from jax import lax
from jax.experimental import pallas as pl
from jax.experimental.pallas import tpu as pltpu
from jax.sharding import PartitionSpec as P


STEPS = 3
TAIL = 8
ROW_ALIGN = 8
AXES = ("dom", "sub")
VMEM = pl.BlockSpec(memory_space=pltpu.VMEM)
SMEM = pl.BlockSpec(memory_space=pltpu.SMEM)
HBM = pl.BlockSpec(memory_space=pltpu.HBM)
F32 = jnp.float32


def call(body, outs, specs, scratch=(), work=10_000_000):
    return pl.pallas_call(
        body,
        out_shape=[jax.ShapeDtypeStruct(shape, F32) for shape in outs],
        in_specs=specs,
        out_specs=[VMEM] * len(outs),
        scratch_shapes=list(scratch),
        cost_estimate=pl.CostEstimate(flops=work, bytes_accessed=1 << 20, transcendentals=0),
        compiler_params=pltpu.CompilerParams(vmem_limit_bytes=16 * 1024 * 1024),
    )


def round_up(value, step):
    return -(-value // step) * step


def eye(rows, lanes):
    down = lax.broadcasted_iota(jnp.int32, (rows, lanes), 0)
    across = lax.broadcasted_iota(jnp.int32, (rows, lanes), 1)
    return down == across


def to_row(column, mask):
    return jnp.sum(jnp.where(mask, column, 0.0), axis=0, keepdims=True)


def tree_sum(parts):
    while len(parts) > 1:
        pairs = [parts[i] + parts[i + 1] for i in range(0, len(parts) - 1, 2)]
        parts = pairs + parts[len(parts) - len(parts) % 2 :]
    return parts[0]


def pack_body(live_ref, load_ref, images_ref, own_ref, mask_ref):
    count, slots, width = images_ref.shape
    rows = own_ref.shape[1]
    line = lax.broadcasted_iota(jnp.int32, mask_ref.shape, 0)
    mask_ref[...] = jnp.where(line < live_ref[0], 1.0, 0.0).astype(F32)
    for slot in range(slots):
        mask = jnp.where(slot < live_ref[0], 1.0, 0.0).astype(F32)
        own_ref[slot, 0:count, :] = images_ref[:, slot, :] * mask
        own_ref[slot, count : count + 1, :] = load_ref[slot : slot + 1, :] * mask
        own_ref[slot, count + 1 : rows, :] = jnp.zeros((rows - count - 1, width), F32)


def join_body(*refs):
    place = 0
    for part in refs[:-1]:
        for block in range(part.shape[0]):
            refs[-1][place] = part[block]
            place += 1


def lane_groups(count, rows, width):
    groups = width // (count + 1)
    if rows % groups == 0 and (rows // groups) % ROW_ALIGN == 0:
        return groups
    return 1


def gram_of(*refs):
    products = []
    for ref in refs:
        for block in range(ref.shape[0]):
            part = ref[block]
            products.append(
                lax.dot_general(
                    part, part, (((1,), (1,)), ((), ())),
                    precision=lax.Precision.HIGHEST, preferred_element_type=F32,
                )
            )
    rows, width = refs[0].shape[1:]
    return jnp.concatenate([tree_sum(products), jnp.zeros((rows, width - rows), F32)], axis=1)


def first_gram_body(*refs):
    refs[-1][...] = gram_of(*refs[:-1])


def gram_body(count, held_ref, *refs):
    parts, out_ref = refs[:-1], refs[-1]
    rows, width = parts[0].shape[1:]
    gram = gram_of(*parts)
    if held_ref is not None:
        gram = gram + held_ref[...]
    groups = lane_groups(count, rows, width)
    each, lanes = rows // groups, width // groups
    packed = gram[0:each]
    for group in range(1, groups):
        packed = packed + pltpu.roll(gram[group * each : (group + 1) * each], group * lanes, 1)
    for copy in range(out_ref.shape[0]):
        out_ref[copy] = packed


def whole_gram_body(count, group_ref, out_ref):
    gram_body(count, None, group_ref, out_ref)


def multiply(left, right):
    return [[tree_sum([a * right[k][j] for k, a in enumerate(row)]) for j in range(len(right[0]))] for row in left]


def symmetric(left, right):
    size = len(left)
    half = [[tree_sum([a * right[k][j] for k, a in enumerate(left[i])]) for j in range(i + 1)] for i in range(size)]
    return [[half[max(i, j)][min(i, j)] for j in range(size)] for i in range(size)]


def small_inverse(matrix):
    size = len(matrix)
    if size == 1:
        return [[1.0 / matrix[0][0]]]
    half = size // 2
    corner = [row[half:] for row in matrix[:half]]
    rest = [row[half:] for row in matrix[half:]]
    first = small_inverse([row[:half] for row in matrix[:half]])
    across = multiply(first, corner)
    taken = symmetric([list(row) for row in zip(*corner)], across)
    left = [[rest[i][j] - taken[i][j] for j in range(i + 1)] for i in range(half)]
    second = small_inverse([[left[max(i, j)][min(i, j)] for j in range(half)] for i in range(half)])
    product = multiply(across, second)
    added = symmetric(product, [list(row) for row in zip(*across)])
    total = [[first[i][j] + added[i][j] for j in range(i + 1)] for i in range(half)]
    top = [[total[max(i, j)][min(i, j)] for j in range(half)] + [-value for value in product[i]] for i in range(half)]
    bottom = [[-product[j][i] for j in range(half)] + second[i] for i in range(half)]
    return top + bottom


def sweep(matrix, count):
    rows, width = matrix.shape
    size = next(size for size in (8, 4, 2, 1) if count % size == 0)
    tiles = [matrix[i : i + 8, :] for i in range(0, rows, 8)]
    across = lax.broadcasted_iota(jnp.int32, (8, width), 1)
    down = lax.broadcasted_iota(jnp.int32, (8, width), 0)

    def spread(value):
        return jnp.broadcast_to(value, (8, width))

    for k in range(0, count, size):
        at, inner = divmod(k, 8)
        columns = [[tile[:, k + i : k + i + 1] for tile in tiles] for i in range(size)]
        lines = [spread(tiles[at][inner + i : inner + i + 1, :]) for i in range(size)]
        full = [spread(columns[i][at]) for i in range(size)]
        pivots = [
            [spread(full[max(i, j)][inner + min(i, j) : inner + min(i, j) + 1, :]) for j in range(size)]
            for i in range(size)
        ]
        inverse = small_inverse(pivots)
        inside = (across >= k) & (across < k + size)
        lines = [jnp.where(inside, jnp.where(across == k + i, 1.0, 0.0), line) for i, line in enumerate(lines)]
        scaled = [tree_sum([lines[j] * inverse[i][j] for j in range(size)]) for i in range(size)]
        updated = []
        for n, tile in enumerate(tiles):
            if n == at and size == 8:
                value = scaled[0]
            else:
                value = jnp.where(inside, 0.0, tile)
                value = value - tree_sum([columns[i][n] * scaled[i] for i in range(size)])
            if n == at:
                for i in range(size):
                    value = jnp.where(down == inner + i, scaled[i], value)
            updated.append(value)
        tiles = updated
    return jnp.concatenate(tiles, axis=0)


def apply_tiles(tiles_ref, pick_ref, vectors, mask_ref):
    slots, per_row, size, _ = tiles_ref.shape
    mask = eye(size, size)
    images = []
    for slot in range(slots):
        picked = tree_sum(
            [pick_ref[e, slot * per_row : (slot + 1) * per_row, :] * vector for e, vector in enumerate(vectors)]
        )
        parts = [tiles_ref[slot, t] * picked[t : t + 1, :] for t in range(per_row)]
        column = jnp.sum(tree_sum(parts), axis=1, keepdims=True)
        images.append(to_row(column, mask) * mask_ref[slot : slot + 1, :])
    return images


def tail_with(old, row, value):
    down = lax.broadcasted_iota(jnp.int32, (TAIL, old.shape[1]), 0)
    return jnp.where(down == row, value, old)


def finish_step(vectors, tails, own_ref, tiles_ref, pick_ref, mask_ref, own_tail_ref, out_ref):
    slots, rows, width = own_ref.shape
    images = apply_tiles(tiles_ref, pick_ref, vectors, mask_ref)
    total = jnp.zeros((rows + TAIL, width), F32)
    for slot in range(slots):
        tail = tail_with(tails[slot], STEPS, images[slot])
        own_tail_ref[slot] = tail
        total = total + jnp.concatenate([own_ref[slot], tail], axis=0) * images[slot]
    partial = to_row(jnp.sum(total, axis=1, keepdims=True), eye(rows + TAIL, width))
    copies, lines, _ = out_ref.shape
    if lines == 1:
        message = partial
    else:
        pad = [jnp.zeros((lines - slots - 1, width), F32)] if lines > slots + 1 else []
        message = jnp.concatenate([*images, partial, *pad], axis=0)
    out_ref[...] = jnp.broadcast_to(message[None], (copies, lines, width))


def near_peers(subs, paired, doubling):
    me = lax.axis_index("sub")
    first = (me + lax.axis_index("dom") + 1) % 2 * 2 if paired else 0
    result = []
    for part, swapped in ((first, 0), (1, 0), (2 - first, 1 if paired else 0)):
        result.append((part, [(peer ^ swapped) ^ me if doubling else peer for peer in range(subs)]))
    return result


def sweep_parts(count, rows, parts_ref, inverse_ref, start_ref):
    width = parts_ref.shape[2]
    groups = lane_groups(count, rows, width)
    lanes = width // groups
    packed = lax.fori_loop(1, parts_ref.shape[0], lambda i, held: held + parts_ref[i], parts_ref[0])
    across = lax.broadcasted_iota(jnp.int32, (rows, width), 1)
    down = lax.broadcasted_iota(jnp.int32, (rows, width), 0)
    pieces = [packed]
    for group in range(1, groups):
        pieces.append(pltpu.roll(packed, width - group * lanes, 1))
    gram = jnp.where(across <= count, jnp.concatenate(pieces, axis=0), 0.0)
    swept = sweep(gram, count)
    keep = (down < count) & (across < count)
    inverse_ref[0:rows, :] = jnp.where(keep, swept, 0.0)
    tail_down = lax.broadcasted_iota(jnp.int32, (TAIL, width), 0)
    tail_across = lax.broadcasted_iota(jnp.int32, (TAIL, width), 1)
    inverse_ref[rows : rows + TAIL, :] = jnp.where(
        (tail_down < STEPS) & (tail_across == tail_down + rows), 1.0, 0.0
    )
    squared = jnp.broadcast_to(swept[count : count + 1, count : count + 1], (TAIL, width))
    inverse_norm = lax.rsqrt(squared)
    start = jnp.where(down < count, -swept[:, count : count + 1], jnp.where(down == count, 1.0, 0.0))
    start_ref[0:rows, :] = start
    start_ref[rows : rows + TAIL, :] = jnp.where(tail_down == 0, squared * inverse_norm, inverse_norm)


def odd_core():
    return lax.axis_index("sub") % 2 == 1


def early_body(count, rows, columns_ref, ghosts_ref, parts_ref, inverse_ref, start_ref):
    @pl.when(odd_core())
    def _():
        sweep_parts(count, rows, parts_ref, inverse_ref, start_ref)


def factor_body(
    count, rows, paired, doubling, columns_ref, ghosts_ref, tiles_ref, parts_ref, *refs,
):
    early_refs, (inverse_ref, start_ref, pick_ref, here_ref, sem) = refs[:-5], refs[-5:]
    move = pltpu.make_async_copy(tiles_ref, here_ref, sem)
    move.start()
    width = parts_ref.shape[2]
    if early_refs:
        @pl.when(odd_core())
        def _():
            inverse_ref[...] = early_refs[0][...]
            start_ref[...] = early_refs[1][...]

        @pl.when(jnp.logical_not(odd_core()))
        def _():
            sweep_parts(count, rows, parts_ref, inverse_ref, start_ref)
    else:
        sweep_parts(count, rows, parts_ref, inverse_ref, start_ref)
    slots, per_row = columns_ref.shape
    blocks = (pick_ref.shape[0] - slots) // 3
    places = [
        part * blocks + peer * slots + slot
        for part, peers in near_peers(blocks // slots, paired, doubling)
        for peer in peers
        for slot in range(slots)
    ]
    places += [3 * blocks + slot for slot in range(slots)]
    for slot in range(slots):
        names = columns_ref[slot : slot + 1, :]
        wanted = names + 3 * blocks
        for ghost in range(ghosts_ref.shape[1]):
            wanted = jnp.where(names == slots + ghost, ghosts_ref[:, ghost : ghost + 1], wanted)
        wanted = wanted.astype(F32)
        column = jnp.sum(jnp.where(eye(per_row, per_row), wanted, 0.0), axis=1, keepdims=True)
        column = jnp.broadcast_to(column, (per_row, width)).astype(jnp.int32)
        for at, place in enumerate(places):
            pick_ref[at, slot * per_row : (slot + 1) * per_row, :] = jnp.where(column == place, 1.0, 0.0)
    move.wait()


def start_body(
    start_ref, own_ref, one_ref, group_ref, two_ref, tiles_ref, pick_ref, mask_ref, out_ref, tail_ref, own_tail_ref
):
    _, rows, width = own_ref.shape
    blocks = group_ref.shape[0]
    coefficients = start_ref[0:rows, :] * start_ref[rows + 1 : rows + 2, :]
    empty = jnp.zeros((TAIL, width), F32)
    vectors = []
    tails = []
    for part in (one_ref, group_ref, two_ref, own_ref):
        for place in range(part.shape[0]):
            vector = jnp.sum(part[place] * coefficients, axis=0, keepdims=True)
            tail = tail_with(empty, 0, vector)
            if len(vectors) < 3 * blocks:
                tail_ref[len(vectors)] = tail
            else:
                tails.append(tail)
            vectors.append(vector)
    finish_step(vectors, tails, own_ref, tiles_ref, pick_ref, mask_ref, own_tail_ref, out_ref)


def project(total_row, inverse, rows, width):
    full = rows + TAIL
    down = lax.broadcasted_iota(jnp.int32, (full, width), 0)
    projected = jnp.sum(inverse * total_row, axis=1, keepdims=True)
    column = jnp.sum(jnp.where(eye(full, width), total_row, 0.0), axis=1, keepdims=True)
    projected = jnp.broadcast_to(projected, (full, width))
    squared = jnp.sum(
        jnp.where(down == rows + STEPS, column, -(column * projected)), axis=0, keepdims=True
    )
    inverse_norm = lax.rsqrt(squared)
    return projected, squared * inverse_norm, inverse_norm, down


def step_body(
    step, count, paired, doubling, every_ref, own_ref, one_ref, group_ref, two_ref, old_ref, old_own_ref, inverse_ref,
    tiles_ref, pick_ref, mask_ref, out_ref, tail_ref, own_tail_ref, history_ref,
):
    slots, rows, width = own_ref.shape
    subs = lax.axis_size("sub")
    last_dom = lax.axis_size("dom") - 1
    total_row = tree_sum([every_ref[i, slots : slots + 1, :] for i in range(every_ref.shape[0])])
    projected, norm, inverse_norm, down = project(total_row, inverse_ref[...], rows, width)
    history_ref[...] = jnp.where(down == count, norm, projected)
    coefficients = jnp.where(down == rows + STEPS, inverse_norm, -(projected * inverse_norm))
    head, foot = coefficients[0:rows], coefficients[rows : rows + TAIL]
    vectors = []
    for part, (offset, peers) in zip((one_ref, group_ref, two_ref), near_peers(subs, paired, doubling)):
        first = jnp.clip(lax.axis_index("dom") + offset - 1, 0, last_dom) * subs
        for place in range(part.shape[0]):
            at = len(vectors)
            old = old_ref[at]
            image = every_ref[first + peers[place // slots], place % slots : place % slots + 1, :]
            vector = jnp.sum(part[place] * head, axis=0, keepdims=True)
            vector = vector + jnp.sum(old * foot, axis=0, keepdims=True) + image * inverse_norm
            if tail_ref is not None:
                tail_ref[at] = tail_with(old, step, vector)
            vectors.append(vector)
    tails = []
    for slot in range(slots):
        old = old_own_ref[slot]
        vector = jnp.sum(own_ref[slot] * head, axis=0, keepdims=True)
        vector = vector + jnp.sum(old * foot, axis=0, keepdims=True)
        tails.append(tail_with(old, step, vector))
        vectors.append(vector)
    finish_step(vectors, tails, own_ref, tiles_ref, pick_ref, mask_ref, own_tail_ref, out_ref)


def last_step_body(step, count, paired, doubling, *refs):
    step_body(step, count, paired, doubling, *refs[:12], None, *refs[12:])


def small_solve(matrix, target):
    size = len(target)
    low = [[None] * size for _ in range(size)]
    inverses = []
    for j in range(size):
        value = matrix[j][j]
        for k in range(j):
            value = value - low[j][k] * low[j][k]
        inverses.append(1.0 / jnp.sqrt(value))
        for i in range(j + 1, size):
            value = matrix[i][j]
            for k in range(j):
                value = value - low[i][k] * low[j][k]
            low[i][j] = value * inverses[j]
    forward = []
    for i in range(size):
        value = target[i]
        for k in range(i):
            value = value - low[i][k] * forward[k]
        forward.append(value * inverses[i])
    back = [None] * size
    for i in reversed(range(size)):
        value = forward[i]
        for k in range(i + 1, size):
            value = value - low[k][i] * back[k]
        back[i] = value * inverses[i]
    return back


def end_body(count, mask_ref, every_ref, own_ref, tail_ref, inverse_ref, start_ref, recycled_ref, *rest):
    histories, (solution_ref, residual_ref) = rest[:-2], rest[-2:]
    slots, rows, width = own_ref.shape
    total_row = tree_sum([every_ref[i] for i in range(every_ref.shape[0])])
    projected, norm, _, down = project(total_row, inverse_ref[...], rows, width)
    columns = [history[...] for history in histories]
    columns.append(jnp.where(down == count, norm, projected))
    entries = []
    for j in range(STEPS):
        column = [columns[j][rows + i : rows + i + 1, :] for i in range(j + 1)]
        column.append(columns[j][count : count + 1, :])
        entries.append(column)
    normal = [[None] * STEPS for _ in range(STEPS)]
    for a in range(STEPS):
        for b in range(a + 1):
            shared = range(min(len(entries[a]), len(entries[b])))
            normal[a][b] = tree_sum([entries[a][r] * entries[b][r] for r in shared])
    initial = start_ref[rows : rows + 1, :]
    least = small_solve(normal, [initial * entries[j][0] for j in range(STEPS)])
    image = []
    for r in range(STEPS + 1):
        image.append(tree_sum([entries[j][r] * least[j] for j in range(STEPS) if r < len(entries[j])]))
    start = start_ref[0:rows, :]
    recycled_coefficients = start[0:count] * -1.0
    for j in range(STEPS):
        recycled_coefficients = recycled_coefficients - columns[j][0:count] * least[j]
    ratio = image[STEPS] / norm
    head = jnp.where(down[0:rows] < count, start + columns[-1][0:rows] * ratio, start)
    tail_down = down[0:TAIL]
    solution_tail = jnp.zeros((TAIL, width), F32)
    residual_tail = jnp.zeros((TAIL, width), F32)
    for j in range(STEPS):
        solution_tail = jnp.where(tail_down == j, least[j], solution_tail)
        residual_tail = jnp.where(tail_down == j, entries[-1][j] * ratio - image[j], residual_tail)
    residual_tail = jnp.where(tail_down == STEPS, -ratio, residual_tail)
    for slot in range(slots):
        tail = tail_ref[slot]
        mask = mask_ref[slot : slot + 1, :]
        point = jnp.sum(recycled_ref[:, slot, :] * mask * recycled_coefficients, axis=0, keepdims=True)
        point = point + jnp.sum(tail * solution_tail, axis=0, keepdims=True)
        solution_ref[slot : slot + 1, :] = point
        left = jnp.sum(own_ref[slot] * head, axis=0, keepdims=True)
        left = left + jnp.sum(tail * residual_tail, axis=0, keepdims=True)
        residual_ref[slot : slot + 1, :] = left


def local(load_vector, recycled, images, matrix_tiles, tile_columns, ghost_list, live_counts):
    slots, width = load_vector.shape
    count = recycled.shape[0]
    doms, subs = lax.axis_size("dom"), lax.axis_size("sub")
    devices = doms * subs
    rows = round_up(count + 1, ROW_ALIGN)
    full = rows + TAIL
    per_row = tile_columns.shape[1]
    own, mask = call(
        pack_body, [(slots, rows, width), (round_up(slots, 8), width)], [SMEM, VMEM, VMEM]
    )(live_counts, load_vector, images)
    each = rows // lane_groups(count, rows, width)
    paired = subs % 2 == 0
    doubling = subs == 4

    def turn(value, bit):
        return lax.ppermute(value, "sub", [(i, i ^ bit) for i in range(subs)])

    if doubling:
        inner = turn(own, 1)
        outer = turn(own, 2)
        corner = turn(own, 3)
        (held,) = call(first_gram_body, [(rows, width)], [VMEM] * 2)(own, inner)
        outer, corner, held = lax.optimization_barrier((outer, corner, held))
        (group,) = call(join_body, [(subs * slots, rows, width)], [VMEM] * 4)(own, inner, outer, corner)
        (grams,) = call(functools.partial(gram_body, count), [(doms, each, width)], [VMEM] * 3)(held, outer, corner)
    else:
        group = lax.all_gather(own, "sub", axis=0, tiled=True)
        (grams,) = call(functools.partial(whole_gram_body, count), [(doms, each, width)], [VMEM])(group)
    parts = lax.all_to_all(grams, "dom", 0, 0)
    if paired:
        pairs = []
        for d in range(doms):
            for s in range(subs):
                to = d + 1 if (s + d) % 2 == 0 else d - 1
                if 0 <= to < doms:
                    pairs.append((d * subs + s, to * subs + s))
        one = lax.ppermute(group, AXES, pairs)
        early = call(functools.partial(early_body, count, rows), [(full, width)] * 2, [VMEM] * 3)(
            tile_columns, ghost_list, parts
        )
        one, parts, early = lax.optimization_barrier((one, parts, early))
        two = turn(one, 1)
    else:
        up = [(i, i + 1) for i in range(doms - 1)]
        one = lax.ppermute(group, "dom", up)
        two = lax.ppermute(group, "dom", [(j, i) for i, j in up])
        early = []
    lines = round_up(slots + 1, 4)
    near = 3 * group.shape[0]
    inverse, start, pick, tiles = call(
        functools.partial(factor_body, count, rows, paired, doubling),
        [(full, width), (full, width), (near + slots, slots * per_row, width), matrix_tiles.shape],
        [VMEM, VMEM, HBM, VMEM] + [VMEM] * len(early),
        [pltpu.SemaphoreType.DMA],
    )(tile_columns, ghost_list, pltpu.with_memory_space_constraint(matrix_tiles, pltpu.HBM), parts, *early)
    message, tails, own_tails = call(
        start_body, [(devices, lines, width), (near, TAIL, width), (slots, TAIL, width)], [VMEM] * 8
    )(start, own, one, group, two, tiles, pick, mask)
    histories = []
    for step in range(1, STEPS):
        every = lax.all_to_all(message, AXES, 0, 0)
        last = step == STEPS - 1
        sent = 1 if last else lines
        results = call(
            functools.partial(last_step_body if last else step_body, step, count, paired, doubling),
            [(devices, sent, width)]
            + ([] if last else [(near, TAIL, width)])
            + [(slots, TAIL, width), (full, width)],
            [VMEM] * 11,
        )(every, own, one, group, two, tails, own_tails, inverse, tiles, pick, mask)
        message, own_tails, history = results[0], results[-2], results[-1]
        tails = tails if last else results[1]
        histories.append(history)
    every = lax.all_to_all(message, AXES, 0, 0)
    return tuple(
        call(
            functools.partial(end_body, count), [(slots, width), (slots, width)], [VMEM] * (7 + len(histories))
        )(mask, every, own, own_tails, inverse, start, recycled, *histories)
    )


def solution(mesh):
    return jax.shard_map(
        local,
        mesh=mesh,
        in_specs=(
            P(("dom", "sub"), None),
            P(None, ("dom", "sub"), None),
            P(None, ("dom", "sub"), None),
            P(("dom", "sub"), None, None, None),
            P(("dom", "sub"), None),
            P(("dom", "sub"), None),
            P(("dom", "sub")),
        ),
        out_specs=(P(("dom", "sub"), None), P(("dom", "sub"), None)),
        check_vma=False,
    )
```

```python
import functools

import jax
import jax.numpy as jnp
from jax import lax
from jax.experimental import pallas as pl
from jax.experimental.pallas import tpu as pltpu
from jax.sharding import PartitionSpec as P


STEPS = 3
TAIL = 8
ROW_ALIGN = 8
AXES = ("dom", "sub")
VMEM = pl.BlockSpec(memory_space=pltpu.VMEM)
SMEM = pl.BlockSpec(memory_space=pltpu.SMEM)
HBM = pl.BlockSpec(memory_space=pltpu.HBM)
F32 = jnp.float32


def call(body, outs, specs, scratch=(), work=10_000_000):
    return pl.pallas_call(
        body,
        out_shape=[jax.ShapeDtypeStruct(shape, F32) for shape in outs],
        in_specs=specs,
        out_specs=[VMEM] * len(outs),
        scratch_shapes=list(scratch),
        cost_estimate=pl.CostEstimate(flops=work, bytes_accessed=1 << 20, transcendentals=0),
        compiler_params=pltpu.CompilerParams(vmem_limit_bytes=16 * 1024 * 1024),
    )


def round_up(value, step):
    return -(-value // step) * step


def eye(rows, lanes):
    down = lax.broadcasted_iota(jnp.int32, (rows, lanes), 0)
    across = lax.broadcasted_iota(jnp.int32, (rows, lanes), 1)
    return down == across


def to_row(column, mask):
    return jnp.sum(jnp.where(mask, column, 0.0), axis=0, keepdims=True)


def tree_sum(parts):
    while len(parts) > 1:
        pairs = [parts[i] + parts[i + 1] for i in range(0, len(parts) - 1, 2)]
        parts = pairs + parts[len(parts) - len(parts) % 2 :]
    return parts[0]


def pack_body(live_ref, load_ref, images_ref, own_ref, mask_ref):
    count, slots, width = images_ref.shape
    rows = own_ref.shape[1]
    line = lax.broadcasted_iota(jnp.int32, mask_ref.shape, 0)
    mask_ref[...] = jnp.where(line < live_ref[0], 1.0, 0.0).astype(F32)
    for slot in range(slots):
        mask = jnp.where(slot < live_ref[0], 1.0, 0.0).astype(F32)
        own_ref[slot, 0:count, :] = images_ref[:, slot, :] * mask
        own_ref[slot, count : count + 1, :] = load_ref[slot : slot + 1, :] * mask
        own_ref[slot, count + 1 : rows, :] = jnp.zeros((rows - count - 1, width), F32)


def join_body(*refs):
    place = 0
    for part in refs[:-1]:
        for block in range(part.shape[0]):
            refs[-1][place] = part[block]
            place += 1


def lane_groups(count, rows, width):
    groups = width // (count + 1)
    if rows % groups == 0 and (rows // groups) % ROW_ALIGN == 0:
        return groups
    return 1


def gram_of(*refs):
    products = []
    for ref in refs:
        for block in range(ref.shape[0]):
            part = ref[block]
            products.append(
                lax.dot_general(
                    part, part, (((1,), (1,)), ((), ())),
                    precision=lax.Precision.HIGHEST, preferred_element_type=F32,
                )
            )
    rows, width = refs[0].shape[1:]
    return jnp.concatenate([tree_sum(products), jnp.zeros((rows, width - rows), F32)], axis=1)


def first_gram_body(paired, doubling, columns_ref, ghosts_ref, *refs):
    parts, (out_ref, pick_ref) = refs[:-2], refs[-2:]
    out_ref[...] = gram_of(*parts)
    write_picks(paired, doubling, columns_ref, ghosts_ref, pick_ref)


def gram_body(count, held_ref, *refs):
    parts, out_ref = refs[:-1], refs[-1]
    rows, width = parts[0].shape[1:]
    gram = gram_of(*parts)
    if held_ref is not None:
        gram = gram + held_ref[...]
    groups = lane_groups(count, rows, width)
    each, lanes = rows // groups, width // groups
    packed = gram[0:each]
    for group in range(1, groups):
        packed = packed + pltpu.roll(gram[group * each : (group + 1) * each], group * lanes, 1)
    for copy in range(out_ref.shape[0]):
        out_ref[copy] = packed


def whole_gram_body(count, group_ref, out_ref):
    gram_body(count, None, group_ref, out_ref)


def multiply(left, right):
    return [[tree_sum([a * right[k][j] for k, a in enumerate(row)]) for j in range(len(right[0]))] for row in left]


def symmetric(left, right):
    size = len(left)
    half = [[tree_sum([a * right[k][j] for k, a in enumerate(left[i])]) for j in range(i + 1)] for i in range(size)]
    return [[half[max(i, j)][min(i, j)] for j in range(size)] for i in range(size)]


def small_inverse(matrix):
    size = len(matrix)
    if size == 1:
        return [[1.0 / matrix[0][0]]]
    half = size // 2
    corner = [row[half:] for row in matrix[:half]]
    rest = [row[half:] for row in matrix[half:]]
    first = small_inverse([row[:half] for row in matrix[:half]])
    across = multiply(first, corner)
    taken = symmetric([list(row) for row in zip(*corner)], across)
    left = [[rest[i][j] - taken[i][j] for j in range(i + 1)] for i in range(half)]
    second = small_inverse([[left[max(i, j)][min(i, j)] for j in range(half)] for i in range(half)])
    product = multiply(across, second)
    added = symmetric(product, [list(row) for row in zip(*across)])
    total = [[first[i][j] + added[i][j] for j in range(i + 1)] for i in range(half)]
    top = [[total[max(i, j)][min(i, j)] for j in range(half)] + [-value for value in product[i]] for i in range(half)]
    bottom = [[-product[j][i] for j in range(half)] + second[i] for i in range(half)]
    return top + bottom


def sweep(matrix, count):
    rows, width = matrix.shape
    size = next(size for size in (8, 4, 2, 1) if count % size == 0)
    tiles = [matrix[i : i + 8, :] for i in range(0, rows, 8)]
    across = lax.broadcasted_iota(jnp.int32, (8, width), 1)
    down = lax.broadcasted_iota(jnp.int32, (8, width), 0)

    def spread(value):
        return jnp.broadcast_to(value, (8, width))

    for k in range(0, count, size):
        at, inner = divmod(k, 8)
        columns = [[tile[:, k + i : k + i + 1] for tile in tiles] for i in range(size)]
        lines = [spread(tiles[at][inner + i : inner + i + 1, :]) for i in range(size)]
        full = [spread(columns[i][at]) for i in range(size)]
        pivots = [
            [spread(full[max(i, j)][inner + min(i, j) : inner + min(i, j) + 1, :]) for j in range(size)]
            for i in range(size)
        ]
        inverse = small_inverse(pivots)
        inside = (across >= k) & (across < k + size)
        lines = [jnp.where(inside, jnp.where(across == k + i, 1.0, 0.0), line) for i, line in enumerate(lines)]
        scaled = [tree_sum([lines[j] * inverse[i][j] for j in range(size)]) for i in range(size)]
        updated = []
        for n, tile in enumerate(tiles):
            if n == at and size == 8:
                value = scaled[0]
            else:
                value = jnp.where(inside, 0.0, tile)
                value = value - tree_sum([columns[i][n] * scaled[i] for i in range(size)])
            if n == at:
                for i in range(size):
                    value = jnp.where(down == inner + i, scaled[i], value)
            updated.append(value)
        tiles = updated
    return jnp.concatenate(tiles, axis=0)


def apply_tiles(tiles_ref, pick_ref, vectors, mask_ref):
    slots, per_row, size, _ = tiles_ref.shape
    mask = eye(size, size)
    images = []
    for slot in range(slots):
        picked = tree_sum(
            [pick_ref[e, slot * per_row : (slot + 1) * per_row, :] * vector for e, vector in enumerate(vectors)]
        )
        parts = [tiles_ref[slot, t] * picked[t : t + 1, :] for t in range(per_row)]
        column = jnp.sum(tree_sum(parts), axis=1, keepdims=True)
        images.append(to_row(column, mask) * mask_ref[slot : slot + 1, :])
    return images


def tail_with(old, row, value):
    down = lax.broadcasted_iota(jnp.int32, (TAIL, old.shape[1]), 0)
    return jnp.where(down == row, value, old)


def finish_step(vectors, tails, own_ref, tiles_ref, pick_ref, mask_ref, own_tail_ref, out_ref):
    slots, rows, width = own_ref.shape
    images = apply_tiles(tiles_ref, pick_ref, vectors, mask_ref)
    total = jnp.zeros((rows + TAIL, width), F32)
    for slot in range(slots):
        tail = tail_with(tails[slot], STEPS, images[slot])
        own_tail_ref[slot] = tail
        total = total + jnp.concatenate([own_ref[slot], tail], axis=0) * images[slot]
    partial = to_row(jnp.sum(total, axis=1, keepdims=True), eye(rows + TAIL, width))
    copies, lines, _ = out_ref.shape
    if lines == 1:
        message = partial
    else:
        pad = [jnp.zeros((lines - slots - 1, width), F32)] if lines > slots + 1 else []
        message = jnp.concatenate([*images, partial, *pad], axis=0)
    out_ref[...] = jnp.broadcast_to(message[None], (copies, lines, width))


def near_peers(subs, paired, doubling):
    me = lax.axis_index("sub")
    first = (1 - me % 2) * 2 if paired else 0
    result = []
    for part, swapped in ((first, 0), (1, 0), (2 - first, 1 if paired else 0)):
        result.append((part, [(peer ^ swapped) ^ me if doubling else peer for peer in range(subs)]))
    return result


def write_picks(paired, doubling, columns_ref, ghosts_ref, pick_ref):
    width = pick_ref.shape[2]
    slots, per_row = columns_ref.shape
    blocks = (pick_ref.shape[0] - slots) // 3
    places = [
        part * blocks + peer * slots + slot
        for part, peers in near_peers(blocks // slots, paired, doubling)
        for peer in peers
        for slot in range(slots)
    ]
    places += [3 * blocks + slot for slot in range(slots)]
    for slot in range(slots):
        names = columns_ref[slot : slot + 1, :]
        wanted = names + 3 * blocks
        for ghost in range(ghosts_ref.shape[1]):
            wanted = jnp.where(names == slots + ghost, ghosts_ref[:, ghost : ghost + 1], wanted)
        wanted = wanted.astype(F32)
        column = jnp.sum(jnp.where(eye(per_row, per_row), wanted, 0.0), axis=1, keepdims=True)
        column = jnp.broadcast_to(column, (per_row, width)).astype(jnp.int32)
        for at, place in enumerate(places):
            pick_ref[at, slot * per_row : (slot + 1) * per_row, :] = jnp.where(column == place, 1.0, 0.0)


def factor_body(count, rows, tiles_ref, parts_ref, inverse_ref, start_ref, here_ref, sem):
    move = pltpu.make_async_copy(tiles_ref, here_ref, sem)
    move.start()
    width = parts_ref.shape[2]
    groups = lane_groups(count, rows, width)
    lanes = width // groups
    packed = lax.fori_loop(1, parts_ref.shape[0], lambda i, held: held + parts_ref[i], parts_ref[0])
    across = lax.broadcasted_iota(jnp.int32, (rows, width), 1)
    down = lax.broadcasted_iota(jnp.int32, (rows, width), 0)
    pieces = [packed]
    for group in range(1, groups):
        pieces.append(pltpu.roll(packed, width - group * lanes, 1))
    gram = jnp.where(across <= count, jnp.concatenate(pieces, axis=0), 0.0)
    swept = sweep(gram, count)
    keep = (down < count) & (across < count)
    inverse_ref[0:rows, :] = jnp.where(keep, swept, 0.0)
    tail_down = lax.broadcasted_iota(jnp.int32, (TAIL, width), 0)
    tail_across = lax.broadcasted_iota(jnp.int32, (TAIL, width), 1)
    inverse_ref[rows : rows + TAIL, :] = jnp.where(
        (tail_down < STEPS) & (tail_across == tail_down + rows), 1.0, 0.0
    )
    squared = jnp.broadcast_to(swept[count : count + 1, count : count + 1], (TAIL, width))
    inverse_norm = lax.rsqrt(squared)
    start = jnp.where(down < count, -swept[:, count : count + 1], jnp.where(down == count, 1.0, 0.0))
    start_ref[0:rows, :] = start
    start_ref[rows : rows + TAIL, :] = jnp.where(tail_down == 0, squared * inverse_norm, inverse_norm)
    move.wait()


def start_body(
    start_ref, own_ref, one_ref, group_ref, two_ref, tiles_ref, pick_ref, mask_ref, out_ref, tail_ref, own_tail_ref
):
    _, rows, width = own_ref.shape
    blocks = group_ref.shape[0]
    coefficients = start_ref[0:rows, :] * start_ref[rows + 1 : rows + 2, :]
    empty = jnp.zeros((TAIL, width), F32)
    vectors = []
    tails = []
    for part in (one_ref, group_ref, two_ref, own_ref):
        for place in range(part.shape[0]):
            vector = jnp.sum(part[place] * coefficients, axis=0, keepdims=True)
            tail = tail_with(empty, 0, vector)
            if len(vectors) < 3 * blocks:
                tail_ref[len(vectors)] = tail
            else:
                tails.append(tail)
            vectors.append(vector)
    finish_step(vectors, tails, own_ref, tiles_ref, pick_ref, mask_ref, own_tail_ref, out_ref)


def project(total_row, inverse, rows, width):
    full = rows + TAIL
    down = lax.broadcasted_iota(jnp.int32, (full, width), 0)
    projected = jnp.sum(inverse * total_row, axis=1, keepdims=True)
    column = jnp.sum(jnp.where(eye(full, width), total_row, 0.0), axis=1, keepdims=True)
    projected = jnp.broadcast_to(projected, (full, width))
    squared = jnp.sum(
        jnp.where(down == rows + STEPS, column, -(column * projected)), axis=0, keepdims=True
    )
    inverse_norm = lax.rsqrt(squared)
    return projected, squared * inverse_norm, inverse_norm, down


def step_body(
    step, count, paired, doubling, every_ref, own_ref, one_ref, group_ref, two_ref, old_ref, old_own_ref, inverse_ref,
    tiles_ref, pick_ref, mask_ref, out_ref, tail_ref, own_tail_ref, history_ref,
):
    slots, rows, width = own_ref.shape
    subs = lax.axis_size("sub")
    last_dom = lax.axis_size("dom") - 1
    total_row = tree_sum([every_ref[i, slots : slots + 1, :] for i in range(every_ref.shape[0])])
    projected, norm, inverse_norm, down = project(total_row, inverse_ref[...], rows, width)
    history_ref[...] = jnp.where(down == count, norm, projected)
    coefficients = jnp.where(down == rows + STEPS, inverse_norm, -(projected * inverse_norm))
    head, foot = coefficients[0:rows], coefficients[rows : rows + TAIL]
    vectors = []
    for part, (offset, peers) in zip((one_ref, group_ref, two_ref), near_peers(subs, paired, doubling)):
        first = jnp.clip(lax.axis_index("dom") + offset - 1, 0, last_dom) * subs
        for place in range(part.shape[0]):
            at = len(vectors)
            old = old_ref[at]
            image = every_ref[first + peers[place // slots], place % slots : place % slots + 1, :]
            vector = jnp.sum(part[place] * head, axis=0, keepdims=True)
            vector = vector + jnp.sum(old * foot, axis=0, keepdims=True) + image * inverse_norm
            if tail_ref is not None:
                tail_ref[at] = tail_with(old, step, vector)
            vectors.append(vector)
    tails = []
    for slot in range(slots):
        old = old_own_ref[slot]
        vector = jnp.sum(own_ref[slot] * head, axis=0, keepdims=True)
        vector = vector + jnp.sum(old * foot, axis=0, keepdims=True)
        tails.append(tail_with(old, step, vector))
        vectors.append(vector)
    finish_step(vectors, tails, own_ref, tiles_ref, pick_ref, mask_ref, own_tail_ref, out_ref)


def last_step_body(step, count, paired, doubling, *refs):
    step_body(step, count, paired, doubling, *refs[:12], None, *refs[12:])


def small_solve(matrix, target):
    size = len(target)
    low = [[None] * size for _ in range(size)]
    inverses = []
    for j in range(size):
        value = matrix[j][j]
        for k in range(j):
            value = value - low[j][k] * low[j][k]
        inverses.append(1.0 / jnp.sqrt(value))
        for i in range(j + 1, size):
            value = matrix[i][j]
            for k in range(j):
                value = value - low[i][k] * low[j][k]
            low[i][j] = value * inverses[j]
    forward = []
    for i in range(size):
        value = target[i]
        for k in range(i):
            value = value - low[i][k] * forward[k]
        forward.append(value * inverses[i])
    back = [None] * size
    for i in reversed(range(size)):
        value = forward[i]
        for k in range(i + 1, size):
            value = value - low[k][i] * back[k]
        back[i] = value * inverses[i]
    return back


def end_body(count, mask_ref, every_ref, own_ref, tail_ref, inverse_ref, start_ref, recycled_ref, *rest):
    histories, (solution_ref, residual_ref) = rest[:-2], rest[-2:]
    slots, rows, width = own_ref.shape
    total_row = tree_sum([every_ref[i] for i in range(every_ref.shape[0])])
    projected, norm, _, down = project(total_row, inverse_ref[...], rows, width)
    columns = [history[...] for history in histories]
    columns.append(jnp.where(down == count, norm, projected))
    entries = []
    for j in range(STEPS):
        column = [columns[j][rows + i : rows + i + 1, :] for i in range(j + 1)]
        column.append(columns[j][count : count + 1, :])
        entries.append(column)
    normal = [[None] * STEPS for _ in range(STEPS)]
    for a in range(STEPS):
        for b in range(a + 1):
            shared = range(min(len(entries[a]), len(entries[b])))
            normal[a][b] = tree_sum([entries[a][r] * entries[b][r] for r in shared])
    initial = start_ref[rows : rows + 1, :]
    least = small_solve(normal, [initial * entries[j][0] for j in range(STEPS)])
    image = []
    for r in range(STEPS + 1):
        image.append(tree_sum([entries[j][r] * least[j] for j in range(STEPS) if r < len(entries[j])]))
    start = start_ref[0:rows, :]
    recycled_coefficients = start[0:count] * -1.0
    for j in range(STEPS):
        recycled_coefficients = recycled_coefficients - columns[j][0:count] * least[j]
    ratio = image[STEPS] / norm
    head = jnp.where(down[0:rows] < count, start + columns[-1][0:rows] * ratio, start)
    tail_down = down[0:TAIL]
    solution_tail = jnp.zeros((TAIL, width), F32)
    residual_tail = jnp.zeros((TAIL, width), F32)
    for j in range(STEPS):
        solution_tail = jnp.where(tail_down == j, least[j], solution_tail)
        residual_tail = jnp.where(tail_down == j, entries[-1][j] * ratio - image[j], residual_tail)
    residual_tail = jnp.where(tail_down == STEPS, -ratio, residual_tail)
    for slot in range(slots):
        tail = tail_ref[slot]
        mask = mask_ref[slot : slot + 1, :]
        point = jnp.sum(recycled_ref[:, slot, :] * mask * recycled_coefficients, axis=0, keepdims=True)
        point = point + jnp.sum(tail * solution_tail, axis=0, keepdims=True)
        solution_ref[slot : slot + 1, :] = point
        left = jnp.sum(own_ref[slot] * head, axis=0, keepdims=True)
        left = left + jnp.sum(tail * residual_tail, axis=0, keepdims=True)
        residual_ref[slot : slot + 1, :] = left


def local(load_vector, recycled, images, matrix_tiles, tile_columns, ghost_list, live_counts):
    slots, width = load_vector.shape
    count = recycled.shape[0]
    doms, subs = lax.axis_size("dom"), lax.axis_size("sub")
    devices = doms * subs
    rows = round_up(count + 1, ROW_ALIGN)
    full = rows + TAIL
    own, mask = call(
        pack_body, [(slots, rows, width), (round_up(slots, 8), width)], [SMEM, VMEM, VMEM]
    )(live_counts, load_vector, images)
    each = rows // lane_groups(count, rows, width)
    paired = subs % 2 == 0
    doubling = subs == 4
    near = 3 * subs * slots
    picks = (near + slots, slots * tile_columns.shape[1], width)

    def turn(value, bit):
        return lax.ppermute(value, "sub", [(i, i ^ bit) for i in range(subs)])

    if doubling:
        inner = turn(own, 1)
        outer = turn(own, 2)
        corner = turn(own, 3)
        held, pick = call(
            functools.partial(first_gram_body, paired, doubling), [(rows, width), picks], [VMEM] * 4
        )(tile_columns, ghost_list, own, inner)
        outer, corner, held = lax.optimization_barrier((outer, corner, held))
        (group,) = call(join_body, [(subs * slots, rows, width)], [VMEM] * 4)(own, inner, outer, corner)
        (grams,) = call(functools.partial(gram_body, count), [(doms, each, width)], [VMEM] * 3)(held, outer, corner)
    else:
        group = lax.all_gather(own, "sub", axis=0, tiled=True)
        (pick,) = call(functools.partial(write_picks, paired, doubling), [picks], [VMEM] * 2)(tile_columns, ghost_list)
        (grams,) = call(functools.partial(whole_gram_body, count), [(doms, each, width)], [VMEM])(group)
    parts = lax.all_to_all(grams, "dom", 0, 0)
    if paired:
        pairs = []
        for d in range(doms):
            for s in range(subs):
                to = d + 1 if s % 2 else d - 1
                if 0 <= to < doms:
                    pairs.append((d * subs + s, to * subs + s))
        one = lax.ppermute(group, AXES, pairs)
        one, parts = lax.optimization_barrier((one, parts))
        two = turn(one, 1)
    else:
        up = [(i, i + 1) for i in range(doms - 1)]
        one = lax.ppermute(group, "dom", up)
        two = lax.ppermute(group, "dom", [(j, i) for i, j in up])
    lines = round_up(slots + 1, 4)
    inverse, start, tiles = call(
        functools.partial(factor_body, count, rows),
        [(full, width), (full, width), matrix_tiles.shape],
        [HBM, VMEM],
        [pltpu.SemaphoreType.DMA],
    )(pltpu.with_memory_space_constraint(matrix_tiles, pltpu.HBM), parts)
    message, tails, own_tails = call(
        start_body, [(devices, lines, width), (near, TAIL, width), (slots, TAIL, width)], [VMEM] * 8
    )(start, own, one, group, two, tiles, pick, mask)
    histories = []
    for step in range(1, STEPS):
        every = lax.all_to_all(message, AXES, 0, 0)
        last = step == STEPS - 1
        sent = 1 if last else lines
        results = call(
            functools.partial(last_step_body if last else step_body, step, count, paired, doubling),
            [(devices, sent, width)]
            + ([] if last else [(near, TAIL, width)])
            + [(slots, TAIL, width), (full, width)],
            [VMEM] * 11,
        )(every, own, one, group, two, tails, own_tails, inverse, tiles, pick, mask)
        message, own_tails, history = results[0], results[-2], results[-1]
        tails = tails if last else results[1]
        histories.append(history)
    every = lax.all_to_all(message, AXES, 0, 0)
    return tuple(
        call(
            functools.partial(end_body, count), [(slots, width), (slots, width)], [VMEM] * (7 + len(histories))
        )(mask, every, own, own_tails, inverse, start, recycled, *histories)
    )


def solution(mesh):
    return jax.shard_map(
        local,
        mesh=mesh,
        in_specs=(
            P(("dom", "sub"), None),
            P(None, ("dom", "sub"), None),
            P(None, ("dom", "sub"), None),
            P(("dom", "sub"), None, None, None),
            P(("dom", "sub"), None),
            P(("dom", "sub"), None),
            P(("dom", "sub")),
        ),
        out_specs=(P(("dom", "sub"), None), P(("dom", "sub"), None)),
        check_vma=False,
    )
```
